512 devices in a mesh: gx: 4 (over x), gy: 8 (over y), gz: 16 (over z, core).
Axes of the slice: x: 4, y: 8, z: 8, core: 2. Of those that a mesh axis runs over, the one named last changes fastest.
Arguments:
- opening_warmth_field: float32 [32, 128, 2048], P('gx', 'gy', 'gz'), may hold values from -42 to 42
- cellwise_warming_source: float32 [32, 128, 2048], P('gx', 'gy', 'gz'), may hold values from -6 to 6
- substance_category_per_voxel: int32 [32, 128, 2048], P('gx', 'gy', 'gz'), may hold values from 0 to 15
- thermal_coefficient_table: float32 [16], replicated, may hold values from 0.2 to 5
- boundary_cooling_flags: int32 [32, 128, 2048], P('gx', 'gy', 'gz'), may hold values 0 or 1
Outputs:
- closing_warmth_field: float32 [32, 128, 2048], P('gx', 'gy', 'gz')
- remaining_mismatch: float32 [32, 128, 2048], P('gx', 'gy', 'gz')
The draws below stay inside these ranges and needn't reach their ends.
All inputs are finite; a program needn't handle non-finite values. No bound on the sum of `boundary_cooling_flags` on one device may be relied on, other than what follows from the above.
Results may differ from the reference program's by a relative error of at most 0.00055.
Values sent between devices are 32-bit elements; how exact they have to be, the bound alone decides.
No kernel may reach another device: no remote copies, remote signals or barrier semaphores. Data moves between devices by JAX's collectives and lax.ppermute only.
A program may use at most 64 MiB of HBM per device.

```python
import math
import jax
import jax.numpy as jnp
from jax import lax

ITERS = 4
TSTEPS = 1
CLASSES = 16
NX = 32
NY = 128
NZ = 2048


def draw_opening_warmth_field(key, part):
    keys = jax.random.split(key, 1)
    ramp = (1.0 + 2.0 * jnp.arange(NX, dtype=jnp.float32) / (NX - 1))[:, None, None]
    values = jax.random.truncated_normal(keys[0], -5.0, 5.0, (NX, NY, NZ), jnp.float32) * ramp
    return values.astype(jnp.float32)


def place_ends(entries, key, least, top_value):
    longest = entries.shape.index(max(entries.shape))
    spots = []
    for shift in (0, 1):
        where = [jax.random.randint(jax.random.fold_in(key, axis), (), 0, length) for axis, length in enumerate(entries.shape)]
        where[longest] = (where[longest] + shift) % entries.shape[longest]
        spots.append(tuple(where))
    return entries.at[spots[0]].set(least).at[spots[1]].set(top_value)


def block_scale(stream_key, extent, cuts, least, high):
    def one(dim, blocks):
        draws = jax.random.uniform(jax.random.fold_in(jax.random.fold_in(stream_key, 6), dim), (blocks,), jnp.float32, least / len(cuts), high / len(cuts))
        return jnp.repeat(jnp.exp(draws), extent[dim] // blocks).reshape((-1,) + (1,) * (len(extent) - dim - 1))

    factor_of = one(*cuts[0])
    for cut in cuts[1:]:
        factor_of = factor_of * one(*cut)
    return factor_of


def normal_values(own_key, shape, scale, reach, cuts=(), held_as=jnp.bfloat16):
    loudness = block_scale(own_key, shape, cuts, -0.22, 0.18) if cuts else 1.0
    drawn = jax.random.normal(own_key, shape, jnp.float32) * scale * loudness
    return jnp.minimum(jnp.maximum(drawn, -reach), reach).astype(held_as)


def setup_inputs(seed: int = 0) -> dict:
    key_list = jax.random.split(jax.random.key(seed), 6)
    opening_warmth_field = draw_opening_warmth_field(jax.random.fold_in(key_list[5], 71), 0)
    cellwise_warming_source = normal_values(key_list[1], (NX, NY, NZ), 1.0, 6.0, ((0, 4), (1, 8), (2, 16)), jnp.float32)
    substance_category_per_voxel = place_ends(jax.random.randint(key_list[2], (NX, NY, NZ), 0, CLASSES), jax.random.fold_in(key_list[2], 1), 0, CLASSES - 1).astype(jnp.int32)
    thermal_coefficient_table = jnp.clip(jnp.exp(jax.random.uniform(key_list[3], (CLASSES,), jnp.float32, math.log(0.2), math.log(5.0))), 0.2, 5.0)
    boundary_cooling_flags = place_ends((jax.random.randint(key_list[4], (NX, NY, NZ), 0, 4) < 1).astype(jnp.int32), jax.random.fold_in(key_list[4], 1), 0, 1)
    return {"opening_warmth_field": opening_warmth_field, "cellwise_warming_source": cellwise_warming_source, "substance_category_per_voxel": substance_category_per_voxel, "thermal_coefficient_table": thermal_coefficient_table, "boundary_cooling_flags": boundary_cooling_flags}


interval_delta = 2.0
cooling = 3.0
kind_weights = (1.0, 0.5, 0.25)
kind_counts = (6.0, 12.0, 8.0)


def split_axis(values, axis):
    length = values.shape[axis] - 2
    center = lax.slice_in_dim(values, 1, length + 1, axis=axis)
    beside = lax.slice_in_dim(values, 0, length, axis=axis) + lax.slice_in_dim(values, 2, length + 2, axis=axis)
    return center, beside


def neighbor_sums(padded):
    leading_extent = padded.ndim - 3
    pieces = [(padded, 0)]
    for shift_vector in range(3):
        next_pieces = []
        for values, neighbors in pieces:
            center, beside = split_axis(values, leading_extent + shift_vector)
            next_pieces.append((center, neighbors))
            next_pieces.append((beside, neighbors + 1))
        pieces = next_pieces
    totals = [None, None, None]
    for values, neighbors in pieces:
        if neighbors > 0:
            if totals[neighbors - 1] is None:
                totals[neighbors - 1] = values
            else:
                totals[neighbors - 1] = totals[neighbors - 1] + values
    return totals


def coupling(padded, padded_flux, cond):
    field_sums = neighbor_sums(padded)
    accumulated_flux = neighbor_sums(padded_flux)
    computed_output = kind_weights[0] * (cond * field_sums[0] + accumulated_flux[0])
    computed_output = computed_output + kind_weights[1] * (cond * field_sums[1] + accumulated_flux[1])
    computed_output = computed_output + kind_weights[2] * (cond * field_sums[2] + accumulated_flux[2])
    return computed_output


def reference(opening_warmth_field, cellwise_warming_source, substance_category_per_voxel, thermal_coefficient_table, boundary_cooling_flags):
    cond = jnp.take(thermal_coefficient_table, substance_category_per_voxel)
    cond_sums = neighbor_sums(jnp.pad(cond, 1))
    spread = kind_weights[0] * (kind_counts[0] * cond + cond_sums[0])
    spread = spread + kind_weights[1] * (kind_counts[1] * cond + cond_sums[1])
    spread = spread + kind_weights[2] * (kind_counts[2] * cond + cond_sums[2])
    diagonal = 1.0 + interval_delta * cooling * boundary_cooling_flags.astype(jnp.float32) + 0.5 * interval_delta * spread

    def apply_stencil_matrix(field):
        padded = jnp.pad(field, 1)
        padded_flux = jnp.pad(cond * field, 1)
        return diagonal * field - 0.5 * interval_delta * coupling(padded, padded_flux, cond)

    closing_warmth_field = opening_warmth_field
    remaining_mismatch = opening_warmth_field
    for tstep in range(TSTEPS):
        forcing_term = closing_warmth_field + interval_delta * cellwise_warming_source
        remaining_mismatch = forcing_term - apply_stencil_matrix(closing_warmth_field)
        search_heading = remaining_mismatch
        norm_now = jnp.sum(remaining_mismatch * remaining_mismatch)
        for step in range(ITERS):
            image = apply_stencil_matrix(search_heading)
            descent_alpha = norm_now / jnp.sum(search_heading * image)
            closing_warmth_field = closing_warmth_field + descent_alpha * search_heading
            remaining_mismatch = remaining_mismatch - descent_alpha * image
            following_norm = jnp.sum(remaining_mismatch * remaining_mismatch)
            search_heading = remaining_mismatch + (following_norm / norm_now) * search_heading
            norm_now = following_norm
    return closing_warmth_field, remaining_mismatch
```

```python
import jax
import jax.numpy as jnp
from jax import lax
from jax.sharding import Mesh
from jax.sharding import PartitionSpec as P

ITERS = 4
GZ = ("gz_0", "gz_1")
HALO = ITERS + 1


def padded(cells, sides, width):
    for axis, dim in sides:
        count = lax.axis_size(axis)
        ends = count - 1
        head = lax.slice_in_dim(cells, 0, width, axis=dim)
        tail = lax.slice_in_dim(cells, cells.shape[dim] - width, cells.shape[dim], axis=dim)
        cells = jnp.concatenate(
            [
                lax.ppermute(tail, axis, [(i, i + 1) for i in range(ends)]),
                cells,
                lax.ppermute(head, axis, [(i + 1, i) for i in range(ends)]),
            ],
            axis=dim,
        )
    return cells


def over(array, axes):
    copies = jnp.broadcast_to(array, (lax.axis_size(axes), 1, array.shape[0]))
    return lax.all_to_all(copies, axes, split_axis=0, concat_axis=0, tiled=True).sum(axis=(0, 1))


def smooth(values):
    for dim in range(3):
        n = values.shape[dim]
        low = lax.slice_in_dim(values, 0, n - 2, axis=dim)
        mid = lax.slice_in_dim(values, 1, n - 1, axis=dim)
        high = lax.slice_in_dim(values, 2, n, axis=dim)
        values = mid + 0.5 * (low + high)
    return values


def inner(values, by):
    return values[by:-by, by:-by, by:-by] if by else values


def body(opening, source, category, table, flags):
    classes = table.shape[0]
    picks = category[None] == jnp.arange(classes, dtype=jnp.int32)[:, None, None, None]
    cond = jnp.sum(jnp.where(picks, table[:, None, None, None], 0.0), axis=0)
    flag = flags.astype(jnp.float32)
    rest = 2.0 * source - 6.0 * flag * opening
    fields = padded(
        jnp.stack([cond, opening, rest, flag]), (("gx", 1), ("gy", 2), (GZ, 3)), HALO
    )
    cond, start, rest, flag = fields

    least, most, mean = jnp.min(table), jnp.max(table), jnp.mean(table)
    top = 4.0 + 16.0 * most + 16.0 * mean
    low = 2.0 + 8.0 * least + 8.0 * mean
    half = 0.5 * (top - low)
    middle = 0.5 * (top + low)
    shifts = [middle + half * c for c in (0.9238795, -0.9238795, 0.3826834, -0.3826834)]

    near = 16.0 * inner(cond, 1) + 2.0 * smooth(cond)
    diagonal = near + 1.0 + 6.0 * inner(flag, 1)
    inside = (inner(cond, 1) > 0.0).astype(jnp.float32)
    c1 = inner(cond, 1)
    vector = inside * (
        inner(rest, 1) - near * inner(start, 1) + 2.0 * (c1 * smooth(start) + smooth(cond * start))
    )
    basis = [vector]
    for k in range(ITERS):
        at = inner(cond, k + 1)
        d, c, m = (inner(a, k + 1) for a in (diagonal, c1, inside))
        image = (d - shifts[k]) * inner(vector, 1) - 2.0 * (c * smooth(vector) + smooth(at * vector))
        vector = m * image / half
        basis.append(vector)
    own = [inner(v, ITERS - k) for k, v in enumerate(basis)]
    start = inner(start, HALO)

    pairs = [(i, j) for i in range(ITERS) for j in range(i, ITERS + 1)]
    dots = jnp.stack([jnp.sum(own[i] * own[j]) for i, j in pairs])
    dots = over(over(dots, ("gx", "gz_1")), ("gy", "gz_0"))
    gram = {}
    for n, (i, j) in enumerate(pairs):
        gram[i, j] = gram[j, i] = dots[n]

    def product(a, b):
        return sum(
            sum(gram[i, j] * a[i] * b[j] for j in range(len(b))) for i in range(len(a))
        )

    zero = jnp.zeros((), jnp.float32)
    r = [zero + 1.0]
    p = list(r)
    y = [zero] * ITERS
    rr = gram[0, 0]
    for k in range(ITERS):
        image = [shifts[i] * p[i] for i in range(k + 1)] + [zero]
        for i in range(k + 1):
            image[i + 1] = image[i + 1] + half * p[i]
        step = rr / product(p, image)
        y = [y[i] + step * p[i] if i <= k else y[i] for i in range(ITERS)]
        r = [(r[i] if i <= k else zero) - step * image[i] for i in range(k + 2)]
        if k + 1 < ITERS:
            new = product(r, r)
            p = [r[i] + (new / rr) * (p[i] if i <= k else zero) for i in range(k + 2)]
            rr = new
    closing = start + sum(y[i] * own[i] for i in range(ITERS))
    mismatch = sum(r[i] * own[i] for i in range(ITERS + 1))
    return closing, mismatch


def solution(mesh):
    split = Mesh(
        mesh.devices.reshape(mesh.shape["gx"], mesh.shape["gy"], 8, 2), ("gx", "gy", "gz_0", "gz_1")
    )
    spec = P("gx", "gy", GZ)
    return jax.shard_map(
        body, mesh=split, in_specs=(spec, spec, spec, P(), spec), out_specs=(spec, spec), check_vma=False
    )
```

```python
import jax
import jax.numpy as jnp
from jax import lax
from jax.experimental import pallas as pl
from jax.experimental.pallas import tpu as pltpu
from jax.sharding import Mesh
from jax.sharding import PartitionSpec as P

ITERS = 4
GZ = ("gz_0", "gz_1")
F32 = jnp.float32
X, Y, Z = 8, 16, 128
HALO = ITERS + 1
WIDTHS = (5, 5, 4, 3)
PLANES = X + 2 * HALO
ROWS = 32
TOP = 8
SLAB_X = sum(WIDTHS)
AT_X = (0, 5, 10, 14)
AT_Y = (0, 90, 180, 244)
SLAB_Y = 288
GROUPS, PER_GROUP, STRIDE = 3, 6, 40
BASES = (5, 15, 24, 31)
SCALE = 64.0
PAIRS = [(i, j) for i in range(ITERS) for j in range(i, ITERS + 1)]
VMEM = pl.BlockSpec(memory_space=pltpu.VMEM)
SMEM = pl.BlockSpec(memory_space=pltpu.SMEM)


def planes_of(k):
    return range(HALO - WIDTHS[k], PLANES - HALO + WIDTHS[k])


def call(kernel, ins, outs, scratch=(), flops=100000, vmem=8):
    return pl.pallas_call(
        kernel,
        in_specs=ins,
        out_specs=[VMEM] * len(outs),
        out_shape=[jax.ShapeDtypeStruct(s, F32) for s in outs],
        scratch_shapes=[pltpu.VMEM(s, F32) for s in scratch],
        compiler_params=pltpu.CompilerParams(vmem_limit_bytes=vmem * 2**20),
        cost_estimate=pl.CostEstimate(flops=flops, bytes_accessed=1000000, transcendentals=0),
    )


def prepare(opening, source, category, flags, table, fields, low, high):
    for p in range(X):
        kind = category[p]
        cond = jnp.full((Y, Z), table[0], F32)
        for n in range(1, table.shape[0]):
            cond = jnp.where(kind == n, table[n], cond)
        flag = flags[p].astype(F32)
        start = opening[p]
        values = (cond, start, 2.0 * source[p] - 6.0 * flag * start, flag)
        for k, v in enumerate(values):
            fields[k, p] = v
            if p < WIDTHS[k]:
                low[AT_X[k] + p] = v
            if p >= X - WIDTHS[k]:
                high[AT_X[k] + p - (X - WIDTHS[k])] = v


def plane(fields, left, right, k, p):
    if p < HALO:
        return left, (AT_X[k] + p - (HALO - WIDTHS[k]),)
    if p < HALO + X:
        return fields, (k, p - HALO)
    return right, (AT_X[k] + p - HALO - X,)


def slabs_y(fields, left, right, low, high):
    for k, w in enumerate(WIDTHS):
        for n, p in enumerate(planes_of(k)):
            ref, at = plane(fields, left, right, k, p)
            to = pl.ds(AT_Y[k] + w * n, w)
            low[to] = ref[(*at, pl.ds(0, w))]
            high[to] = ref[(*at, pl.ds(Y - w, w))]


def assemble(fields, left, right, below, above, wide, packed):
    lane = lax.broadcasted_iota(jnp.int32, (ROWS, Z), 1)
    nothing = jnp.zeros((8, Z), F32)
    for k, w in enumerate(WIDTHS):
        for n, p in enumerate(planes_of(k)):
            ref, at = plane(fields, left, right, k, p)
            wide[k, p, 0:TOP] = nothing
            wide[k, p, TOP + Y : ROWS] = nothing
            wide[k, p, TOP : TOP + Y] = ref[at]
            wide[k, p, TOP - w : TOP] = below[AT_Y[k] + w * n : AT_Y[k] + w * (n + 1)]
            wide[k, p, TOP + Y : TOP + Y + w] = above[AT_Y[k] + w * n : AT_Y[k] + w * (n + 1)]
    for q in range(PER_GROUP):
        out = jnp.zeros((ROWS, Z), F32)
        for g in range(GROUPS):
            p = PER_GROUP * g + q
            for k, w in enumerate(WIDTHS):
                if p in planes_of(k):
                    base = STRIDE * g + BASES[k]
                    here = (lane >= base - w) & (lane < base + w)
                    out = jnp.where(here, pltpu.roll(wide[k, p], base, 1), out)
        packed[q] = out


def shifts_of(table):
    values = [jnp.full((8, Z), table[n], F32) for n in range(table.shape[0])]
    least, most, mean = values[0], values[0], values[0]
    for v in values[1:]:
        least, most, mean = jnp.minimum(least, v), jnp.maximum(most, v), mean + v
    mean = mean * (1.0 / len(values))
    top = 4.0 + 16.0 * most + 16.0 * mean
    low = 2.0 + 8.0 * least + 8.0 * mean
    middle, half = 0.5 * (top + low), 0.5 * (top - low)
    return [
        (middle + half * c) * (1.0 / SCALE) for c in (0.9238795, -0.9238795, 0.3826834, -0.3826834)
    ]


def krylov(wide, from_left, from_right, table, basis, dots, ends, fore, fore_c, back, back_c, diag, mid):
    lane = lax.broadcasted_iota(jnp.int32, (ROWS, Z), 1)

    for q in range(PER_GROUP):
        left = lane < 0
        for g in range(GROUPS):
            for k, w in enumerate(WIDTHS):
                base = STRIDE * g + BASES[k]
                left = left | ((lane >= base - w) & (lane < base))
        both = jnp.where(left, from_left[q], from_right[q])
        for g in range(GROUPS):
            p = PER_GROUP * g + q
            for k, w in enumerate(WIDTHS):
                if p in planes_of(k):
                    turned = pltpu.roll(both, (Z - STRIDE * g - BASES[k]) % Z, 1)
                    ends[k, p] = jnp.where((lane < w) | (lane >= Z - w), turned, 0.0)

    def field(k, side, p):
        return wide[k, p] if side == 0 else ends[k, p]

    def smooth(get, slot, p, first, count, sides):
        summed = []
        for side in (0, 1):
            mid[slot, side, pl.ds(8, ROWS)] = get(side, p) + 0.5 * (get(side, p - 1) + get(side, p + 1))
        for side in (0, 1):
            ref = mid.at[slot, side]
            centre = ref[pl.ds(8 + first, count)]
            summed.append(
                centre + 0.5 * (ref[pl.ds(7 + first, count)] + ref[pl.ds(9 + first, count)])
            )
        up = [pltpu.roll(a, 1, 1) for a in summed]
        down = [pltpu.roll(a, Z - 1, 1) for a in summed]
        at = lane[:count]
        out = []
        for side in range(sides):
            lower = jnp.where(at == 0, up[1 - side], up[side])
            upper = jnp.where(at == Z - 1, down[1 - side], down[side])
            out.append(summed[side] + 0.5 * (lower + upper))
        return out

    for p in range(PLANES):
        for side in (0, 1):
            back_c[side, p] = field(0, side, p) * field(1, side, p)
    slots = mid.shape[0]
    slot = 0
    for p in range(1, PLANES - 1):
        tc = smooth(lambda s, n: field(0, s, n), slot % slots, p, 0, ROWS, 2)
        tx = smooth(lambda s, n: field(1, s, n), (slot + 1) % slots, p, 0, ROWS, 2)
        tcx = smooth(lambda s, n: back_c[s, n], (slot + 2) % slots, p, 0, ROWS, 2)
        slot += 3
        for side in (0, 1):
            c = field(0, side, p)
            near = 16.0 * c + 2.0 * tc[side]
            if p in planes_of(3):
                diag[side, p] = (1.0 + 6.0 * field(3, side, p) + near) * (1.0 / SCALE)
            r = field(2, side, p) - near * field(1, side, p) + 2.0 * (c * tx[side] + tcx[side])
            r = jnp.where(c > 0.0, r, 0.0)
            fore[side, p] = r
            fore_c[side, p] = r * (c * (2.0 / SCALE))
            if side == 0 and HALO <= p < HALO + X:
                basis[0, p - HALO] = r[TOP : TOP + Y]

    theta = shifts_of(table)
    for k in range(ITERS):
        old, old_c, new, new_c = (
            (fore, fore_c, back, back_c) if k % 2 == 0 else (back, back_c, fore, fore_c)
        )
        last = k + 1 == ITERS
        first, count, sides = (TOP, Y, 1) if last else (0, ROWS, 2)
        turn = jnp.tile(theta[k], (count // 8, 1))
        for p in range(2 + k, PLANES - 2 - k):
            tv = smooth(lambda s, n: old[s, n], slot % slots, p, first, count, sides)
            tu = smooth(lambda s, n: old_c[s, n], (slot + 1) % slots, p, first, count, sides)
            slot += 2
            for side in range(sides):
                rows = pl.ds(first, count)
                c = (wide if side == 0 else ends)[0, p, rows]
                half_c = c * (2.0 / SCALE)
                v = (diag[side, p, rows] - turn) * old[side, p, rows] - (half_c * tv[side] + tu[side])
                v = jnp.where(c > 0.0, v, 0.0)
                if not last:
                    new[side, p] = v
                    new_c[side, p] = v * half_c
                if side == 0 and HALO <= p < HALO + X:
                    basis[k + 1, p - HALO] = v if last else v[TOP : TOP + Y]

    sums = []
    for i, j in PAIRS:
        total = None
        for p in range(X):
            for half in (0, 8):
                term = basis[i, p, half : half + 8] * basis[j, p, half : half + 8]
                total = term if total is None else total + term
        sums.append(total)
    sums += [jnp.zeros((8, Z), F32)] * (16 - len(sums))
    at = lane[:8]
    step = 64
    while len(sums) > 1:
        half = len(sums) // 2
        low = (at // step) % 2 == 0
        sums = [
            jnp.where(low, a, b) + jnp.where(low, pltpu.roll(a, Z - step, 1), pltpu.roll(b, step, 1))
            for a, b in zip(sums[:half], sums[half:])
        ]
        step //= 2
    (total,) = sums
    for by in (4, 2, 1):
        turned = jnp.where((at & by) == 0, pltpu.roll(total, Z - by, 1), pltpu.roll(total, by, 1))
        total = total + turned
    for by in (4, 2, 1):
        total = total + pltpu.roll(total, by, 0)
    for n in range(dots.shape[0]):
        dots[n] = total[0:1]


def lane_of(n):
    return sum(((n >> (3 - b)) & 1) * (64 >> b) for b in range(4))


def two_sum(a, b):
    s = a + b
    t = s - a
    return s, (a - (s - t)) + (b - t)


def row_sum(parts):
    rows = [(parts[n], None) for n in range(parts.shape[0])]
    while len(rows) > 1:
        pairs, rows = zip(rows[::2], rows[1::2]), []
        for (a, ea), (b, eb) in pairs:
            s, e = two_sum(a, b)
            rows.append((s, e if ea is None else e + (ea + eb)))
    return rows[0]


def relay(parts, copies):
    total, rest = row_sum(parts)
    lane = lax.broadcasted_iota(jnp.int32, total.shape, 1)
    total = jnp.where((lane & 4) == 0, total, rest)
    for n in range(copies.shape[0]):
        copies[n] = total


def quick(a, b):
    s = a + b
    return s, b - (s - a)


def halves(a):
    t = 4097.0 * a
    high = t - (t - a)
    return high, a - high


def plus(a, b):
    s, e = two_sum(a[0], b[0])
    return quick(s, e + (a[1] + b[1]))


def minus(a, b):
    return plus(a, (-b[0], -b[1]))


def times(a, b):
    p = a[0] * b[0]
    ah, al = halves(a[0])
    bh, bl = halves(b[0])
    e = ((ah * bh - p) + ah * bl + al * bh) + al * bl
    return quick(p, e + (a[0] * b[1] + a[1] * b[0]))


def over(a, b):
    q = a[0] / b[0]
    none = jnp.zeros_like(q)
    rest = minus(a, times((q, none), b))
    return quick(q, rest[0] / b[0])


def conjugate_gradients(gram, theta):
    none = jnp.zeros_like(theta[0])
    zero, one = (none, none), (none + 1.0, none)
    shift = [(t, none) for t in theta]

    def along(k, vector):
        total = times(gram[k, 0], vector[0])
        for j in range(1, len(vector)):
            total = plus(total, times(gram[k, j], vector[j]))
        return total

    r, p = [one], [one]
    y = [zero] * ITERS
    rr = gram[0, 0]
    for k in range(ITERS):
        image = [times(shift[i], p[i]) for i in range(k + 1)] + [zero]
        image = [image[0]] + [plus(image[i], p[i - 1]) for i in range(1, k + 2)]
        step = over(rr, times(p[k], along(k, image)))
        y = [plus(y[i], times(step, p[i])) if i <= k else y[i] for i in range(ITERS)]
        r = [minus(r[i] if i <= k else zero, times(step, image[i])) for i in range(k + 2)]
        if k + 1 < ITERS:
            new = times(r[k + 1], along(k + 1, r))
            ratio = over(new, rr)
            p = [plus(r[i], times(ratio, p[i])) if i <= k else r[i] for i in range(k + 2)]
            rr = new
    return [a[0] * (1.0 / SCALE) for a in y], [a[0] for a in r]


def finish(parts, basis, opening, table, closing, mismatch):
    total, rest = row_sum(parts)
    rest = rest + pltpu.roll(total, Z - 4, 1)
    gram = {}
    for n, (i, j) in enumerate(PAIRS):
        at = lane_of(n)
        gram[i, j] = gram[j, i] = quick(
            *(jnp.broadcast_to(v[0:1, at : at + 1], (8, Z)) for v in (total, rest))
        )
    y, r = conjugate_gradients(gram, shifts_of(table))
    for p in range(X):
        for half in (0, 8):
            rows = pl.ds(half, 8)
            v = [basis[k, p, rows] for k in range(ITERS + 1)]
            x, m = opening[p, rows], r[ITERS] * v[ITERS]
            for k in range(ITERS):
                x, m = x + y[k] * v[k], m + r[k] * v[k]
            closing[p, rows] = x
            mismatch[p, rows] = m


def both_ways(low, high, axis):
    ends = lax.axis_size(axis) - 1
    from_below = lax.ppermute(high, axis, [(i, i + 1) for i in range(ends)])
    from_above = lax.ppermute(low, axis, [(i + 1, i) for i in range(ends)])
    return from_below, from_above


def exchange(copies, axes):
    return lax.all_to_all(copies, axes, split_axis=0, concat_axis=0, tiled=True)


def body(opening, source, category, table, flags):
    brick = (X, Y, Z)
    fields, low, high = call(
        prepare, [VMEM] * 4 + [SMEM], [(4, *brick), (SLAB_X, Y, Z), (SLAB_X, Y, Z)]
    )(opening, source, category, flags, table)
    left, right = both_ways(low, high, "gx")
    low, high = call(slabs_y, [VMEM] * 3, [(SLAB_Y, Z)] * 2)(fields, left, right)
    below, above = both_ways(low, high, "gy")
    wide, packed = call(
        assemble, [VMEM] * 5, [(4, PLANES, ROWS, Z), (PER_GROUP, ROWS, Z)]
    )(fields, left, right, below, above)
    from_left, from_right = both_ways(packed, packed, GZ)
    first, second = ("gx", "gz_1"), ("gy", "gz_0")
    sided = (2, PLANES, ROWS, Z)
    basis, dots = call(
        krylov,
        [VMEM] * 3 + [SMEM],
        [(ITERS + 1, *brick), (lax.axis_size(first), 1, Z)],
        [(4, PLANES, ROWS, Z)] + [sided] * 5 + [(6, 2, ROWS + 16, Z)],
        flops=20000000,
        vmem=16,
    )(wide, from_left, from_right, table)
    parts = exchange(dots, first)
    (copies,) = call(relay, [VMEM], [(lax.axis_size(second), 1, Z)])(parts)
    parts = exchange(copies, second)
    closing, mismatch = call(finish, [VMEM] * 3 + [SMEM], [brick, brick])(
        parts, basis, opening, table
    )
    return closing, mismatch


def solution(mesh):
    shape = mesh.devices.shape
    split = Mesh(mesh.devices.reshape(shape[0], shape[1], shape[2] // 2, 2), ("gx", "gy", *GZ))
    spec = P("gx", "gy", GZ)
    return jax.shard_map(
        body, mesh=split, in_specs=(spec, spec, spec, P(), spec), out_specs=(spec, spec), check_vma=False
    )
```

```python
import jax
import jax.numpy as jnp
from jax import lax
from jax.experimental import pallas as pl
from jax.experimental.pallas import tpu as pltpu
from jax.sharding import Mesh
from jax.sharding import PartitionSpec as P

ITERS = 4
GZ = ("gz_0", "gz_1")
F32 = jnp.float32
X, Y, Z = 8, 16, 128
HALO = ITERS + 1
WIDTHS = (5, 5, 4, 3)
PLANES = X + 2 * HALO
ROWS = 32
TOP = 8
SLAB_X = sum(WIDTHS)
AT_X = (0, 5, 10, 14)
AT_Y = (0, 90, 180, 244)
SLAB_Y = 288
GROUPS, PER_GROUP, STRIDE = 3, 6, 40
BASES = (5, 15, 24, 31)
SCALE = 64.0
PAIRS = [(i, j) for i in range(ITERS) for j in range(i, ITERS + 1)]
VMEM = pl.BlockSpec(memory_space=pltpu.VMEM)
HBM = pl.BlockSpec(memory_space=pltpu.HBM)
SMEM = pl.BlockSpec(memory_space=pltpu.SMEM)


def planes_of(k):
    return range(HALO - WIDTHS[k], PLANES - HALO + WIDTHS[k])


def call(kernel, ins, outs, scratch=(), flops=100000, vmem=8):
    return pl.pallas_call(
        kernel,
        in_specs=ins,
        out_specs=[VMEM] * len(outs),
        out_shape=[jax.ShapeDtypeStruct(s, F32) for s in outs],
        scratch_shapes=[pltpu.VMEM(s, F32) if isinstance(s, tuple) else s for s in scratch],
        compiler_params=pltpu.CompilerParams(vmem_limit_bytes=vmem * 2**20),
        cost_estimate=pl.CostEstimate(flops=flops, bytes_accessed=1000000, transcendentals=0),
    )


def prepare(
    opening_at, source_at, category_at, flags_at, table_at, fields, low, high, theta,
    opening, source, category, flags, table, arrived,
):
    copies = [
        pltpu.make_async_copy(a, b, arrived.at[n])
        for n, (a, b) in enumerate(
            (
                (table_at, table),
                (category_at, category),
                (flags_at, flags),
                (opening_at, opening),
                (source_at, source),
            )
        )
    ]
    for copy in copies:
        copy.start()
    for copy in copies:
        copy.wait()
    for k, shift in enumerate(shifts_of(table)):
        theta[k] = shift
    for p in range(X):
        kind = category[p]
        cond = jnp.full((Y, Z), table[0], F32)
        for n in range(1, table.shape[0]):
            cond = jnp.where(kind == n, table[n], cond)
        flag = flags[p].astype(F32)
        start = opening[p]
        values = (cond, start, 2.0 * source[p] - 6.0 * flag * start, flag)
        for k, v in enumerate(values):
            fields[k, p] = v
            if p < WIDTHS[k]:
                low[AT_X[k] + p] = v
            if p >= X - WIDTHS[k]:
                high[AT_X[k] + p - (X - WIDTHS[k])] = v


def plane(fields, left, right, k, p):
    if p < HALO:
        return left, (AT_X[k] + p - (HALO - WIDTHS[k]),)
    if p < HALO + X:
        return fields, (k, p - HALO)
    return right, (AT_X[k] + p - HALO - X,)


def slabs_y(fields, left, right, low, high):
    for k, w in enumerate(WIDTHS):
        for n, p in enumerate(planes_of(k)):
            ref, at = plane(fields, left, right, k, p)
            to = pl.ds(AT_Y[k] + w * n, w)
            low[to] = ref[(*at, pl.ds(0, w))]
            high[to] = ref[(*at, pl.ds(Y - w, w))]


def assemble(fields, left, right, below, above, wide, packed):
    lane = lax.broadcasted_iota(jnp.int32, (ROWS, Z), 1)
    nothing = jnp.zeros((8, Z), F32)
    for k, w in enumerate(WIDTHS):
        for n, p in enumerate(planes_of(k)):
            ref, at = plane(fields, left, right, k, p)
            wide[k, p, 0:TOP] = nothing
            wide[k, p, TOP + Y : ROWS] = nothing
            wide[k, p, TOP : TOP + Y] = ref[at]
            wide[k, p, TOP - w : TOP] = below[AT_Y[k] + w * n : AT_Y[k] + w * (n + 1)]
            wide[k, p, TOP + Y : TOP + Y + w] = above[AT_Y[k] + w * n : AT_Y[k] + w * (n + 1)]
    for q in range(PER_GROUP):
        out = jnp.zeros((ROWS, Z), F32)
        for g in range(GROUPS):
            p = PER_GROUP * g + q
            for k, w in enumerate(WIDTHS):
                if p in planes_of(k):
                    base = STRIDE * g + BASES[k]
                    here = (lane >= base - w) & (lane < base + w)
                    out = jnp.where(here, pltpu.roll(wide[k, p], base, 1), out)
        packed[q] = out


def shifts_of(table):
    values = [jnp.full((8, Z), table[n], F32) for n in range(table.shape[0])]
    least, most, mean = values[0], values[0], values[0]
    for v in values[1:]:
        least, most, mean = jnp.minimum(least, v), jnp.maximum(most, v), mean + v
    mean = mean * (1.0 / len(values))
    top = 4.0 + 16.0 * most + 16.0 * mean
    low = 2.0 + 8.0 * least + 8.0 * mean
    middle, half = 0.5 * (top + low), 0.5 * (top - low)
    return [
        (middle + half * c) * (1.0 / SCALE) for c in (0.9238795, -0.9238795, 0.3826834, -0.3826834)
    ]


def krylov(core, wide, far, chip, theta, basis, dots, ends, fore, fore_c, back, back_c, diag, mid):
    lane = lax.broadcasted_iota(jnp.int32, (ROWS, Z), 1)
    first_core = core[0] == 0
    partner = 1 - core[0]

    for q in range(PER_GROUP):
        left = lane < 0
        for g in range(GROUPS):
            for k, w in enumerate(WIDTHS):
                base = STRIDE * g + BASES[k]
                left = left | ((lane >= base - w) & (lane < base))
        other, near = far[q], chip[partner, q]
        both = jnp.where(jnp.logical_xor(left, first_core), near, other)
        for g in range(GROUPS):
            p = PER_GROUP * g + q
            for k, w in enumerate(WIDTHS):
                if p in planes_of(k):
                    turned = pltpu.roll(both, (Z - STRIDE * g - BASES[k]) % Z, 1)
                    ends[k, p] = jnp.where((lane < w) | (lane >= Z - w), turned, 0.0)

    def field(k, side, p):
        return wide[k, p] if side == 0 else ends[k, p]

    def smooth(get, slot, p, first, count, sides):
        summed = []
        for side in (0, 1):
            mid[slot, side, pl.ds(8, ROWS)] = get(side, p) + 0.5 * (get(side, p - 1) + get(side, p + 1))
        for side in (0, 1):
            ref = mid.at[slot, side]
            centre = ref[pl.ds(8 + first, count)]
            summed.append(
                centre + 0.5 * (ref[pl.ds(7 + first, count)] + ref[pl.ds(9 + first, count)])
            )
        up = [pltpu.roll(a, 1, 1) for a in summed]
        down = [pltpu.roll(a, Z - 1, 1) for a in summed]
        at = lane[:count]
        out = []
        for side in range(sides):
            lower = jnp.where(at == 0, up[1 - side], up[side])
            upper = jnp.where(at == Z - 1, down[1 - side], down[side])
            out.append(summed[side] + 0.5 * (lower + upper))
        return out

    for p in range(PLANES):
        for side in (0, 1):
            back_c[side, p] = field(0, side, p) * field(1, side, p)
    slots = mid.shape[0]
    slot = 0
    for p in range(1, PLANES - 1):
        tc = smooth(lambda s, n: field(0, s, n), slot % slots, p, 0, ROWS, 2)
        tx = smooth(lambda s, n: field(1, s, n), (slot + 1) % slots, p, 0, ROWS, 2)
        tcx = smooth(lambda s, n: back_c[s, n], (slot + 2) % slots, p, 0, ROWS, 2)
        slot += 3
        for side in (0, 1):
            c = field(0, side, p)
            near = 16.0 * c + 2.0 * tc[side]
            if p in planes_of(3):
                diag[side, p] = (1.0 + 6.0 * field(3, side, p) + near) * (1.0 / SCALE)
            r = field(2, side, p) - near * field(1, side, p) + 2.0 * (c * tx[side] + tcx[side])
            r = jnp.where(c > 0.0, r, 0.0)
            fore[side, p] = r
            fore_c[side, p] = r * (c * (2.0 / SCALE))
            if side == 0 and HALO <= p < HALO + X:
                basis[0, p - HALO] = r[TOP : TOP + Y]

    for k in range(ITERS):
        old, old_c, new, new_c = (
            (fore, fore_c, back, back_c) if k % 2 == 0 else (back, back_c, fore, fore_c)
        )
        last = k + 1 == ITERS
        first, count, sides = (TOP, Y, 1) if last else (0, ROWS, 2)
        turn = jnp.tile(theta[k], (count // 8, 1))
        for p in range(2 + k, PLANES - 2 - k):
            tv = smooth(lambda s, n: old[s, n], slot % slots, p, first, count, sides)
            tu = smooth(lambda s, n: old_c[s, n], (slot + 1) % slots, p, first, count, sides)
            slot += 2
            for side in range(sides):
                rows = pl.ds(first, count)
                c = (wide if side == 0 else ends)[0, p, rows]
                half_c = c * (2.0 / SCALE)
                v = (diag[side, p, rows] - turn) * old[side, p, rows] - (half_c * tv[side] + tu[side])
                v = jnp.where(c > 0.0, v, 0.0)
                if not last:
                    new[side, p] = v
                    new_c[side, p] = v * half_c
                if side == 0 and HALO <= p < HALO + X:
                    basis[k + 1, p - HALO] = v if last else v[TOP : TOP + Y]

    sums = []
    for i, j in PAIRS:
        total = None
        for p in range(X):
            for half in (0, 8):
                term = basis[i, p, half : half + 8] * basis[j, p, half : half + 8]
                total = term if total is None else total + term
        sums.append(total)
    sums += [jnp.zeros((8, Z), F32)] * (16 - len(sums))
    at = lane[:8]
    step = 64
    while len(sums) > 1:
        half = len(sums) // 2
        low = (at // step) % 2 == 0
        sums = [
            jnp.where(low, a, b) + jnp.where(low, pltpu.roll(a, Z - step, 1), pltpu.roll(b, step, 1))
            for a, b in zip(sums[:half], sums[half:])
        ]
        step //= 2
    (total,) = sums
    for by in (4, 2, 1):
        turned = jnp.where((at & by) == 0, pltpu.roll(total, Z - by, 1), pltpu.roll(total, by, 1))
        total = total + turned
    for by in (4, 2, 1):
        total = total + pltpu.roll(total, by, 0)
    for n in range(dots.shape[0]):
        dots[n] = total[0:1]


def lane_of(n):
    return sum(((n >> (3 - b)) & 1) * (64 >> b) for b in range(4))


def two_sum(a, b):
    s = a + b
    t = s - a
    return s, (a - (s - t)) + (b - t)


def row_sum(parts):
    rows = [(parts[n], None) for n in range(parts.shape[0])]
    while len(rows) > 1:
        pairs, rows = zip(rows[::2], rows[1::2]), []
        for (a, ea), (b, eb) in pairs:
            s, e = two_sum(a, b)
            rows.append((s, e if ea is None else e + (ea + eb)))
    return rows[0]


def relay(parts, copies):
    total, rest = row_sum(parts)
    lane = lax.broadcasted_iota(jnp.int32, total.shape, 1)
    total = jnp.where((lane & 4) == 0, total, rest)
    for n in range(copies.shape[0]):
        copies[n] = total


def quick(a, b):
    s = a + b
    return s, b - (s - a)


def halves(a):
    t = 4097.0 * a
    high = t - (t - a)
    return high, a - high


def plus(a, b):
    s, e = two_sum(a[0], b[0])
    return quick(s, e + (a[1] + b[1]))


def minus(a, b):
    return plus(a, (-b[0], -b[1]))


def times(a, b):
    p = a[0] * b[0]
    ah, al = halves(a[0])
    bh, bl = halves(b[0])
    e = ((ah * bh - p) + ah * bl + al * bh) + al * bl
    return quick(p, e + (a[0] * b[1] + a[1] * b[0]))


def over(a, b):
    q = a[0] / b[0]
    none = jnp.zeros_like(q)
    rest = minus(a, times((q, none), b))
    return quick(q, rest[0] / b[0])


def conjugate_gradients(gram, theta):
    none = jnp.zeros_like(theta[0])
    zero, one = (none, none), (none + 1.0, none)
    shift = [(t, none) for t in theta]

    def along(k, vector):
        total = times(gram[k, 0], vector[0])
        for j in range(1, len(vector)):
            total = plus(total, times(gram[k, j], vector[j]))
        return total

    r, p = [one], [one]
    y = [zero] * ITERS
    rr = gram[0, 0]
    for k in range(ITERS):
        image = [times(shift[i], p[i]) for i in range(k + 1)] + [zero]
        image = [image[0]] + [plus(image[i], p[i - 1]) for i in range(1, k + 2)]
        step = over(rr, times(p[k], along(k, image)))
        y = [plus(y[i], times(step, p[i])) if i <= k else y[i] for i in range(ITERS)]
        r = [minus(r[i] if i <= k else zero, times(step, image[i])) for i in range(k + 2)]
        if k + 1 < ITERS:
            new = times(r[k + 1], along(k + 1, r))
            ratio = over(new, rr)
            p = [plus(r[i], times(ratio, p[i])) if i <= k else r[i] for i in range(k + 2)]
            rr = new
    return [a[0] * (1.0 / SCALE) for a in y], [a[0] for a in r]


def finish(parts, basis, fields, theta, closing, mismatch):
    total, rest = row_sum(parts)
    rest = rest + pltpu.roll(total, Z - 4, 1)
    gram = {}
    for n, (i, j) in enumerate(PAIRS):
        at = lane_of(n)
        gram[i, j] = gram[j, i] = quick(
            *(jnp.broadcast_to(v[0:1, at : at + 1], (8, Z)) for v in (total, rest))
        )
    y, r = conjugate_gradients(gram, [theta[k] for k in range(ITERS)])
    for p in range(X):
        for half in (0, 8):
            rows = pl.ds(half, 8)
            v = [basis[k, p, rows] for k in range(ITERS + 1)]
            x, m = fields[1, p, rows], r[ITERS] * v[ITERS]
            for k in range(ITERS):
                x, m = x + y[k] * v[k], m + r[k] * v[k]
            closing[p, rows] = x
            mismatch[p, rows] = m


def both_ways(low, high, axis):
    ends = lax.axis_size(axis) - 1
    from_below = lax.ppermute(high, axis, [(i, i + 1) for i in range(ends)])
    from_above = lax.ppermute(low, axis, [(i + 1, i) for i in range(ends)])
    return from_below, from_above


def exchange(copies, axes):
    return lax.all_to_all(copies, axes, split_axis=0, concat_axis=0, tiled=True)


def body(opening, source, category, table, flags):
    brick = (X, Y, Z)
    whole = pltpu.VMEM(brick, jnp.int32)
    fields, low, high, theta = call(
        prepare,
        [HBM] * 5,
        [(4, *brick), (SLAB_X, Y, Z), (SLAB_X, Y, Z), (ITERS, 8, Z)],
        [brick, brick, whole, whole, pltpu.SMEM(table.shape, F32), pltpu.SemaphoreType.DMA((5,))],
    )(*(pltpu.with_memory_space_constraint(a, pltpu.HBM) for a in (opening, source, category, flags, table)))
    left, right = both_ways(low, high, "gx")
    low, high = call(slabs_y, [VMEM] * 3, [(SLAB_Y, Z)] * 2)(fields, left, right)
    below, above = both_ways(low, high, "gy")
    wide, packed = call(
        assemble, [VMEM] * 5, [(4, PLANES, ROWS, Z), (PER_GROUP, ROWS, Z)]
    )(fields, left, right, below, above)
    far = lax.ppermute(
        packed,
        GZ,
        [p for i in range(1, lax.axis_size(GZ) - 1, 2) for p in ((i, i + 1), (i + 1, i))],
    )
    chip = lax.all_gather(packed, GZ[1], axis=0)
    core = lax.axis_index(GZ[1]).reshape(1)
    first, second = ("gx", "gz_1"), ("gy", "gz_0")
    sided = (2, PLANES, ROWS, Z)
    basis, dots = call(
        krylov,
        [SMEM] + [VMEM] * 4,
        [(ITERS + 1, *brick), (lax.axis_size(first), 1, Z)],
        [(4, PLANES, ROWS, Z)] + [sided] * 5 + [(6, 2, ROWS + 16, Z)],
        flops=20000000,
        vmem=16,
    )(core, wide, far, chip, theta)
    parts = exchange(dots, first)
    (copies,) = call(relay, [VMEM], [(lax.axis_size(second), 1, Z)])(parts)
    parts = exchange(copies, second)
    closing, mismatch = call(finish, [VMEM] * 4, [brick, brick])(
        parts, basis, fields, theta
    )
    return closing, mismatch


def solution(mesh):
    shape = mesh.devices.shape
    split = Mesh(mesh.devices.reshape(shape[0], shape[1], shape[2] // 2, 2), ("gx", "gy", *GZ))
    spec = P("gx", "gy", GZ)
    return jax.shard_map(
        body, mesh=split, in_specs=(spec, spec, spec, P(), spec), out_specs=(spec, spec), check_vma=False
    )
```

```python
import jax
import jax.numpy as jnp
from jax import lax
from jax.experimental import pallas as pl
from jax.experimental.pallas import tpu as pltpu
from jax.sharding import Mesh
from jax.sharding import PartitionSpec as P

ITERS = 4
GZ = ("gz_0", "gz_1")
F32 = jnp.float32
X, Y, Z = 8, 16, 128
HALO = ITERS + 1
WIDTHS = (5, 5, 4, 3)
PLANES = X + 2 * HALO
ROWS = 32
TOP = 8
SLAB_X = sum(WIDTHS)
AT_X = (0, 5, 10, 14)
AT_Y = (0, 90, 180, 244)
SLAB_Y = 288
GROUPS, PER_GROUP, GROUP = 4, 5, 32
LOW_AT, HIGH_AT = 5, 26
SCALE = 64.0
PAIRS = [(i, j) for i in range(ITERS) for j in range(i, ITERS + 1)]
VMEM = pl.BlockSpec(memory_space=pltpu.VMEM)
HBM = pl.BlockSpec(memory_space=pltpu.HBM)
SMEM = pl.BlockSpec(memory_space=pltpu.SMEM)


def planes_of(k):
    return range(HALO - WIDTHS[k], PLANES - HALO + WIDTHS[k])


def call(kernel, ins, outs, scratch=(), flops=100000, vmem=8):
    return pl.pallas_call(
        kernel,
        in_specs=ins,
        out_specs=[VMEM] * len(outs),
        out_shape=[jax.ShapeDtypeStruct(s, F32) for s in outs],
        scratch_shapes=[pltpu.VMEM(s, F32) if isinstance(s, tuple) else s for s in scratch],
        compiler_params=pltpu.CompilerParams(vmem_limit_bytes=vmem * 2**20),
        cost_estimate=pl.CostEstimate(flops=flops, bytes_accessed=1000000, transcendentals=0),
    )


def prepare(
    opening_at, source_at, category_at, flags_at, table_at, fields, low, high, theta,
    opening, source, category, flags, table, arrived,
):
    copies = [
        pltpu.make_async_copy(a, b, arrived.at[n])
        for n, (a, b) in enumerate(
            (
                (table_at, table),
                (category_at, category),
                (flags_at, flags),
                (opening_at, opening),
                (source_at, source),
            )
        )
    ]
    for copy in copies:
        copy.start()
    for copy in copies:
        copy.wait()
    for k, shift in enumerate(shifts_of(table)):
        theta[k] = shift
    for p in range(X):
        kind = category[p]
        cond = jnp.full((Y, Z), table[0], F32)
        for n in range(1, table.shape[0]):
            cond = jnp.where(kind == n, table[n], cond)
        flag = flags[p].astype(F32)
        start = opening[p]
        values = (cond, start, 2.0 * source[p] - 6.0 * flag * start, flag)
        for k, v in enumerate(values):
            fields[k, p] = v
            if p < WIDTHS[k]:
                low[AT_X[k] + p] = v
            if p >= X - WIDTHS[k]:
                high[AT_X[k] + p - (X - WIDTHS[k])] = v


def plane(fields, left, right, k, p):
    if p < HALO:
        return left, (AT_X[k] + p - (HALO - WIDTHS[k]),)
    if p < HALO + X:
        return fields, (k, p - HALO)
    return right, (AT_X[k] + p - HALO - X,)


def slabs_y(fields, left, right, low, high):
    for k, w in enumerate(WIDTHS):
        for n, p in enumerate(planes_of(k)):
            ref, at = plane(fields, left, right, k, p)
            to = pl.ds(AT_Y[k] + w * n, w)
            low[to] = ref[(*at, pl.ds(0, w))]
            high[to] = ref[(*at, pl.ds(Y - w, w))]


def assemble(core, fields, left, right, below, above, wide, near, far):
    lane = lax.broadcasted_iota(jnp.int32, (ROWS, Z), 1)
    first_core = core[0] == 0
    nothing = jnp.zeros((8, Z), F32)
    for k, w in enumerate(WIDTHS):
        for n, p in enumerate(planes_of(k)):
            ref, at = plane(fields, left, right, k, p)
            wide[k, p, 0:TOP] = nothing
            wide[k, p, TOP + Y : ROWS] = nothing
            wide[k, p, TOP : TOP + Y] = ref[at]
            wide[k, p, TOP - w : TOP] = below[AT_Y[k] + w * n : AT_Y[k] + w * (n + 1)]
            wide[k, p, TOP + Y : TOP + Y + w] = above[AT_Y[k] + w * n : AT_Y[k] + w * (n + 1)]
    for q in range(PER_GROUP):
        low = jnp.zeros((ROWS, Z), F32)
        high = low
        for g in range(GROUPS):
            p = PER_GROUP * g + q
            for k, w in enumerate(WIDTHS):
                if p in planes_of(k):
                    base = GROUP * g + AT_X[k]
                    turned = pltpu.roll(wide[k, p], base, 1)
                    place = lane if base else jnp.where(lane < Z // 2, lane, lane - Z)
                    low = jnp.where((place >= base) & (place < base + w), turned, low)
                    high = jnp.where((place >= base - w) & (place < base), turned, high)
        far[q] = jnp.where(first_core, low, high)
        near[q] = jnp.where(first_core, high, low)


def shifts_of(table):
    values = [jnp.full((8, Z), table[n], F32) for n in range(table.shape[0])]
    least, most, mean = values[0], values[0], values[0]
    for v in values[1:]:
        least, most, mean = jnp.minimum(least, v), jnp.maximum(most, v), mean + v
    mean = mean * (1.0 / len(values))
    top = 4.0 + 16.0 * most + 16.0 * mean
    low = 2.0 + 8.0 * least + 8.0 * mean
    middle, half = 0.5 * (top + low), 0.5 * (top - low)
    return [
        (middle + half * c) * (1.0 / SCALE) for c in (0.9238795, -0.9238795, 0.3826834, -0.3826834)
    ]


def smooth_y(mid, first, count):
    sides = mid[pl.ds(7 + first, count)] + mid[pl.ds(9 + first, count)]
    return mid[pl.ds(8 + first, count)] + 0.5 * sides


def smooth_z(values):
    pairs = values + pltpu.roll(values, Z - 1, 1)
    return pairs + pltpu.roll(pairs, 1, 1)


def newton_step(store, shift, at, v, tv, tu):
    slope, diag, inside = store
    return ((diag[at] - shift) * v - (slope[at] * tv + tu)) * inside[at]


def interior(wide, theta, basis, sums, ends, cx, mid, slope, diag, inside, va, vb, ua, ub):
    lane = lax.broadcasted_iota(jnp.int32, (ROWS, Z), 1)
    slots = mid.shape[0]
    slot = [0]

    def smooth(ref, p, first=0, count=ROWS):
        here = mid.at[slot[0] % slots]
        slot[0] += 1
        middle = ref[p]
        here[pl.ds(8, ROWS)] = (ref[p - 1] + middle) + (middle + ref[p + 1])
        return smooth_z(smooth_y(here, first, count))

    cond, start, rest, flag = (wide.at[k] for k in range(4))
    for p in range(PLANES):
        cx[p] = cond[p] * start[p]
    for p in range(1, PLANES - 1):
        tc, tx, tcx = (smooth(ref, p) for ref in (cond, start, cx))
        c = cond[p]
        near = 16.0 * c + 0.5 * tc
        if p in planes_of(3):
            diag[p] = (1.0 + 6.0 * flag[p] + near) * (1.0 / SCALE)
        slope[p] = c * (0.5 / SCALE)
        inside[p] = jnp.where(c > 0.0, 1.0, 0.0)
        r = (rest[p] - near * start[p] + 0.5 * (c * tx + tcx)) * inside[p]
        va[p] = r
        ua[p] = r * slope[p]
        if HALO <= p < HALO + X:
            basis[0, p - HALO] = r[TOP : TOP + Y]
    for k in range(ITERS):
        v_old, u_old, v_new, u_new = (va, ua, vb, ub) if k % 2 == 0 else (vb, ub, va, ua)
        last = k + 1 == ITERS
        first, count = (TOP, Y) if last else (0, ROWS)
        shift = jnp.tile(theta[k], (count // 8, 1))
        for p in range(2 + k, PLANES - 2 - k):
            tv, tu = smooth(v_old, p, first, count), smooth(u_old, p, first, count)
            at = (p, pl.ds(first, count))
            v = newton_step((slope, diag, inside), shift, at, v_old[at], tv, tu)
            if not last:
                v_new[p] = v
                u_new[p] = v * slope[p]
            if HALO <= p < HALO + X:
                basis[k + 1, p - HALO] = v if last else v[TOP : TOP + Y]

    inner = (lane[:8] >= HALO) & (lane[:8] < Z - HALO)
    for n, (i, j) in enumerate(PAIRS):
        total = None
        for p in range(X):
            for half in (0, 8):
                rows = pl.ds(half, 8)
                term = basis[i, p, rows] * basis[j, p, rows]
                total = term if total is None else total + term
        sums[n] = jnp.where(inner, total, 0.0)

    place = lane % GROUP
    for k in range(4):
        for q in range(PER_GROUP):
            out = jnp.zeros((ROWS, Z), F32)
            for g in range(GROUPS):
                p = PER_GROUP * g + q
                if p in planes_of(k):
                    mine = (lane // GROUP) == g
                    low = pltpu.roll(wide[k, p], GROUP * g + LOW_AT, 1)
                    high = pltpu.roll(wide[k, p], (GROUP * g + HIGH_AT) % Z, 1)
                    low_here = mine & (place >= LOW_AT) & (place < LOW_AT + 2 * HALO)
                    high_here = mine & (place >= HIGH_AT - 2 * HALO) & (place < HIGH_AT)
                    out = jnp.where(low_here, low, jnp.where(high_here, high, out))
            ends[k, q] = out


def edges(core, ends, far, chip, theta, inner_sums, basis, dots, cells, cx, mid, slope, diag, inside, va, vb, ua, ub, stack):
    lane = lax.broadcasted_iota(jnp.int32, (ROWS, Z), 1)
    place = lane % GROUP
    first_core = core[0] == 0
    partner = 1 - core[0]
    slots = mid.shape[0]
    slot = [0]

    for q in range(PER_GROUP):
        near, other = chip[partner, q], far[q]
        below = jnp.where(first_core, other, near)
        above = jnp.where(first_core, near, other)
        for k in range(4):
            low = pltpu.roll(below, (LOW_AT - AT_X[k]) % Z, 1)
            high = pltpu.roll(above, (HIGH_AT - AT_X[k]) % Z, 1)
            out = jnp.where(place < LOW_AT, low, ends[k, q])
            cells[k, q] = jnp.where((place >= HIGH_AT) & (place < HIGH_AT + HALO), high, out)

    def next_group(values, by):
        return pltpu.roll(values, (GROUP * by) % Z, 1)

    def smooth(ref, q, first=0, count=ROWS):
        here = mid.at[slot[0] % slots]
        slot[0] += 1
        before = ref[q - 1] if q else next_group(ref[PER_GROUP - 1], 1)
        after = ref[q + 1] if q + 1 < PER_GROUP else next_group(ref[0], -1)
        middle = ref[q]
        here[pl.ds(8, ROWS)] = (before + middle) + (middle + after)
        return smooth_z(smooth_y(here, first, count))

    cond, start, rest, flag = (cells.at[k] for k in range(4))
    for q in range(PER_GROUP):
        cx[q] = cond[q] * start[q]
    for q in range(PER_GROUP):
        tc, tx, tcx = (smooth(ref, q) for ref in (cond, start, cx))
        c = cond[q]
        near = 16.0 * c + 0.5 * tc
        diag[q] = (1.0 + 6.0 * flag[q] + near) * (1.0 / SCALE)
        slope[q] = c * (0.5 / SCALE)
        inside[q] = jnp.where(c > 0.0, 1.0, 0.0)
        r = (rest[q] - near * start[q] + 0.5 * (c * tx + tcx)) * inside[q]
        va[q] = r
        ua[q] = r * slope[q]
        basis[0, q] = r[TOP : TOP + Y]
    for k in range(ITERS):
        v_old, u_old, v_new, u_new = (va, ua, vb, ub) if k % 2 == 0 else (vb, ub, va, ua)
        last = k + 1 == ITERS
        first, count = (TOP, Y) if last else (0, ROWS)
        shift = jnp.tile(theta[k], (count // 8, 1))
        for q in range(PER_GROUP):
            tv, tu = smooth(v_old, q, first, count), smooth(u_old, q, first, count)
            at = (q, pl.ds(first, count))
            v = newton_step((slope, diag, inside), shift, at, v_old[at], tv, tu)
            if not last:
                v_new[q] = v
                u_new[q] = v * slope[q]
            basis[k + 1, q] = v if last else v[TOP : TOP + Y]

    end_cells = ((place >= LOW_AT) & (place < LOW_AT + HALO)) | ((place >= HIGH_AT - HALO) & (place < HIGH_AT))
    mine = []
    for q in range(PER_GROUP):
        own = [g for g in range(GROUPS) if HALO <= PER_GROUP * g + q < HALO + X]
        at = (lane >= GROUP * own[0]) & (lane < GROUP * (own[-1] + 1))
        mine.append(jnp.where(at & end_cells, 1.0, 0.0)[:8])
    for n in range(16):
        total = None
        if n < len(PAIRS):
            i, j = PAIRS[n]
            total = inner_sums[n]
            for q in range(PER_GROUP):
                for half in (0, 8):
                    rows = pl.ds(half, 8)
                    total = total + (basis[i, q, rows] * mine[q]) * basis[j, q, rows]
        else:
            total = jnp.zeros((8, Z), F32)
        stack[pl.ds(8 * n, 8)] = total
    row = lax.broadcasted_iota(jnp.int32, (Z, Z), 0)
    column = lax.broadcasted_iota(jnp.int32, (Z, Z), 1)
    pick = jnp.where((row // 8 == column % 16) & (column < 32), 1.0, 0.0)
    by_row = lax.dot_general(
        jnp.ones((8, Z), F32), stack[...], (((1,), (1,)), ((), ())),
        precision=lax.Precision.HIGHEST, preferred_element_type=F32,
    )
    total = lax.dot_general(
        by_row, pick, (((1,), (0,)), ((), ())),
        precision=lax.Precision.HIGHEST, preferred_element_type=F32,
    )
    for n in range(dots.shape[0]):
        dots[n] = total[0:1]


def two_sum(a, b):
    s = a + b
    t = s - a
    return s, (a - (s - t)) + (b - t)


def row_sum(parts):
    rows = [(parts[n], None) for n in range(parts.shape[0])]
    while len(rows) > 1:
        pairs, rows = zip(rows[::2], rows[1::2]), []
        for (a, ea), (b, eb) in pairs:
            s, e = two_sum(a, b)
            rows.append((s, e if ea is None else e + (ea + eb)))
    return rows[0]


def relay(parts, copies):
    total, rest = row_sum(parts)
    lane = lax.broadcasted_iota(jnp.int32, total.shape, 1)
    total = jnp.where(lane < 16, total, rest)
    for n in range(copies.shape[0]):
        copies[n] = total


def quick(a, b):
    s = a + b
    return s, b - (s - a)


def halves(a):
    t = 4097.0 * a
    high = t - (t - a)
    return high, a - high


def plus(a, b):
    s, e = two_sum(a[0], b[0])
    return quick(s, e + (a[1] + b[1]))


def minus(a, b):
    return plus(a, (-b[0], -b[1]))


def times(a, b):
    p = a[0] * b[0]
    ah, al = halves(a[0])
    bh, bl = halves(b[0])
    e = ((ah * bh - p) + ah * bl + al * bh) + al * bl
    return quick(p, e + (a[0] * b[1] + a[1] * b[0]))


def over(a, b):
    q = a[0] / b[0]
    none = jnp.zeros_like(q)
    rest = minus(a, times((q, none), b))
    return quick(q, rest[0] / b[0])


def conjugate_gradients(gram, theta):
    none = jnp.zeros_like(theta[0])
    zero, one = (none, none), (none + 1.0, none)
    shift = [(t, none) for t in theta]

    def along(k, vector):
        total = times(gram[k, 0], vector[0])
        for j in range(1, len(vector)):
            total = plus(total, times(gram[k, j], vector[j]))
        return total

    r, p = [one], [one]
    y = [zero] * ITERS
    rr = gram[0, 0]
    for k in range(ITERS):
        image = [times(shift[i], p[i]) for i in range(k + 1)] + [zero]
        image = [image[0]] + [plus(image[i], p[i - 1]) for i in range(1, k + 2)]
        step = over(rr, times(p[k], along(k, image)))
        y = [plus(y[i], times(step, p[i])) if i <= k else y[i] for i in range(ITERS)]
        r = [minus(r[i] if i <= k else zero, times(step, image[i])) for i in range(k + 2)]
        if k + 1 < ITERS:
            new = times(r[k + 1], along(k + 1, r))
            ratio = over(new, rr)
            p = [plus(r[i], times(ratio, p[i])) if i <= k else r[i] for i in range(k + 2)]
            rr = new
    return [a[0] * (1.0 / SCALE) for a in y], [a[0] for a in r]


def finish(parts, basis, end_basis, fields, theta, closing, mismatch):
    total, rest = row_sum(parts)
    rest = rest + pltpu.roll(total, Z - 16, 1)
    gram = {}
    for n, (i, j) in enumerate(PAIRS):
        gram[i, j] = gram[j, i] = quick(
            *(jnp.broadcast_to(v[0:1, n : n + 1], (8, Z)) for v in (total, rest))
        )
    y, r = conjugate_gradients(gram, [theta[k] for k in range(ITERS)])

    def combine(v):
        x, m = y[0] * v[0], r[ITERS] * v[ITERS]
        for k in range(1, ITERS):
            x = x + y[k] * v[k]
        for k in range(ITERS):
            m = m + r[k] * v[k]
        return x, m

    lane = lax.broadcasted_iota(jnp.int32, (8, Z), 1)
    for half in (0, 8):
        rows = pl.ds(half, 8)
        ends = [
            combine([end_basis[k, q, rows] for k in range(ITERS + 1)]) for q in range(PER_GROUP)
        ]
        for p in range(X):
            g, q = divmod(p + HALO, PER_GROUP)
            inner = combine([basis[k, p, rows] for k in range(ITERS + 1)])
            both = []
            for value, end in zip(inner, ends[q]):
                low = pltpu.roll(end, (Z - GROUP * g - LOW_AT) % Z, 1)
                high = pltpu.roll(end, (Z - GROUP * g - HIGH_AT) % Z, 1)
                value = jnp.where(lane < HALO, low, value)
                both.append(jnp.where(lane >= Z - HALO, high, value))
            closing[p, rows] = fields[1, p, rows] + both[0]
            mismatch[p, rows] = both[1]


def both_ways(low, high, axis):
    ends = lax.axis_size(axis) - 1
    from_below = lax.ppermute(high, axis, [(i, i + 1) for i in range(ends)])
    from_above = lax.ppermute(low, axis, [(i + 1, i) for i in range(ends)])
    return from_below, from_above


def exchange(copies, axes):
    return lax.all_to_all(copies, axes, split_axis=0, concat_axis=0, tiled=True)


def body(opening, source, category, table, flags):
    brick = (X, Y, Z)
    whole = pltpu.VMEM(brick, jnp.int32)
    fields, low, high, theta = call(
        prepare,
        [HBM] * 5,
        [(4, *brick), (SLAB_X, Y, Z), (SLAB_X, Y, Z), (ITERS, 8, Z)],
        [brick, brick, whole, whole, pltpu.SMEM(table.shape, F32), pltpu.SemaphoreType.DMA((5,))],
    )(*(pltpu.with_memory_space_constraint(a, pltpu.HBM) for a in (opening, source, category, flags, table)))
    left, right = both_ways(low, high, "gx")
    low, high = call(slabs_y, [VMEM] * 3, [(SLAB_Y, Z)] * 2)(fields, left, right)
    below, above = both_ways(low, high, "gy")
    core = lax.axis_index(GZ[1]).reshape(1)
    packed = (PER_GROUP, ROWS, Z)
    wide, near, far = call(assemble, [SMEM] + [VMEM] * 5, [(4, PLANES, ROWS, Z), packed, packed])(
        core, fields, left, right, below, above
    )
    far = lax.ppermute(
        far,
        GZ,
        [p for i in range(1, lax.axis_size(GZ) - 1, 2) for p in ((i, i + 1), (i + 1, i))],
    )
    chip = lax.all_gather(near, GZ[1], axis=0)
    sided = (PLANES, ROWS, Z)
    middle = (6, ROWS + 16, Z)
    basis, sums, ends = call(
        interior,
        [VMEM] * 2,
        [(ITERS + 1, *brick), (len(PAIRS), 8, Z), (4, *packed)],
        [sided, middle] + [sided] * 7,
        flops=20000000,
        vmem=12,
    )(wide, theta)
    first, second = ("gx", "gz_0"), ("gy", "gz_1")
    end_basis, dots = call(
        edges,
        [SMEM] + [VMEM] * 5,
        [(ITERS + 1, PER_GROUP, Y, Z), (lax.axis_size(first), 1, Z)],
        [(4, *packed), packed, middle] + [packed] * 7 + [(Z, Z)],
        flops=5000000,
    )(core, ends, far, chip, theta, sums)
    parts = exchange(dots, first)
    (copies,) = call(relay, [VMEM], [(lax.axis_size(second), 1, Z)])(parts)
    parts = exchange(copies, second)
    closing, mismatch = call(finish, [VMEM] * 5, [brick, brick])(
        parts, basis, end_basis, fields, theta
    )
    return closing, mismatch


def solution(mesh):
    shape = mesh.devices.shape
    split = Mesh(mesh.devices.reshape(shape[0], shape[1], shape[2] // 2, 2), ("gx", "gy", *GZ))
    spec = P("gx", "gy", GZ)
    return jax.shard_map(
        body, mesh=split, in_specs=(spec, spec, spec, P(), spec), out_specs=(spec, spec), check_vma=False
    )
```

```python
import jax
import jax.numpy as jnp
from jax import lax
from jax.experimental import pallas as pl
from jax.experimental.pallas import tpu as pltpu
from jax.sharding import Mesh
from jax.sharding import PartitionSpec as P

ITERS = 4
GZ = ("gz_0", "gz_1")
F32 = jnp.float32
X, Y, Z = 8, 16, 128
HALO = ITERS + 1
WIDTHS = (5, 5, 4, 3)
PLANES = X + 2 * HALO
ROWS = 32
TOP = 8
SLAB_X = sum(WIDTHS)
AT_X = (0, 5, 10, 14)
AT_Y = (0, 90, 180, 244)
SLAB_Y = 288
GROUPS, PER_GROUP, GROUP = 4, 5, 32
LOW_AT, HIGH_AT = 5, 26
SCALE = 64.0
CHUNK = 4
PAIRS = [(i, j) for i in range(ITERS) for j in range(i, ITERS + 1)]
VMEM = pl.BlockSpec(memory_space=pltpu.VMEM)
HBM = pl.BlockSpec(memory_space=pltpu.HBM)
SMEM = pl.BlockSpec(memory_space=pltpu.SMEM)


def planes_of(k):
    return range(HALO - WIDTHS[k], PLANES - HALO + WIDTHS[k])


def call(kernel, ins, outs, scratch=(), flops=100000, vmem=8):
    return pl.pallas_call(
        kernel,
        in_specs=ins,
        out_specs=[VMEM] * len(outs),
        out_shape=[jax.ShapeDtypeStruct(s, F32) for s in outs],
        scratch_shapes=[pltpu.VMEM(s, F32) if isinstance(s, tuple) else s for s in scratch],
        compiler_params=pltpu.CompilerParams(vmem_limit_bytes=vmem * 2**20),
        cost_estimate=pl.CostEstimate(flops=flops, bytes_accessed=1000000, transcendentals=0),
    )


def prepare(
    opening_at, source_at, category_at, flags_at, table_at, fields, low, high, theta,
    opening, source, category, flags, table, arrived,
):
    copies = [
        pltpu.make_async_copy(a, b, arrived.at[n])
        for n, (a, b) in enumerate(
            (
                (table_at, table),
                (category_at, category),
                (flags_at, flags),
                (opening_at, opening),
                (source_at, source),
            )
        )
    ]
    for copy in copies:
        copy.start()
    for copy in copies:
        copy.wait()
    for k, shift in enumerate(shifts_of(table)):
        theta[k] = shift
    for p in range(X):
        kind = category[p]
        cond = jnp.full((Y, Z), table[0], F32)
        for n in range(1, table.shape[0]):
            cond = jnp.where(kind == n, table[n], cond)
        flag = flags[p].astype(F32)
        start = opening[p]
        values = (cond, start, 2.0 * source[p] - 6.0 * flag * start, flag)
        for k, v in enumerate(values):
            fields[k, p] = v
            if p < WIDTHS[k]:
                low[AT_X[k] + p] = v
            if p >= X - WIDTHS[k]:
                high[AT_X[k] + p - (X - WIDTHS[k])] = v


def plane(fields, left, right, k, p):
    if p < HALO:
        return left, (AT_X[k] + p - (HALO - WIDTHS[k]),)
    if p < HALO + X:
        return fields, (k, p - HALO)
    return right, (AT_X[k] + p - HALO - X,)


def slabs_y(fields, left, right, low, high):
    for k, w in enumerate(WIDTHS):
        for n, p in enumerate(planes_of(k)):
            ref, at = plane(fields, left, right, k, p)
            to = pl.ds(AT_Y[k] + w * n, w)
            low[to] = ref[(*at, pl.ds(0, w))]
            high[to] = ref[(*at, pl.ds(Y - w, w))]


def assemble(core, fields, left, right, below, above, wide, near, far):
    lane = lax.broadcasted_iota(jnp.int32, (ROWS, Z), 1)
    first_core = core[0] == 0
    nothing = jnp.zeros((8, Z), F32)
    for k, w in enumerate(WIDTHS):
        for n, p in enumerate(planes_of(k)):
            ref, at = plane(fields, left, right, k, p)
            wide[k, p, 0:TOP] = nothing
            wide[k, p, TOP + Y : ROWS] = nothing
            wide[k, p, TOP : TOP + Y] = ref[at]
            wide[k, p, TOP - w : TOP] = below[AT_Y[k] + w * n : AT_Y[k] + w * (n + 1)]
            wide[k, p, TOP + Y : TOP + Y + w] = above[AT_Y[k] + w * n : AT_Y[k] + w * (n + 1)]
    for q in range(PER_GROUP):
        low = jnp.zeros((ROWS, Z), F32)
        high = low
        for g in range(GROUPS):
            p = PER_GROUP * g + q
            for k, w in enumerate(WIDTHS):
                if p in planes_of(k):
                    base = GROUP * g + AT_X[k]
                    turned = pltpu.roll(wide[k, p], base, 1)
                    place = lane if base else jnp.where(lane < Z // 2, lane, lane - Z)
                    low = jnp.where((place >= base) & (place < base + w), turned, low)
                    high = jnp.where((place >= base - w) & (place < base), turned, high)
        far[q] = jnp.where(first_core, low, high)
        near[q] = jnp.where(first_core, high, low)


def shifts_of(table):
    values = [jnp.full((8, Z), table[n], F32) for n in range(table.shape[0])]
    least, most, mean = values[0], values[0], values[0]
    for v in values[1:]:
        least, most, mean = jnp.minimum(least, v), jnp.maximum(most, v), mean + v
    mean = mean * (1.0 / len(values))
    top = 4.0 + 16.0 * most + 16.0 * mean
    low = 2.0 + 8.0 * least + 8.0 * mean
    middle, half = 0.5 * (top + low), 0.5 * (top - low)
    return [
        (middle + half * c) * (1.0 / SCALE) for c in (0.9238795, -0.9238795, 0.3826834, -0.3826834)
    ]


def smooth(mid, ahead, here, behind, first, count):
    n = here.shape[0]
    mid[0:n, 8 : 8 + ROWS] = (ahead + here) + (here + behind)
    sides = mid[0:n, pl.ds(7 + first, count)] + mid[0:n, pl.ds(9 + first, count)]
    rows = mid[0:n, pl.ds(8 + first, count)] + 0.5 * sides
    return rows + 0.5 * (pltpu.roll(rows, 1, 2) + pltpu.roll(rows, Z - 1, 2))


def newton_step(slope, diag, inside, shift, v, tv, tu):
    return ((diag - shift) * v - (slope * tv + tu)) * inside


def chunks(low, high, most):
    count = -(-(high - low) // most)
    size = -(-(high - low) // count)
    return [(p, min(p + size, high)) for p in range(low, high, size)]


def interior(wide, theta, basis, sums, ends, cx, mid, slope, diag, inside, va, vb, ua, ub):
    lane = lax.broadcasted_iota(jnp.int32, (ROWS, Z), 1)
    slots = mid.shape[0]
    slot = [0]

    def along(ref, p, q, first=0, count=ROWS):
        slot[0] += 1
        return smooth(
            mid.at[slot[0] % slots], ref[p - 1 : q - 1], ref[p:q], ref[p + 1 : q + 1], first, count
        )

    cond, start, rest, flag = (wide.at[k] for k in range(4))
    cx[...] = cond[...] * start[...]
    for p, q in chunks(1, PLANES - 1, CHUNK):
        tc, tx, tcx = (along(ref, p, q) for ref in (cond, start, cx))
        c = cond[p:q]
        near = 16.0 * c + tc
        diag[p:q] = (1.0 + 6.0 * flag[p:q] + near) * (1.0 / SCALE)
        half_c = c * (1.0 / SCALE)
        slope[p:q] = half_c
        there = jnp.where(c > 0.0, 1.0, 0.0)
        inside[p:q] = there
        r = (rest[p:q] - near * start[p:q] + (c * tx + tcx)) * there
        va[p:q] = r
        ua[p:q] = r * half_c
    basis[0] = va[HALO : HALO + X, TOP : TOP + Y]
    for k in range(ITERS):
        v_old, u_old, v_new, u_new = (va, ua, vb, ub) if k % 2 == 0 else (vb, ub, va, ua)
        last = k + 1 == ITERS
        first, count = (TOP, Y) if last else (0, ROWS)
        rows = pl.ds(first, count)
        shift = jnp.tile(theta[k], (count // 8, 1))[None]
        for p, q in chunks(2 + k, PLANES - 2 - k, CHUNK):
            tv, tu = along(v_old, p, q, first, count), along(u_old, p, q, first, count)
            v = newton_step(slope[p:q, rows], diag[p:q, rows], inside[p:q, rows], shift, v_old[p:q, rows], tv, tu)
            if last:
                basis[k + 1, p - HALO : q - HALO] = v
            else:
                v_new[p:q] = v
                u_new[p:q] = v * slope[p:q]
        if not last:
            basis[k + 1] = v_new[HALO : HALO + X, TOP : TOP + Y]

    inner = (lane[:8] >= HALO) & (lane[:8] < Z - HALO)
    for n, (i, j) in enumerate(PAIRS):
        total = None
        for p in range(X):
            for half in (0, 8):
                rows = pl.ds(half, 8)
                term = basis[i, p, rows] * basis[j, p, rows]
                total = term if total is None else total + term
        sums[n] = jnp.where(inner, total, 0.0)

    place = lane % GROUP
    for k in range(4):
        for q in range(PER_GROUP):
            out = jnp.zeros((ROWS, Z), F32)
            for g in range(GROUPS):
                p = PER_GROUP * g + q
                if p in planes_of(k):
                    mine = (lane // GROUP) == g
                    low = pltpu.roll(wide[k, p], GROUP * g + LOW_AT, 1)
                    high = pltpu.roll(wide[k, p], (GROUP * g + HIGH_AT) % Z, 1)
                    low_here = mine & (place >= LOW_AT) & (place < LOW_AT + 2 * HALO)
                    high_here = mine & (place >= HIGH_AT - 2 * HALO) & (place < HIGH_AT)
                    out = jnp.where(low_here, low, jnp.where(high_here, high, out))
            ends[k, q] = out


def edges(core, ends, far, chip, theta, inner_sums, basis, dots, cells, cx, mid, slope, diag, inside, va, vb, ua, ub, stack):
    lane = lax.broadcasted_iota(jnp.int32, (ROWS, Z), 1)
    place = lane % GROUP
    first_core = core[0] == 0
    partner = 1 - core[0]
    slots = mid.shape[0]
    slot = [0]

    for q in range(PER_GROUP):
        near, other = chip[partner, q], far[q]
        below = jnp.where(first_core, other, near)
        above = jnp.where(first_core, near, other)
        for k in range(4):
            low = pltpu.roll(below, (LOW_AT - AT_X[k]) % Z, 1)
            high = pltpu.roll(above, (HIGH_AT - AT_X[k]) % Z, 1)
            out = jnp.where(place < LOW_AT, low, ends[k, q])
            cells[k, q] = jnp.where((place >= HIGH_AT) & (place < HIGH_AT + HALO), high, out)

    def along(ref, first=0, count=ROWS):
        slot[0] += 1
        here = ref[...]
        before = pltpu.roll(ref[PER_GROUP - 1], GROUP, 1)[None]
        after = pltpu.roll(ref[0], Z - GROUP, 1)[None]
        return smooth(
            mid.at[slot[0] % slots],
            jnp.concatenate([before, ref[: PER_GROUP - 1]]),
            here,
            jnp.concatenate([ref[1:], after]),
            first,
            count,
        )

    cond, start, rest, flag = (cells.at[k] for k in range(4))
    cx[...] = cond[...] * start[...]
    tc, tx, tcx = (along(ref) for ref in (cond, start, cx))
    c = cond[...]
    near = 16.0 * c + tc
    diag[...] = (1.0 + 6.0 * flag[...] + near) * (1.0 / SCALE)
    half_c = c * (1.0 / SCALE)
    slope[...] = half_c
    there = jnp.where(c > 0.0, 1.0, 0.0)
    inside[...] = there
    r = (rest[...] - near * start[...] + (c * tx + tcx)) * there
    va[...] = r
    ua[...] = r * half_c
    basis[0] = r[:, TOP : TOP + Y]
    for k in range(ITERS):
        v_old, u_old, v_new, u_new = (va, ua, vb, ub) if k % 2 == 0 else (vb, ub, va, ua)
        last = k + 1 == ITERS
        first, count = (TOP, Y) if last else (0, ROWS)
        rows = pl.ds(first, count)
        shift = jnp.tile(theta[k], (count // 8, 1))[None]
        tv, tu = along(v_old, first, count), along(u_old, first, count)
        v = newton_step(slope[:, rows], diag[:, rows], inside[:, rows], shift, v_old[:, rows], tv, tu)
        if not last:
            v_new[...] = v
            u_new[...] = v * slope[...]
        basis[k + 1] = v if last else v[:, TOP : TOP + Y]

    end_cells = ((place >= LOW_AT) & (place < LOW_AT + HALO)) | ((place >= HIGH_AT - HALO) & (place < HIGH_AT))
    mine = []
    for q in range(PER_GROUP):
        own = [g for g in range(GROUPS) if HALO <= PER_GROUP * g + q < HALO + X]
        at = (lane >= GROUP * own[0]) & (lane < GROUP * (own[-1] + 1))
        mine.append(jnp.where(at & end_cells, 1.0, 0.0)[:8])
    for n in range(16):
        total = None
        if n < len(PAIRS):
            i, j = PAIRS[n]
            total = inner_sums[n]
            for q in range(PER_GROUP):
                for half in (0, 8):
                    rows = pl.ds(half, 8)
                    total = total + (basis[i, q, rows] * mine[q]) * basis[j, q, rows]
        else:
            total = jnp.zeros((8, Z), F32)
        stack[pl.ds(8 * n, 8)] = total
    by_sum = stack[pl.ds(0, 16, stride=8)]
    for n in range(1, 8):
        by_sum = by_sum + stack[pl.ds(n, 16, stride=8)]
    total = lax.dot_general(
        jnp.ones((8, Z), F32), jnp.tile(by_sum, (8, 1)), (((1,), (1,)), ((), ())),
        precision=lax.Precision.HIGHEST, preferred_element_type=F32,
    )
    for n in range(dots.shape[0]):
        dots[n] = total[0:1]


def two_sum(a, b):
    s = a + b
    t = s - a
    return s, (a - (s - t)) + (b - t)


def row_sum(parts):
    rows = [(parts[n], None) for n in range(parts.shape[0])]
    while len(rows) > 1:
        pairs, rows = zip(rows[::2], rows[1::2]), []
        for (a, ea), (b, eb) in pairs:
            s, e = two_sum(a, b)
            rows.append((s, e if ea is None else e + (ea + eb)))
    return rows[0]


def relay(parts, copies):
    total, rest = row_sum(parts)
    lane = lax.broadcasted_iota(jnp.int32, total.shape, 1)
    total = jnp.where(lane < 16, total, rest)
    for n in range(copies.shape[0]):
        copies[n] = total


def quick(a, b):
    s = a + b
    return s, b - (s - a)


def halves(a):
    t = 4097.0 * a
    high = t - (t - a)
    return high, a - high


def plus(a, b):
    s, e = two_sum(a[0], b[0])
    return quick(s, e + (a[1] + b[1]))


def minus(a, b):
    return plus(a, (-b[0], -b[1]))


def times(a, b):
    p = a[0] * b[0]
    ah, al = halves(a[0])
    bh, bl = halves(b[0])
    e = ((ah * bh - p) + ah * bl + al * bh) + al * bl
    return quick(p, e + (a[0] * b[1] + a[1] * b[0]))


def over(a, b):
    q = a[0] / b[0]
    none = jnp.zeros_like(q)
    rest = minus(a, times((q, none), b))
    return quick(q, rest[0] / b[0])


def conjugate_gradients(gram, theta):
    none = jnp.zeros_like(theta[0])
    zero, one = (none, none), (none + 1.0, none)
    shift = [(t, none) for t in theta]

    def along(k, vector):
        total = times(gram[k, 0], vector[0])
        for j in range(1, len(vector)):
            total = plus(total, times(gram[k, j], vector[j]))
        return total

    r, p = [one], [one]
    y = [zero] * ITERS
    rr = gram[0, 0]
    for k in range(ITERS):
        image = [times(shift[i], p[i]) for i in range(k + 1)] + [zero]
        image = [image[0]] + [plus(image[i], p[i - 1]) for i in range(1, k + 2)]
        step = over(rr, times(p[k], along(k, image)))
        y = [plus(y[i], times(step, p[i])) if i <= k else y[i] for i in range(ITERS)]
        r = [minus(r[i] if i <= k else zero, times(step, image[i])) for i in range(k + 2)]
        if k + 1 < ITERS:
            new = times(r[k + 1], along(k + 1, r))
            ratio = over(new, rr)
            p = [plus(r[i], times(ratio, p[i])) if i <= k else r[i] for i in range(k + 2)]
            rr = new
    return [a[0] * (1.0 / SCALE) for a in y], [a[0] for a in r]


def finish(parts, basis, end_basis, fields, theta, closing, mismatch):
    total, rest = row_sum(parts)
    rest = rest + pltpu.roll(total, Z - 16, 1)
    gram = {}
    for n, (i, j) in enumerate(PAIRS):
        gram[i, j] = gram[j, i] = quick(
            *(jnp.broadcast_to(v[0:1, n : n + 1], (8, Z)) for v in (total, rest))
        )
    y, r = conjugate_gradients(gram, [theta[k] for k in range(ITERS)])

    def combine(v):
        x, m = y[0] * v[0], r[ITERS] * v[ITERS]
        for k in range(1, ITERS):
            x = x + y[k] * v[k]
        for k in range(ITERS):
            m = m + r[k] * v[k]
        return x, m

    lane = lax.broadcasted_iota(jnp.int32, (8, Z), 1)
    for half in (0, 8):
        rows = pl.ds(half, 8)
        ends = [
            combine([end_basis[k, q, rows] for k in range(ITERS + 1)]) for q in range(PER_GROUP)
        ]
        for p in range(X):
            g, q = divmod(p + HALO, PER_GROUP)
            inner = combine([basis[k, p, rows] for k in range(ITERS + 1)])
            both = []
            for value, end in zip(inner, ends[q]):
                low = pltpu.roll(end, (Z - GROUP * g - LOW_AT) % Z, 1)
                high = pltpu.roll(end, (Z - GROUP * g - HIGH_AT) % Z, 1)
                value = jnp.where(lane < HALO, low, value)
                both.append(jnp.where(lane >= Z - HALO, high, value))
            closing[p, rows] = fields[1, p, rows] + both[0]
            mismatch[p, rows] = both[1]


def both_ways(low, high, axis):
    ends = lax.axis_size(axis) - 1
    from_below = lax.ppermute(high, axis, [(i, i + 1) for i in range(ends)])
    from_above = lax.ppermute(low, axis, [(i + 1, i) for i in range(ends)])
    return from_below, from_above


def exchange(copies, axes):
    return lax.all_to_all(copies, axes, split_axis=0, concat_axis=0, tiled=True)


def body(opening, source, category, table, flags):
    brick = (X, Y, Z)
    whole = pltpu.VMEM(brick, jnp.int32)
    fields, low, high, theta = call(
        prepare,
        [HBM] * 5,
        [(4, *brick), (SLAB_X, Y, Z), (SLAB_X, Y, Z), (ITERS, 8, Z)],
        [brick, brick, whole, whole, pltpu.SMEM(table.shape, F32), pltpu.SemaphoreType.DMA((5,))],
    )(*(pltpu.with_memory_space_constraint(a, pltpu.HBM) for a in (opening, source, category, flags, table)))
    left, right = both_ways(low, high, "gx")
    low, high = call(slabs_y, [VMEM] * 3, [(SLAB_Y, Z)] * 2)(fields, left, right)
    below, above = both_ways(low, high, "gy")
    core = lax.axis_index(GZ[1]).reshape(1)
    packed = (PER_GROUP, ROWS, Z)
    wide, near, far = call(assemble, [SMEM] + [VMEM] * 5, [(4, PLANES, ROWS, Z), packed, packed])(
        core, fields, left, right, below, above
    )
    far = lax.ppermute(
        far,
        GZ,
        [p for i in range(1, lax.axis_size(GZ) - 1, 2) for p in ((i, i + 1), (i + 1, i))],
    )
    chip = lax.all_gather(near, GZ[1], axis=0)
    sided = (PLANES, ROWS, Z)
    middle = (3, PLANES, ROWS + 16, Z)
    basis, sums, ends = call(
        interior,
        [VMEM] * 2,
        [(ITERS + 1, *brick), (len(PAIRS), 8, Z), (4, *packed)],
        [sided, middle] + [sided] * 7,
        flops=20000000,
        vmem=12,
    )(wide, theta)
    first, second = ("gx", "gz_0"), ("gy", "gz_1")
    end_basis, dots = call(
        edges,
        [SMEM] + [VMEM] * 5,
        [(ITERS + 1, PER_GROUP, Y, Z), (lax.axis_size(first), 1, Z)],
        [(4, *packed), packed, (3, PER_GROUP, ROWS + 16, Z)] + [packed] * 7 + [(Z, Z)],
        flops=5000000,
    )(core, ends, far, chip, theta, sums)
    parts = exchange(dots, first)
    (copies,) = call(relay, [VMEM], [(lax.axis_size(second), 1, Z)])(parts)
    parts = exchange(copies, second)
    closing, mismatch = call(finish, [VMEM] * 5, [brick, brick])(
        parts, basis, end_basis, fields, theta
    )
    return closing, mismatch


def solution(mesh):
    shape = mesh.devices.shape
    split = Mesh(mesh.devices.reshape(shape[0], shape[1], shape[2] // 2, 2), ("gx", "gy", *GZ))
    spec = P("gx", "gy", GZ)
    return jax.shard_map(
        body, mesh=split, in_specs=(spec, spec, spec, P(), spec), out_specs=(spec, spec), check_vma=False
    )
```

```python
import jax
import jax.numpy as jnp
from jax import lax
from jax.experimental import pallas as pl
from jax.experimental.pallas import tpu as pltpu
from jax.sharding import Mesh
from jax.sharding import PartitionSpec as P

ITERS = 4
GX, GY, GZ = (("gx_0", "gx_1"), ("gy_0", "gy_1"), ("gz_0", "gz_1"))
F32 = jnp.float32
X, Y, Z = 8, 16, 128
HALO = ITERS + 1
WIDTHS = (5, 5, 4, 3)
PLANES = X + 2 * HALO
ROWS = 32
TOP = 8
SLAB_X = sum(WIDTHS)
AT_X = (0, 5, 10, 14)
AT_Y = (0, 90, 180, 244)
SLAB_Y = 288
GROUPS, PER_GROUP, GROUP = 4, 5, 32
LOW_AT, HIGH_AT = 5, 26
SCALE = 64.0
CHUNK = 4
PAIRS = [(i, j) for i in range(ITERS) for j in range(i, ITERS + 1)]
VMEM = pl.BlockSpec(memory_space=pltpu.VMEM)
HBM = pl.BlockSpec(memory_space=pltpu.HBM)
SMEM = pl.BlockSpec(memory_space=pltpu.SMEM)


def planes_of(k):
    return range(HALO - WIDTHS[k], PLANES - HALO + WIDTHS[k])


def call(kernel, ins, outs, scratch=(), flops=100000, vmem=8):
    return pl.pallas_call(
        kernel,
        in_specs=ins,
        out_specs=[VMEM] * len(outs),
        out_shape=[jax.ShapeDtypeStruct(s, F32) for s in outs],
        scratch_shapes=[pltpu.VMEM(s, F32) if isinstance(s, tuple) else s for s in scratch],
        compiler_params=pltpu.CompilerParams(vmem_limit_bytes=vmem * 2**20),
        cost_estimate=pl.CostEstimate(flops=flops, bytes_accessed=1000000, transcendentals=0),
    )


def prepare(
    place_x, opening_at, source_at, category_at, flags_at, table_at, fields, near, far, theta,
    opening, source, category, flags, table, arrived,
):
    copies = [
        pltpu.make_async_copy(a, b, arrived.at[n])
        for n, (a, b) in enumerate(
            (
                (table_at, table),
                (category_at, category),
                (flags_at, flags),
                (opening_at, opening),
                (source_at, source),
            )
        )
    ]
    for copy in copies:
        copy.start()
    for copy in copies:
        copy.wait()
    for k, shift in enumerate(shifts_of(table)):
        theta[k] = shift
    for p in range(X):
        kind = category[p]
        cond = jnp.full((Y, Z), table[0], F32)
        for n in range(1, table.shape[0]):
            cond = jnp.where(kind == n, table[n], cond)
        flag = flags[p].astype(F32)
        start = opening[p]
        values = (cond, start, 2.0 * source[p] - 6.0 * flag * start, flag)
        for k, v in enumerate(values):
            fields[k, p] = v
    first = place_x[0] == 0
    for k, w in enumerate(WIDTHS):
        for n in range(w):
            low, high = fields[k, n], fields[k, X - w + n]
            near[AT_X[k] + n] = jnp.where(first, high, low)
            far[AT_X[k] + n] = jnp.where(first, low, high)


def halo(place, far, pair, at, lower):
    far_side = (place == 0) if lower else (place == 1)
    return jnp.where(far_side, far[at], pair[(1 - place, *at)])


def plane(place, fields, far, pair, k, p, rows=slice(None)):
    if p < HALO:
        return halo(place, far, pair, (AT_X[k] + p - (HALO - WIDTHS[k]), rows), True)
    if p < HALO + X:
        return fields[k, p - HALO, rows]
    return halo(place, far, pair, (AT_X[k] + p - HALO - X, rows), False)


def slabs_y(place_x, place_y, fields, far_x, pair_x, near, far):
    first = place_y[0] == 0
    for k, w in enumerate(WIDTHS):
        for n, p in enumerate(planes_of(k)):
            to = pl.ds(AT_Y[k] + w * n, w)
            low, high = (
                plane(place_x[0], fields, far_x, pair_x, k, p, pl.ds(at, w)) for at in (0, Y - w)
            )
            near[to] = jnp.where(first, high, low)
            far[to] = jnp.where(first, low, high)


def assemble(place_x, place_y, place_z, fields, far_x, pair_x, far_y, pair_y, wide, near, far):
    lane = lax.broadcasted_iota(jnp.int32, (ROWS, Z), 1)
    first_core = place_z[0] == 0
    nothing = jnp.zeros((8, Z), F32)
    for k, w in enumerate(WIDTHS):
        for n, p in enumerate(planes_of(k)):
            at = (pl.ds(AT_Y[k] + w * n, w),)
            wide[k, p, 0:TOP] = nothing
            wide[k, p, TOP + Y : ROWS] = nothing
            wide[k, p, TOP : TOP + Y] = plane(place_x[0], fields, far_x, pair_x, k, p)
            wide[k, p, TOP - w : TOP] = halo(place_y[0], far_y, pair_y, at, True)
            wide[k, p, TOP + Y : TOP + Y + w] = halo(place_y[0], far_y, pair_y, at, False)
    for q in range(PER_GROUP):
        low = jnp.zeros((ROWS, Z), F32)
        high = low
        for g in range(GROUPS):
            p = PER_GROUP * g + q
            for k, w in enumerate(WIDTHS):
                if p in planes_of(k):
                    base = GROUP * g + AT_X[k]
                    turned = pltpu.roll(wide[k, p], base, 1)
                    place = lane if base else jnp.where(lane < Z // 2, lane, lane - Z)
                    low = jnp.where((place >= base) & (place < base + w), turned, low)
                    high = jnp.where((place >= base - w) & (place < base), turned, high)
        far[q] = jnp.where(first_core, low, high)
        near[q] = jnp.where(first_core, high, low)


def shifts_of(table):
    values = [jnp.full((8, Z), table[n], F32) for n in range(table.shape[0])]
    least, most, mean = values[0], values[0], values[0]
    for v in values[1:]:
        least, most, mean = jnp.minimum(least, v), jnp.maximum(most, v), mean + v
    mean = mean * (1.0 / len(values))
    top = 4.0 + 16.0 * most + 16.0 * mean
    low = 2.0 + 8.0 * least + 8.0 * mean
    middle, half = 0.5 * (top + low), 0.5 * (top - low)
    return [
        (middle + half * c) * (1.0 / SCALE) for c in (0.9238795, -0.9238795, 0.3826834, -0.3826834)
    ]


def smooth(mid, ahead, here, behind, first, count):
    n = here.shape[0]
    mid[0:n, 8 : 8 + ROWS] = (ahead + here) + (here + behind)
    sides = mid[0:n, pl.ds(7 + first, count)] + mid[0:n, pl.ds(9 + first, count)]
    rows = mid[0:n, pl.ds(8 + first, count)] + 0.5 * sides
    return rows + 0.5 * (pltpu.roll(rows, 1, 2) + pltpu.roll(rows, Z - 1, 2))


def newton_step(slope, diag, inside, shift, v, tv, tu):
    return ((diag - shift) * v - (slope * tv + tu)) * inside


def chunks(low, high, most):
    count = -(-(high - low) // most)
    size = -(-(high - low) // count)
    return [(p, min(p + size, high)) for p in range(low, high, size)]


def interior(wide, theta, basis, sums, ends, cx, mid, slope, diag, inside, va, vb, ua, ub):
    lane = lax.broadcasted_iota(jnp.int32, (ROWS, Z), 1)
    slots = mid.shape[0]
    slot = [0]

    def along(ref, p, q, first=0, count=ROWS):
        slot[0] += 1
        return smooth(
            mid.at[slot[0] % slots], ref[p - 1 : q - 1], ref[p:q], ref[p + 1 : q + 1], first, count
        )

    cond, start, rest, flag = (wide.at[k] for k in range(4))
    cx[...] = cond[...] * start[...]
    for p, q in chunks(1, PLANES - 1, CHUNK):
        tc, tx, tcx = (along(ref, p, q) for ref in (cond, start, cx))
        c = cond[p:q]
        near = 16.0 * c + tc
        diag[p:q] = (1.0 + 6.0 * flag[p:q] + near) * (1.0 / SCALE)
        half_c = c * (1.0 / SCALE)
        slope[p:q] = half_c
        there = jnp.where(c > 0.0, 1.0, 0.0)
        inside[p:q] = there
        r = (rest[p:q] - near * start[p:q] + (c * tx + tcx)) * there
        va[p:q] = r
        ua[p:q] = r * half_c
    basis[0] = va[HALO : HALO + X, TOP : TOP + Y]
    for k in range(ITERS):
        v_old, u_old, v_new, u_new = (va, ua, vb, ub) if k % 2 == 0 else (vb, ub, va, ua)
        last = k + 1 == ITERS
        first, count = (TOP, Y) if last else (0, ROWS)
        rows = pl.ds(first, count)
        shift = jnp.tile(theta[k], (count // 8, 1))[None]
        for p, q in chunks(2 + k, PLANES - 2 - k, CHUNK):
            tv, tu = along(v_old, p, q, first, count), along(u_old, p, q, first, count)
            v = newton_step(slope[p:q, rows], diag[p:q, rows], inside[p:q, rows], shift, v_old[p:q, rows], tv, tu)
            if last:
                basis[k + 1, p - HALO : q - HALO] = v
            else:
                v_new[p:q] = v
                u_new[p:q] = v * slope[p:q]
        if not last:
            basis[k + 1] = v_new[HALO : HALO + X, TOP : TOP + Y]

    inner = (lane[:8] >= HALO) & (lane[:8] < Z - HALO)
    for n, (i, j) in enumerate(PAIRS):
        total = None
        for p in range(X):
            for half in (0, 8):
                rows = pl.ds(half, 8)
                term = basis[i, p, rows] * basis[j, p, rows]
                total = term if total is None else total + term
        sums[n] = jnp.where(inner, total, 0.0)

    place = lane % GROUP
    for k in range(4):
        for q in range(PER_GROUP):
            out = jnp.zeros((ROWS, Z), F32)
            for g in range(GROUPS):
                p = PER_GROUP * g + q
                if p in planes_of(k):
                    mine = (lane // GROUP) == g
                    low = pltpu.roll(wide[k, p], GROUP * g + LOW_AT, 1)
                    high = pltpu.roll(wide[k, p], (GROUP * g + HIGH_AT) % Z, 1)
                    low_here = mine & (place >= LOW_AT) & (place < LOW_AT + 2 * HALO)
                    high_here = mine & (place >= HIGH_AT - 2 * HALO) & (place < HIGH_AT)
                    out = jnp.where(low_here, low, jnp.where(high_here, high, out))
            ends[k, q] = out


def edges(place_z, ends, far, chip, theta, inner_sums, basis, dots, cells, cx, mid, slope, diag, inside, va, vb, ua, ub, stack):
    lane = lax.broadcasted_iota(jnp.int32, (ROWS, Z), 1)
    place = lane % GROUP
    slots = mid.shape[0]
    slot = [0]

    for q in range(PER_GROUP):
        below, above = (halo(place_z[0], far, chip, (q,), lower) for lower in (True, False))
        for k in range(4):
            low = pltpu.roll(below, (LOW_AT - AT_X[k]) % Z, 1)
            high = pltpu.roll(above, (HIGH_AT - AT_X[k]) % Z, 1)
            out = jnp.where(place < LOW_AT, low, ends[k, q])
            cells[k, q] = jnp.where((place >= HIGH_AT) & (place < HIGH_AT + HALO), high, out)

    def along(ref, first=0, count=ROWS):
        slot[0] += 1
        here = ref[...]
        before = pltpu.roll(ref[PER_GROUP - 1], GROUP, 1)[None]
        after = pltpu.roll(ref[0], Z - GROUP, 1)[None]
        return smooth(
            mid.at[slot[0] % slots],
            jnp.concatenate([before, ref[: PER_GROUP - 1]]),
            here,
            jnp.concatenate([ref[1:], after]),
            first,
            count,
        )

    cond, start, rest, flag = (cells.at[k] for k in range(4))
    cx[...] = cond[...] * start[...]
    tc, tx, tcx = (along(ref) for ref in (cond, start, cx))
    c = cond[...]
    near = 16.0 * c + tc
    diag[...] = (1.0 + 6.0 * flag[...] + near) * (1.0 / SCALE)
    half_c = c * (1.0 / SCALE)
    slope[...] = half_c
    there = jnp.where(c > 0.0, 1.0, 0.0)
    inside[...] = there
    r = (rest[...] - near * start[...] + (c * tx + tcx)) * there
    va[...] = r
    ua[...] = r * half_c
    basis[0] = r[:, TOP : TOP + Y]
    for k in range(ITERS):
        v_old, u_old, v_new, u_new = (va, ua, vb, ub) if k % 2 == 0 else (vb, ub, va, ua)
        last = k + 1 == ITERS
        first, count = (TOP, Y) if last else (0, ROWS)
        rows = pl.ds(first, count)
        shift = jnp.tile(theta[k], (count // 8, 1))[None]
        tv, tu = along(v_old, first, count), along(u_old, first, count)
        v = newton_step(slope[:, rows], diag[:, rows], inside[:, rows], shift, v_old[:, rows], tv, tu)
        if not last:
            v_new[...] = v
            u_new[...] = v * slope[...]
        basis[k + 1] = v if last else v[:, TOP : TOP + Y]

    end_cells = ((place >= LOW_AT) & (place < LOW_AT + HALO)) | ((place >= HIGH_AT - HALO) & (place < HIGH_AT))
    mine = []
    for q in range(PER_GROUP):
        own = [g for g in range(GROUPS) if HALO <= PER_GROUP * g + q < HALO + X]
        at = (lane >= GROUP * own[0]) & (lane < GROUP * (own[-1] + 1))
        mine.append(jnp.where(at & end_cells, 1.0, 0.0)[:8])
    for n in range(16):
        total = None
        if n < len(PAIRS):
            i, j = PAIRS[n]
            total = inner_sums[n]
            for q in range(PER_GROUP):
                for half in (0, 8):
                    rows = pl.ds(half, 8)
                    total = total + (basis[i, q, rows] * mine[q]) * basis[j, q, rows]
        else:
            total = jnp.zeros((8, Z), F32)
        stack[pl.ds(8 * n, 8)] = total
    by_sum = stack[pl.ds(0, 16, stride=8)]
    for n in range(1, 8):
        by_sum = by_sum + stack[pl.ds(n, 16, stride=8)]
    total = lax.dot_general(
        jnp.ones((8, Z), F32), jnp.tile(by_sum, (8, 1)), (((1,), (1,)), ((), ())),
        precision=lax.Precision.HIGHEST, preferred_element_type=F32,
    )
    for n in range(dots.shape[0]):
        dots[n] = total[0:1]


def two_sum(a, b):
    s = a + b
    t = s - a
    return s, (a - (s - t)) + (b - t)


def row_sum(parts):
    rows = [(parts[n], None) for n in range(parts.shape[0])]
    while len(rows) > 1:
        pairs, rows = zip(rows[::2], rows[1::2]), []
        for (a, ea), (b, eb) in pairs:
            s, e = two_sum(a, b)
            rows.append((s, e if ea is None else e + (ea + eb)))
    return rows[0]


def relay(parts, copies):
    total, rest = row_sum(parts)
    lane = lax.broadcasted_iota(jnp.int32, total.shape, 1)
    total = jnp.where(lane < 16, total, rest)
    for n in range(copies.shape[0]):
        copies[n] = total


def quick(a, b):
    s = a + b
    return s, b - (s - a)


def halves(a):
    t = 4097.0 * a
    high = t - (t - a)
    return high, a - high


def plus(a, b):
    s, e = two_sum(a[0], b[0])
    return quick(s, e + (a[1] + b[1]))


def minus(a, b):
    return plus(a, (-b[0], -b[1]))


def times(a, b):
    p = a[0] * b[0]
    ah, al = halves(a[0])
    bh, bl = halves(b[0])
    e = ((ah * bh - p) + ah * bl + al * bh) + al * bl
    return quick(p, e + (a[0] * b[1] + a[1] * b[0]))


def over(a, b):
    q = a[0] / b[0]
    none = jnp.zeros_like(q)
    rest = minus(a, times((q, none), b))
    return quick(q, rest[0] / b[0])


def conjugate_gradients(gram, theta):
    none = jnp.zeros_like(theta[0])
    zero, one = (none, none), (none + 1.0, none)
    shift = [(t, none) for t in theta]

    def along(k, vector):
        total = times(gram[k, 0], vector[0])
        for j in range(1, len(vector)):
            total = plus(total, times(gram[k, j], vector[j]))
        return total

    r, p = [one], [one]
    y = [zero] * ITERS
    rr = gram[0, 0]
    for k in range(ITERS):
        image = [times(shift[i], p[i]) for i in range(k + 1)] + [zero]
        image = [image[0]] + [plus(image[i], p[i - 1]) for i in range(1, k + 2)]
        step = over(rr, times(p[k], along(k, image)))
        y = [plus(y[i], times(step, p[i])) if i <= k else y[i] for i in range(ITERS)]
        r = [minus(r[i] if i <= k else zero, times(step, image[i])) for i in range(k + 2)]
        if k + 1 < ITERS:
            new = times(r[k + 1], along(k + 1, r))
            ratio = over(new, rr)
            p = [plus(r[i], times(ratio, p[i])) if i <= k else r[i] for i in range(k + 2)]
            rr = new
    return [a[0] * (1.0 / SCALE) for a in y], [a[0] for a in r]


def finish(parts, basis, end_basis, fields, theta, closing, mismatch):
    total, rest = row_sum(parts)
    rest = rest + pltpu.roll(total, Z - 16, 1)
    gram = {}
    for n, (i, j) in enumerate(PAIRS):
        gram[i, j] = gram[j, i] = quick(
            *(jnp.broadcast_to(v[0:1, n : n + 1], (8, Z)) for v in (total, rest))
        )
    y, r = conjugate_gradients(gram, [theta[k] for k in range(ITERS)])

    def combine(v):
        x, m = y[0] * v[0], r[ITERS] * v[ITERS]
        for k in range(1, ITERS):
            x = x + y[k] * v[k]
        for k in range(ITERS):
            m = m + r[k] * v[k]
        return x, m

    lane = lax.broadcasted_iota(jnp.int32, (8, Z), 1)
    for half in (0, 8):
        rows = pl.ds(half, 8)
        ends = [
            combine([end_basis[k, q, rows] for k in range(ITERS + 1)]) for q in range(PER_GROUP)
        ]
        for p in range(X):
            g, q = divmod(p + HALO, PER_GROUP)
            inner = combine([basis[k, p, rows] for k in range(ITERS + 1)])
            both = []
            for value, end in zip(inner, ends[q]):
                low = pltpu.roll(end, (Z - GROUP * g - LOW_AT) % Z, 1)
                high = pltpu.roll(end, (Z - GROUP * g - HIGH_AT) % Z, 1)
                value = jnp.where(lane < HALO, low, value)
                both.append(jnp.where(lane >= Z - HALO, high, value))
            closing[p, rows] = fields[1, p, rows] + both[0]
            mismatch[p, rows] = both[1]


def trade(near, far, axes):
    ends = lax.axis_size(axes) - 1
    others = [p for i in range(1, ends, 2) for p in ((i, i + 1), (i + 1, i))]
    return lax.ppermute(far, axes, others), lax.all_gather(near, axes[1], axis=0)


def exchange(copies, axes):
    return lax.all_to_all(copies, axes, split_axis=0, concat_axis=0, tiled=True)


def body(opening, source, category, table, flags):
    brick = (X, Y, Z)
    place_x, place_y, place_z = (lax.axis_index(axes[1]).reshape(1) for axes in (GX, GY, GZ))
    whole = pltpu.VMEM(brick, jnp.int32)
    fields, near, far, theta = call(
        prepare,
        [SMEM] + [HBM] * 5,
        [(4, *brick), (SLAB_X, Y, Z), (SLAB_X, Y, Z), (ITERS, 8, Z)],
        [brick, brick, whole, whole, pltpu.SMEM(table.shape, F32), pltpu.SemaphoreType.DMA((5,))],
    )(
        place_x,
        *(
            pltpu.with_memory_space_constraint(a, pltpu.HBM)
            for a in (opening, source, category, flags, table)
        ),
    )
    by_x = trade(near, far, GX)
    near, far = call(slabs_y, [SMEM] * 2 + [VMEM] * 3, [(SLAB_Y, Z)] * 2)(
        place_x, place_y, fields, *by_x
    )
    by_y = trade(near, far, GY)
    packed = (PER_GROUP, ROWS, Z)
    wide, near, far = call(assemble, [SMEM] * 3 + [VMEM] * 5, [(4, PLANES, ROWS, Z), packed, packed])(
        place_x, place_y, place_z, fields, *by_x, *by_y
    )
    far, chip = trade(near, far, GZ)
    sided = (PLANES, ROWS, Z)
    middle = (3, PLANES, ROWS + 16, Z)
    basis, sums, ends = call(
        interior,
        [VMEM] * 2,
        [(ITERS + 1, *brick), (len(PAIRS), 8, Z), (4, *packed)],
        [sided, middle] + [sided] * 7,
        flops=20000000,
        vmem=12,
    )(wide, theta)
    first, second = (*GX, "gz_0"), (*GY, "gz_1")
    end_basis, dots = call(
        edges,
        [SMEM] + [VMEM] * 5,
        [(ITERS + 1, PER_GROUP, Y, Z), (lax.axis_size(first), 1, Z)],
        [(4, *packed), packed, (3, PER_GROUP, ROWS + 16, Z)] + [packed] * 7 + [(Z, Z)],
        flops=5000000,
    )(place_z, ends, far, chip, theta, sums)
    parts = exchange(dots, first)
    (copies,) = call(relay, [VMEM], [(lax.axis_size(second), 1, Z)])(parts)
    parts = exchange(copies, second)
    closing, mismatch = call(finish, [VMEM] * 5, [brick, brick])(
        parts, basis, end_basis, fields, theta
    )
    return closing, mismatch


def solution(mesh):
    pairs = [n for size in mesh.devices.shape for n in (size // 2, 2)]
    split = Mesh(mesh.devices.reshape(pairs), (*GX, *GY, *GZ))
    spec = P(GX, GY, GZ)
    return jax.shard_map(
        body, mesh=split, in_specs=(spec, spec, spec, P(), spec), out_specs=(spec, spec), check_vma=False
    )
```

```python
import jax
import jax.numpy as jnp
from jax import lax
from jax.experimental import pallas as pl
from jax.experimental.pallas import tpu as pltpu
from jax.sharding import Mesh
from jax.sharding import PartitionSpec as P

ITERS = 4
GX, GY, GZ = (("gx_0", "gx_1"), ("gy_0", "gy_1"), ("gz_0", "gz_1"))
F32 = jnp.float32
X, Y, Z = 8, 16, 128
HALO = ITERS + 1
WIDTHS = (5, 5, 4, 3)
PLANES = X + 2 * HALO
ROWS = 32
TOP = 8
SLAB_X = sum(WIDTHS)
AT_X = (0, 5, 10, 14)
AT_Y = (0, 90, 180, 244)
SLAB_Y = 288
GROUPS, PER_GROUP, GROUP = 4, 5, 32
LOW_AT, HIGH_AT = 5, 26
SCALE = 64.0
CHUNK = 4
PAIRS = [(i, j) for i in range(ITERS) for j in range(i, ITERS + 1)]
VMEM = pl.BlockSpec(memory_space=pltpu.VMEM)
HBM = pl.BlockSpec(memory_space=pltpu.HBM)
SMEM = pl.BlockSpec(memory_space=pltpu.SMEM)


def planes_of(k):
    return range(HALO - WIDTHS[k], PLANES - HALO + WIDTHS[k])


def call(kernel, ins, outs, scratch=(), flops=100000, vmem=8):
    return pl.pallas_call(
        kernel,
        in_specs=ins,
        out_specs=[VMEM] * len(outs),
        out_shape=[jax.ShapeDtypeStruct(s, F32) for s in outs],
        scratch_shapes=[pltpu.VMEM(s, F32) if isinstance(s, tuple) else s for s in scratch],
        compiler_params=pltpu.CompilerParams(vmem_limit_bytes=vmem * 2**20),
        cost_estimate=pl.CostEstimate(flops=flops, bytes_accessed=1000000, transcendentals=0),
    )


def prepare(
    place_x, opening_at, source_at, category_at, flags_at, table_at, fields, near, far, theta,
    opening, source, category, flags, table, arrived,
):
    copies = [
        pltpu.make_async_copy(a, b, arrived.at[n])
        for n, (a, b) in enumerate(
            (
                (table_at, table),
                (category_at, category),
                (flags_at, flags),
                (opening_at, opening),
                (source_at, source),
            )
        )
    ]
    for copy in copies:
        copy.start()
    for copy in copies:
        copy.wait()
    for k, shift in enumerate(shifts_of(table)):
        theta[k] = shift
    for p in range(X):
        kind = category[p]
        cond = jnp.full((Y, Z), table[0], F32)
        for n in range(1, table.shape[0]):
            cond = jnp.where(kind == n, table[n], cond)
        flag = flags[p].astype(F32)
        start = opening[p]
        values = (cond, start, 2.0 * source[p] - 6.0 * flag * start, flag)
        for k, v in enumerate(values):
            fields[k, p] = v
    first = place_x[0] == 0
    for k, w in enumerate(WIDTHS):
        for n in range(w):
            low, high = fields[k, n], fields[k, X - w + n]
            near[AT_X[k] + n] = jnp.where(first, high, low)
            far[AT_X[k] + n] = jnp.where(first, low, high)


def halo(place, far, pair, at, lower):
    far_side = (place == 0) if lower else (place == 1)
    return jnp.where(far_side, far[at], pair[(1 - place, *at)])


def plane(place, fields, far, pair, k, p, rows=slice(None)):
    if p < HALO:
        return halo(place, far, pair, (AT_X[k] + p - (HALO - WIDTHS[k]), rows), True)
    if p < HALO + X:
        return fields[k, p - HALO, rows]
    return halo(place, far, pair, (AT_X[k] + p - HALO - X, rows), False)


def slabs_y(place_x, place_y, fields, far_x, pair_x, near, far):
    first = place_y[0] == 0
    for k, w in enumerate(WIDTHS):
        for n, p in enumerate(planes_of(k)):
            to = pl.ds(AT_Y[k] + w * n, w)
            low, high = (
                plane(place_x[0], fields, far_x, pair_x, k, p, pl.ds(at, w)) for at in (0, Y - w)
            )
            near[to] = jnp.where(first, high, low)
            far[to] = jnp.where(first, low, high)


def assemble(place_x, place_y, place_z, fields, far_x, pair_x, far_y, pair_y, wide, near, far):
    lane = lax.broadcasted_iota(jnp.int32, (ROWS, Z), 1)
    first_core = place_z[0] == 0
    nothing = jnp.zeros((8, Z), F32)
    for k, w in enumerate(WIDTHS):
        for n, p in enumerate(planes_of(k)):
            at = (pl.ds(AT_Y[k] + w * n, w),)
            wide[k, p, 0:TOP] = nothing
            wide[k, p, TOP + Y : ROWS] = nothing
            wide[k, p, TOP : TOP + Y] = plane(place_x[0], fields, far_x, pair_x, k, p)
            wide[k, p, TOP - w : TOP] = halo(place_y[0], far_y, pair_y, at, True)
            wide[k, p, TOP + Y : TOP + Y + w] = halo(place_y[0], far_y, pair_y, at, False)
    for q in range(PER_GROUP):
        low = jnp.zeros((ROWS, Z), F32)
        high = low
        for g in range(GROUPS):
            p = PER_GROUP * g + q
            for k, w in enumerate(WIDTHS):
                if p in planes_of(k):
                    base = GROUP * g + AT_X[k]
                    turned = pltpu.roll(wide[k, p], base, 1)
                    place = lane if base else jnp.where(lane < Z // 2, lane, lane - Z)
                    low = jnp.where((place >= base) & (place < base + w), turned, low)
                    high = jnp.where((place >= base - w) & (place < base), turned, high)
        far[q] = jnp.where(first_core, low, high)
        near[q] = jnp.where(first_core, high, low)


def shifts_of(table):
    values = [jnp.full((8, Z), table[n], F32) for n in range(table.shape[0])]
    least, most, mean = values[0], values[0], values[0]
    for v in values[1:]:
        least, most, mean = jnp.minimum(least, v), jnp.maximum(most, v), mean + v
    mean = mean * (1.0 / len(values))
    top = 4.0 + 16.0 * most + 16.0 * mean
    low = 2.0 + 8.0 * least + 8.0 * mean
    middle, half = 0.5 * (top + low), 0.5 * (top - low)
    return [
        (middle + half * c) * (1.0 / SCALE) for c in (0.9238795, -0.9238795, 0.3826834, -0.3826834)
    ]


def smooth(mid, ahead, here, behind, first, count):
    n = here.shape[0]
    mid[0:n, 8 : 8 + ROWS] = (ahead + here) + (here + behind)
    sides = mid[0:n, pl.ds(7 + first, count)] + mid[0:n, pl.ds(9 + first, count)]
    rows = mid[0:n, pl.ds(8 + first, count)] + 0.5 * sides
    return rows + 0.5 * (pltpu.roll(rows, 1, 2) + pltpu.roll(rows, Z - 1, 2))


def newton_step(slope, diag, inside, shift, v, tv, tu):
    return ((diag - shift) * v - (slope * tv + tu)) * inside


def chunks(low, high, most):
    count = -(-(high - low) // most)
    size = -(-(high - low) // count)
    return [(p, min(p + size, high)) for p in range(low, high, size)]


def interior(wide, theta, basis, sums, ends, cx, mid, slope, diag, inside, va, vb, ua, ub):
    lane = lax.broadcasted_iota(jnp.int32, (ROWS, Z), 1)
    slots = mid.shape[0]
    slot = [0]

    def along(ref, p, q, first=0, count=ROWS):
        slot[0] += 1
        return smooth(
            mid.at[slot[0] % slots], ref[p - 1 : q - 1], ref[p:q], ref[p + 1 : q + 1], first, count
        )

    cond, start, rest, flag = (wide.at[k] for k in range(4))
    cx[...] = cond[...] * start[...]
    for p, q in chunks(1, PLANES - 1, CHUNK):
        tc, tx, tcx = (along(ref, p, q) for ref in (cond, start, cx))
        c = cond[p:q]
        near = 16.0 * c + tc
        diag[p:q] = (1.0 + 6.0 * flag[p:q] + near) * (1.0 / SCALE)
        half_c = c * (1.0 / SCALE)
        slope[p:q] = half_c
        there = jnp.where(c > 0.0, 1.0, 0.0)
        inside[p:q] = there
        r = (rest[p:q] - near * start[p:q] + (c * tx + tcx)) * there
        va[p:q] = r
        ua[p:q] = r * half_c
    basis[0] = va[HALO : HALO + X, TOP : TOP + Y]
    for k in range(ITERS):
        v_old, u_old, v_new, u_new = (va, ua, vb, ub) if k % 2 == 0 else (vb, ub, va, ua)
        last = k + 1 == ITERS
        first, count = (TOP, Y) if last else (0, ROWS)
        rows = pl.ds(first, count)
        shift = jnp.tile(theta[k], (count // 8, 1))[None]
        for p, q in chunks(2 + k, PLANES - 2 - k, CHUNK):
            tv, tu = along(v_old, p, q, first, count), along(u_old, p, q, first, count)
            v = newton_step(slope[p:q, rows], diag[p:q, rows], inside[p:q, rows], shift, v_old[p:q, rows], tv, tu)
            if last:
                basis[k + 1, p - HALO : q - HALO] = v
            else:
                v_new[p:q] = v
                u_new[p:q] = v * slope[p:q]
        if not last:
            basis[k + 1] = v_new[HALO : HALO + X, TOP : TOP + Y]

    inner = (lane[:8] >= HALO) & (lane[:8] < Z - HALO)
    for n, (i, j) in enumerate(PAIRS):
        total = None
        for p in range(X):
            for half in (0, 8):
                rows = pl.ds(half, 8)
                term = basis[i, p, rows] * basis[j, p, rows]
                total = term if total is None else total + term
        sums[n] = jnp.where(inner, total, 0.0)

    place = lane % GROUP
    for k in range(4):
        for q in range(PER_GROUP):
            out = jnp.zeros((ROWS, Z), F32)
            for g in range(GROUPS):
                p = PER_GROUP * g + q
                if p in planes_of(k):
                    mine = (lane // GROUP) == g
                    low = pltpu.roll(wide[k, p], GROUP * g + LOW_AT, 1)
                    high = pltpu.roll(wide[k, p], (GROUP * g + HIGH_AT) % Z, 1)
                    low_here = mine & (place >= LOW_AT) & (place < LOW_AT + 2 * HALO)
                    high_here = mine & (place >= HIGH_AT - 2 * HALO) & (place < HIGH_AT)
                    out = jnp.where(low_here, low, jnp.where(high_here, high, out))
            ends[k, q] = out


def edges(place_z, ends, far, chip, theta, inner_sums, basis, dots, cells, cx, mid, slope, diag, inside, va, vb, ua, ub, stack):
    lane = lax.broadcasted_iota(jnp.int32, (ROWS, Z), 1)
    place = lane % GROUP
    slots = mid.shape[0]
    slot = [0]

    for q in range(PER_GROUP):
        below, above = (halo(place_z[0], far, chip, (q,), lower) for lower in (True, False))
        for k in range(4):
            low = pltpu.roll(below, (LOW_AT - AT_X[k]) % Z, 1)
            high = pltpu.roll(above, (HIGH_AT - AT_X[k]) % Z, 1)
            out = jnp.where(place < LOW_AT, low, ends[k, q])
            cells[k, q] = jnp.where((place >= HIGH_AT) & (place < HIGH_AT + HALO), high, out)

    def along(ref, first=0, count=ROWS):
        slot[0] += 1
        here = ref[...]
        before = pltpu.roll(ref[PER_GROUP - 1], GROUP, 1)[None]
        after = pltpu.roll(ref[0], Z - GROUP, 1)[None]
        return smooth(
            mid.at[slot[0] % slots],
            jnp.concatenate([before, ref[: PER_GROUP - 1]]),
            here,
            jnp.concatenate([ref[1:], after]),
            first,
            count,
        )

    cond, start, rest, flag = (cells.at[k] for k in range(4))
    cx[...] = cond[...] * start[...]
    tc, tx, tcx = (along(ref) for ref in (cond, start, cx))
    c = cond[...]
    near = 16.0 * c + tc
    diag[...] = (1.0 + 6.0 * flag[...] + near) * (1.0 / SCALE)
    half_c = c * (1.0 / SCALE)
    slope[...] = half_c
    there = jnp.where(c > 0.0, 1.0, 0.0)
    inside[...] = there
    r = (rest[...] - near * start[...] + (c * tx + tcx)) * there
    va[...] = r
    ua[...] = r * half_c
    basis[0] = r[:, TOP : TOP + Y]
    for k in range(ITERS):
        v_old, u_old, v_new, u_new = (va, ua, vb, ub) if k % 2 == 0 else (vb, ub, va, ua)
        last = k + 1 == ITERS
        first, count = (TOP, Y) if last else (0, ROWS)
        rows = pl.ds(first, count)
        shift = jnp.tile(theta[k], (count // 8, 1))[None]
        tv, tu = along(v_old, first, count), along(u_old, first, count)
        v = newton_step(slope[:, rows], diag[:, rows], inside[:, rows], shift, v_old[:, rows], tv, tu)
        if not last:
            v_new[...] = v
            u_new[...] = v * slope[...]
        basis[k + 1] = v if last else v[:, TOP : TOP + Y]

    end_cells = ((place >= LOW_AT) & (place < LOW_AT + HALO)) | ((place >= HIGH_AT - HALO) & (place < HIGH_AT))
    mine = []
    for q in range(PER_GROUP):
        own = [g for g in range(GROUPS) if HALO <= PER_GROUP * g + q < HALO + X]
        at = (lane >= GROUP * own[0]) & (lane < GROUP * (own[-1] + 1))
        mine.append(jnp.where(at & end_cells, 1.0, 0.0)[:8])
    for n in range(16):
        total = None
        if n < len(PAIRS):
            i, j = PAIRS[n]
            total = inner_sums[n]
            for q in range(PER_GROUP):
                for half in (0, 8):
                    rows = pl.ds(half, 8)
                    total = total + (basis[i, q, rows] * mine[q]) * basis[j, q, rows]
        else:
            total = jnp.zeros((8, Z), F32)
        stack[pl.ds(8 * n, 8)] = total
    by_sum = stack[pl.ds(0, 16, stride=8)]
    for n in range(1, 8):
        by_sum = by_sum + stack[pl.ds(n, 16, stride=8)]
    total = lax.dot_general(
        jnp.ones((8, Z), F32), jnp.tile(by_sum, (8, 1)), (((1,), (1,)), ((), ())),
        precision=lax.Precision.HIGHEST, preferred_element_type=F32,
    )
    for n in range(dots.shape[0]):
        dots[n] = total[0:1]


def two_sum(a, b):
    s = a + b
    t = s - a
    return s, (a - (s - t)) + (b - t)


def row_sum(parts):
    rows = [(parts[n], None) for n in range(parts.shape[0])]
    while len(rows) > 1:
        pairs, rows = zip(rows[::2], rows[1::2]), []
        for (a, ea), (b, eb) in pairs:
            s, e = two_sum(a, b)
            rows.append((s, e if ea is None else e + (ea + eb)))
    return rows[0]


def relay(parts, copies):
    total, rest = row_sum(parts)
    lane = lax.broadcasted_iota(jnp.int32, total.shape, 1)
    total = jnp.where(lane < 16, total, rest)
    for n in range(copies.shape[0]):
        copies[n] = total


def quick(a, b):
    s = a + b
    return s, b - (s - a)


def halves(a):
    t = 4097.0 * a
    high = t - (t - a)
    return high, a - high


def plus(a, b):
    s, e = two_sum(a[0], b[0])
    return quick(s, e + (a[1] + b[1]))


def minus(a, b):
    return plus(a, (-b[0], -b[1]))


def times(a, b):
    p = a[0] * b[0]
    ah, al = halves(a[0])
    bh, bl = halves(b[0])
    e = ((ah * bh - p) + ah * bl + al * bh) + al * bl
    return quick(p, e + (a[0] * b[1] + a[1] * b[0]))


def reciprocal(a):
    q = 1.0 / a[0]
    qh, ql = halves(q)
    ah, al = halves(a[0])
    p = q * a[0]
    rest = ((1.0 - p) - (((qh * ah - p) + qh * al + ql * ah) + ql * al)) - q * a[1]
    return quick(q, q * rest)


def coefficients(gram, theta):
    none = jnp.zeros_like(theta[0])
    shift = [(t, none) for t in theta]
    system = [
        [plus(gram[i, j + 1], times(shift[j], gram[i, j])) for j in range(i + 1)]
        for i in range(ITERS)
    ]
    right = [gram[i, 0] for i in range(ITERS)]
    lower, inverse = {}, []
    for j in range(ITERS):
        inverse.append(reciprocal(system[j][j]))
        for i in range(j + 1, ITERS):
            lower[i, j] = times(system[i][j], inverse[j])
        for i in range(j + 1, ITERS):
            for k in range(j + 1, i + 1):
                system[i][k] = minus(system[i][k], times(lower[i, j], system[k][j]))
            right[i] = minus(right[i], times(lower[i, j], right[j]))
    y = [None] * ITERS
    for i in reversed(range(ITERS)):
        y[i] = times(right[i], inverse[i])
        for k in reversed(range(i + 1, ITERS)):
            y[i] = minus(y[i], times(lower[k, i], y[k]))
    r = [minus((none + 1.0, none), times(shift[0], y[0]))]
    for k in range(1, ITERS):
        total = plus(y[k - 1], times(shift[k], y[k]))
        r.append((-total[0], -total[1]))
    r.append((-y[-1][0], -y[-1][1]))
    return [a[0] * (1.0 / SCALE) for a in y], [a[0] for a in r]


def finish(parts, basis, end_basis, fields, theta, closing, mismatch):
    total, rest = row_sum(parts)
    rest = rest + pltpu.roll(total, Z - 16, 1)
    gram = {}
    for n, (i, j) in enumerate(PAIRS):
        gram[i, j] = gram[j, i] = quick(
            *(jnp.broadcast_to(v[0:1, n : n + 1], (8, Z)) for v in (total, rest))
        )
    y, r = coefficients(gram, [theta[k] for k in range(ITERS)])

    def combine(v):
        x, m = y[0] * v[0], r[ITERS] * v[ITERS]
        for k in range(1, ITERS):
            x = x + y[k] * v[k]
        for k in range(ITERS):
            m = m + r[k] * v[k]
        return x, m

    lane = lax.broadcasted_iota(jnp.int32, (8, Z), 1)
    for half in (0, 8):
        rows = pl.ds(half, 8)
        ends = [
            combine([end_basis[k, q, rows] for k in range(ITERS + 1)]) for q in range(PER_GROUP)
        ]
        for p in range(X):
            g, q = divmod(p + HALO, PER_GROUP)
            inner = combine([basis[k, p, rows] for k in range(ITERS + 1)])
            both = []
            for value, end in zip(inner, ends[q]):
                low = pltpu.roll(end, (Z - GROUP * g - LOW_AT) % Z, 1)
                high = pltpu.roll(end, (Z - GROUP * g - HIGH_AT) % Z, 1)
                value = jnp.where(lane < HALO, low, value)
                both.append(jnp.where(lane >= Z - HALO, high, value))
            closing[p, rows] = fields[1, p, rows] + both[0]
            mismatch[p, rows] = both[1]


def trade(near, far, axes):
    ends = lax.axis_size(axes) - 1
    others = [p for i in range(1, ends, 2) for p in ((i, i + 1), (i + 1, i))]
    return lax.ppermute(far, axes, others), lax.all_gather(near, axes[1], axis=0)


def exchange(copies, axes):
    return lax.all_to_all(copies, axes, split_axis=0, concat_axis=0, tiled=True)


def body(opening, source, category, table, flags):
    brick = (X, Y, Z)
    place_x, place_y, place_z = (lax.axis_index(axes[1]).reshape(1) for axes in (GX, GY, GZ))
    whole = pltpu.VMEM(brick, jnp.int32)
    fields, near, far, theta = call(
        prepare,
        [SMEM] + [HBM] * 5,
        [(4, *brick), (SLAB_X, Y, Z), (SLAB_X, Y, Z), (ITERS, 8, Z)],
        [brick, brick, whole, whole, pltpu.SMEM(table.shape, F32), pltpu.SemaphoreType.DMA((5,))],
    )(
        place_x,
        *(
            pltpu.with_memory_space_constraint(a, pltpu.HBM)
            for a in (opening, source, category, flags, table)
        ),
    )
    by_x = trade(near, far, GX)
    near, far = call(slabs_y, [SMEM] * 2 + [VMEM] * 3, [(SLAB_Y, Z)] * 2)(
        place_x, place_y, fields, *by_x
    )
    by_y = trade(near, far, GY)
    packed = (PER_GROUP, ROWS, Z)
    wide, near, far = call(assemble, [SMEM] * 3 + [VMEM] * 5, [(4, PLANES, ROWS, Z), packed, packed])(
        place_x, place_y, place_z, fields, *by_x, *by_y
    )
    far, chip = trade(near, far, GZ)
    sided = (PLANES, ROWS, Z)
    middle = (3, PLANES, ROWS + 16, Z)
    basis, sums, ends = call(
        interior,
        [VMEM] * 2,
        [(ITERS + 1, *brick), (len(PAIRS), 8, Z), (4, *packed)],
        [sided, middle] + [sided] * 7,
        flops=20000000,
        vmem=12,
    )(wide, theta)
    first, second = (*GX, "gz_0"), (*GY, "gz_1")
    end_basis, dots = call(
        edges,
        [SMEM] + [VMEM] * 5,
        [(ITERS + 1, PER_GROUP, Y, Z), (lax.axis_size(first), 1, Z)],
        [(4, *packed), packed, (3, PER_GROUP, ROWS + 16, Z)] + [packed] * 7 + [(Z, Z)],
        flops=5000000,
    )(place_z, ends, far, chip, theta, sums)
    parts = exchange(dots, first)
    (copies,) = call(relay, [VMEM], [(lax.axis_size(second), 1, Z)])(parts)
    parts = exchange(copies, second)
    closing, mismatch = call(finish, [VMEM] * 5, [brick, brick])(
        parts, basis, end_basis, fields, theta
    )
    return closing, mismatch


def solution(mesh):
    pairs = [n for size in mesh.devices.shape for n in (size // 2, 2)]
    split = Mesh(mesh.devices.reshape(pairs), (*GX, *GY, *GZ))
    spec = P(GX, GY, GZ)
    return jax.shard_map(
        body, mesh=split, in_specs=(spec, spec, spec, P(), spec), out_specs=(spec, spec), check_vma=False
    )
```

```python
import jax
import jax.numpy as jnp
from jax import lax
from jax.experimental import pallas as pl
from jax.experimental.pallas import tpu as pltpu
from jax.sharding import Mesh
from jax.sharding import PartitionSpec as P

ITERS = 4
GX, GY, GZ = (("gx_0", "gx_1"), ("gy_0", "gy_1"), ("gz_0", "gz_1"))
F32 = jnp.float32
X, Y, Z = 8, 16, 128
HALO = ITERS + 1
WIDTHS = (5, 5, 4, 3)
PLANES = X + 2 * HALO
ROWS = 32
TOP = 8
SLAB_X = sum(WIDTHS)
AT_X = (0, 5, 10, 14)
AT_Y = (0, 90, 180, 244)
SLAB_Y = 288
GROUPS, PER_GROUP, GROUP = 4, 5, 32
LOW_AT, HIGH_AT = 5, 26
SCALE = 64.0
CHUNK = 4
PAIRS = [(i, j) for i in range(ITERS) for j in range(i, ITERS + 1)]
VMEM = pl.BlockSpec(memory_space=pltpu.VMEM)
HBM = pl.BlockSpec(memory_space=pltpu.HBM)
SMEM = pl.BlockSpec(memory_space=pltpu.SMEM)


def planes_of(k):
    return range(HALO - WIDTHS[k], PLANES - HALO + WIDTHS[k])


def call(kernel, ins, outs, scratch=(), flops=100000, vmem=8):
    return pl.pallas_call(
        kernel,
        in_specs=ins,
        out_specs=[VMEM] * len(outs),
        out_shape=[jax.ShapeDtypeStruct(s, F32) for s in outs],
        scratch_shapes=[pltpu.VMEM(s, F32) if isinstance(s, tuple) else s for s in scratch],
        compiler_params=pltpu.CompilerParams(vmem_limit_bytes=vmem * 2**20),
        cost_estimate=pl.CostEstimate(flops=flops, bytes_accessed=1000000, transcendentals=0),
    )


def prepare(
    place_x, opening_at, source_at, category_at, flags_at, table_at, fields, near, far, theta,
    opening, source, category, flags, table, arrived,
):
    copies = [
        pltpu.make_async_copy(a, b, arrived.at[n])
        for n, (a, b) in enumerate(
            (
                (table_at, table),
                (category_at, category),
                (flags_at, flags),
                (opening_at, opening),
                (source_at, source),
            )
        )
    ]
    for copy in copies:
        copy.start()
    for copy in copies:
        copy.wait()
    for k, shift in enumerate(shifts_of(table)):
        theta[k] = shift
    for p in range(X):
        kind = category[p]
        cond = jnp.full((Y, Z), table[0], F32)
        for n in range(1, table.shape[0]):
            cond = jnp.where(kind == n, table[n], cond)
        flag = flags[p].astype(F32)
        start = opening[p]
        values = (cond, start, 2.0 * source[p] - 6.0 * flag * start, flag)
        for k, v in enumerate(values):
            fields[k, p] = v
    first = place_x[0] == 0
    for k, w in enumerate(WIDTHS):
        for n in range(w):
            low, high = fields[k, n], fields[k, X - w + n]
            near[AT_X[k] + n] = jnp.where(first, high, low)
            far[AT_X[k] + n] = jnp.where(first, low, high)


def halo(place, far, pair, at, lower):
    far_side = (place == 0) if lower else (place == 1)
    return jnp.where(far_side, far[at], pair[(1 - place, *at)])


def plane(place, fields, far, pair, k, p, rows=slice(None)):
    if p < HALO:
        return halo(place, far, pair, (AT_X[k] + p - (HALO - WIDTHS[k]), rows), True)
    if p < HALO + X:
        return fields[k, p - HALO, rows]
    return halo(place, far, pair, (AT_X[k] + p - HALO - X, rows), False)


def slabs_y(place_x, place_y, fields, far_x, pair_x, near, far):
    first = place_y[0] == 0
    for k, w in enumerate(WIDTHS):
        for n, p in enumerate(planes_of(k)):
            to = pl.ds(AT_Y[k] + w * n, w)
            low, high = (
                plane(place_x[0], fields, far_x, pair_x, k, p, pl.ds(at, w)) for at in (0, Y - w)
            )
            near[to] = jnp.where(first, high, low)
            far[to] = jnp.where(first, low, high)


def assemble(place_x, place_y, place_z, fields, far_x, pair_x, far_y, pair_y, wide, near, far):
    lane = lax.broadcasted_iota(jnp.int32, (ROWS, Z), 1)
    first_core = place_z[0] == 0
    nothing = jnp.zeros((8, Z), F32)
    for k, w in enumerate(WIDTHS):
        for n, p in enumerate(planes_of(k)):
            at = (pl.ds(AT_Y[k] + w * n, w),)
            wide[k, p, 0:TOP] = nothing
            wide[k, p, TOP + Y : ROWS] = nothing
            wide[k, p, TOP : TOP + Y] = plane(place_x[0], fields, far_x, pair_x, k, p)
            wide[k, p, TOP - w : TOP] = halo(place_y[0], far_y, pair_y, at, True)
            wide[k, p, TOP + Y : TOP + Y + w] = halo(place_y[0], far_y, pair_y, at, False)
    for q in range(PER_GROUP):
        low = jnp.zeros((ROWS, Z), F32)
        high = low
        for g in range(GROUPS):
            p = PER_GROUP * g + q
            for k, w in enumerate(WIDTHS):
                if p in planes_of(k):
                    base = GROUP * g + AT_X[k]
                    turned = pltpu.roll(wide[k, p], base, 1)
                    place = lane if base else jnp.where(lane < Z // 2, lane, lane - Z)
                    low = jnp.where((place >= base) & (place < base + w), turned, low)
                    high = jnp.where((place >= base - w) & (place < base), turned, high)
        far[q] = jnp.where(first_core, low, high)
        near[q] = jnp.where(first_core, high, low)


def shifts_of(table):
    values = [jnp.full((8, Z), table[n], F32) for n in range(table.shape[0])]
    least, most, mean = values[0], values[0], values[0]
    for v in values[1:]:
        least, most, mean = jnp.minimum(least, v), jnp.maximum(most, v), mean + v
    mean = mean * (1.0 / len(values))
    top = 4.0 + 16.0 * most + 16.0 * mean
    low = 2.0 + 8.0 * least + 8.0 * mean
    middle, half = 0.5 * (top + low), 0.5 * (top - low)
    return [
        (middle + half * c) * (1.0 / SCALE) for c in (0.9238795, -0.9238795, 0.3826834, -0.3826834)
    ]


def smooth(mid, ahead, here, behind, first, count):
    n = here.shape[0]
    mid[0:n, 8 : 8 + ROWS] = (ahead + here) + (here + behind)
    sides = mid[0:n, pl.ds(7 + first, count)] + mid[0:n, pl.ds(9 + first, count)]
    rows = mid[0:n, pl.ds(8 + first, count)] + 0.5 * sides
    return rows + 0.5 * (pltpu.roll(rows, 1, 2) + pltpu.roll(rows, Z - 1, 2))


def newton_step(slope, diag, inside, shift, v, tv, tu):
    return ((diag - shift) * v - (slope * tv + tu)) * inside


def chunks(low, high, most):
    count = -(-(high - low) // most)
    size = -(-(high - low) // count)
    return [(p, min(p + size, high)) for p in range(low, high, size)]


def interior(wide, theta, basis, sums, ends, cx, mid, slope, diag, inside, va, vb, ua, ub):
    lane = lax.broadcasted_iota(jnp.int32, (ROWS, Z), 1)
    slots = mid.shape[0]
    slot = [0]

    def along(ref, p, q, first=0, count=ROWS):
        slot[0] += 1
        return smooth(
            mid.at[slot[0] % slots], ref[p - 1 : q - 1], ref[p:q], ref[p + 1 : q + 1], first, count
        )

    cond, start, rest, flag = (wide.at[k] for k in range(4))
    cx[...] = cond[...] * start[...]
    for p, q in chunks(1, PLANES - 1, CHUNK):
        tc, tx, tcx = (along(ref, p, q) for ref in (cond, start, cx))
        c = cond[p:q]
        near = 16.0 * c + tc
        diag[p:q] = (1.0 + 6.0 * flag[p:q] + near) * (1.0 / SCALE)
        half_c = c * (1.0 / SCALE)
        slope[p:q] = half_c
        there = jnp.where(c > 0.0, 1.0, 0.0)
        inside[p:q] = there
        r = (rest[p:q] - near * start[p:q] + (c * tx + tcx)) * there
        va[p:q] = r
        ua[p:q] = r * half_c
    basis[0] = va[HALO : HALO + X, TOP : TOP + Y]
    for k in range(ITERS):
        v_old, u_old, v_new, u_new = (va, ua, vb, ub) if k % 2 == 0 else (vb, ub, va, ua)
        last = k + 1 == ITERS
        first, count = (TOP, Y) if last else (0, ROWS)
        rows = pl.ds(first, count)
        shift = jnp.tile(theta[k], (count // 8, 1))[None]
        for p, q in chunks(2 + k, PLANES - 2 - k, CHUNK):
            tv, tu = along(v_old, p, q, first, count), along(u_old, p, q, first, count)
            v = newton_step(slope[p:q, rows], diag[p:q, rows], inside[p:q, rows], shift, v_old[p:q, rows], tv, tu)
            if last:
                basis[k + 1, p - HALO : q - HALO] = v
            else:
                v_new[p:q] = v
                u_new[p:q] = v * slope[p:q]
        if not last:
            basis[k + 1] = v_new[HALO : HALO + X, TOP : TOP + Y]

    inner = (lane[:8] >= HALO) & (lane[:8] < Z - HALO)
    for n, (i, j) in enumerate(PAIRS):
        total = None
        for p in range(X):
            for half in (0, 8):
                rows = pl.ds(half, 8)
                term = basis[i, p, rows] * basis[j, p, rows]
                total = term if total is None else total + term
        sums[n] = jnp.where(inner, total, 0.0)

    place = lane % GROUP
    for k in range(4):
        for q in range(PER_GROUP):
            out = jnp.zeros((ROWS, Z), F32)
            for g in range(GROUPS):
                p = PER_GROUP * g + q
                if p in planes_of(k):
                    mine = (lane // GROUP) == g
                    low = pltpu.roll(wide[k, p], GROUP * g + LOW_AT, 1)
                    high = pltpu.roll(wide[k, p], (GROUP * g + HIGH_AT) % Z, 1)
                    low_here = mine & (place >= LOW_AT) & (place < LOW_AT + 2 * HALO)
                    high_here = mine & (place >= HIGH_AT - 2 * HALO) & (place < HIGH_AT)
                    out = jnp.where(low_here, low, jnp.where(high_here, high, out))
            ends[k, q] = out


def edges(place_z, ends, far, chip, theta, inner_sums, basis, dots, cells, cx, mid, slope, diag, inside, va, vb, ua, ub, stack):
    lane = lax.broadcasted_iota(jnp.int32, (ROWS, Z), 1)
    place = lane % GROUP
    slots = mid.shape[0]
    slot = [0]

    for q in range(PER_GROUP):
        below, above = (halo(place_z[0], far, chip, (q,), lower) for lower in (True, False))
        for k in range(4):
            low = pltpu.roll(below, (LOW_AT - AT_X[k]) % Z, 1)
            high = pltpu.roll(above, (HIGH_AT - AT_X[k]) % Z, 1)
            out = jnp.where(place < LOW_AT, low, ends[k, q])
            cells[k, q] = jnp.where((place >= HIGH_AT) & (place < HIGH_AT + HALO), high, out)

    def along(ref, first=0, count=ROWS):
        slot[0] += 1
        here = ref[...]
        before = pltpu.roll(ref[PER_GROUP - 1], GROUP, 1)[None]
        after = pltpu.roll(ref[0], Z - GROUP, 1)[None]
        return smooth(
            mid.at[slot[0] % slots],
            jnp.concatenate([before, ref[: PER_GROUP - 1]]),
            here,
            jnp.concatenate([ref[1:], after]),
            first,
            count,
        )

    cond, start, rest, flag = (cells.at[k] for k in range(4))
    cx[...] = cond[...] * start[...]
    tc, tx, tcx = (along(ref) for ref in (cond, start, cx))
    c = cond[...]
    near = 16.0 * c + tc
    diag[...] = (1.0 + 6.0 * flag[...] + near) * (1.0 / SCALE)
    half_c = c * (1.0 / SCALE)
    slope[...] = half_c
    there = jnp.where(c > 0.0, 1.0, 0.0)
    inside[...] = there
    r = (rest[...] - near * start[...] + (c * tx + tcx)) * there
    va[...] = r
    ua[...] = r * half_c
    basis[0] = r[:, TOP : TOP + Y]
    for k in range(ITERS):
        v_old, u_old, v_new, u_new = (va, ua, vb, ub) if k % 2 == 0 else (vb, ub, va, ua)
        last = k + 1 == ITERS
        first, count = (TOP, Y) if last else (0, ROWS)
        rows = pl.ds(first, count)
        shift = jnp.tile(theta[k], (count // 8, 1))[None]
        tv, tu = along(v_old, first, count), along(u_old, first, count)
        v = newton_step(slope[:, rows], diag[:, rows], inside[:, rows], shift, v_old[:, rows], tv, tu)
        if not last:
            v_new[...] = v
            u_new[...] = v * slope[...]
        basis[k + 1] = v if last else v[:, TOP : TOP + Y]

    end_cells = ((place >= LOW_AT) & (place < LOW_AT + HALO)) | ((place >= HIGH_AT - HALO) & (place < HIGH_AT))
    mine = []
    for q in range(PER_GROUP):
        own = [g for g in range(GROUPS) if HALO <= PER_GROUP * g + q < HALO + X]
        at = (lane >= GROUP * own[0]) & (lane < GROUP * (own[-1] + 1))
        mine.append(jnp.where(at & end_cells, 1.0, 0.0)[:8])
    for n in range(16):
        total = None
        if n < len(PAIRS):
            i, j = PAIRS[n]
            total = inner_sums[n]
            for q in range(PER_GROUP):
                for half in (0, 8):
                    rows = pl.ds(half, 8)
                    total = total + (basis[i, q, rows] * mine[q]) * basis[j, q, rows]
        else:
            total = jnp.zeros((8, Z), F32)
        stack[pl.ds(8 * n, 8)] = total
    by_sum = stack[pl.ds(0, 16, stride=8)]
    for n in range(1, 8):
        by_sum = by_sum + stack[pl.ds(n, 16, stride=8)]
    total = lax.dot_general(
        jnp.ones((8, Z), F32), jnp.tile(by_sum, (8, 1)), (((1,), (1,)), ((), ())),
        precision=lax.Precision.HIGHEST, preferred_element_type=F32,
    )
    for n in range(dots.shape[0]):
        dots[n] = total[0:1]


def two_sum(a, b):
    s = a + b
    t = s - a
    return s, (a - (s - t)) + (b - t)


def row_sum(parts):
    rows = [(parts[n], None) for n in range(parts.shape[0])]
    while len(rows) > 1:
        pairs, rows = zip(rows[::2], rows[1::2]), []
        for (a, ea), (b, eb) in pairs:
            s, e = two_sum(a, b)
            rows.append((s, e if ea is None else e + (ea + eb)))
    return rows[0]


def relay(parts, copies):
    total, rest = row_sum(parts)
    lane = lax.broadcasted_iota(jnp.int32, total.shape, 1)
    total = jnp.where(lane < 16, total, rest)
    for n in range(copies.shape[0]):
        copies[n] = total


def quick(a, b):
    s = a + b
    return s, b - (s - a)


def halves(a):
    t = 4097.0 * a
    high = t - (t - a)
    return high, a - high


def plus(a, b):
    s, e = two_sum(a[0], b[0])
    return quick(s, e + (a[1] + b[1]))


def minus(a, b):
    return plus(a, (-b[0], -b[1]))


def times(a, b):
    p = a[0] * b[0]
    ah, al = halves(a[0])
    bh, bl = halves(b[0])
    e = ((ah * bh - p) + ah * bl + al * bh) + al * bl
    return quick(p, e + (a[0] * b[1] + a[1] * b[0]))


def reciprocal(a):
    q = 1.0 / a[0]
    qh, ql = halves(q)
    ah, al = halves(a[0])
    p = q * a[0]
    rest = ((1.0 - p) - (((qh * ah - p) + qh * al + ql * ah) + ql * al)) - q * a[1]
    return quick(q, q * rest)


def coefficients(gram, theta):
    none = jnp.zeros_like(theta[0])
    shift = [(t, none) for t in theta]
    system = [
        [plus(gram[i, j + 1], times(shift[j], gram[i, j])) for j in range(i + 1)]
        for i in range(ITERS)
    ]
    right = [gram[i, 0] for i in range(ITERS)]
    lower, inverse = {}, []
    for j in range(ITERS):
        inverse.append(reciprocal(system[j][j]))
        for i in range(j + 1, ITERS):
            lower[i, j] = times(system[i][j], inverse[j])
        for i in range(j + 1, ITERS):
            for k in range(j + 1, i + 1):
                system[i][k] = minus(system[i][k], times(lower[i, j], system[k][j]))
            right[i] = minus(right[i], times(lower[i, j], right[j]))
    y = [None] * ITERS
    for i in reversed(range(ITERS)):
        y[i] = times(right[i], inverse[i])
        for k in reversed(range(i + 1, ITERS)):
            y[i] = minus(y[i], times(lower[k, i], y[k]))
    r = [minus((none + 1.0, none), times(shift[0], y[0]))]
    for k in range(1, ITERS):
        total = plus(y[k - 1], times(shift[k], y[k]))
        r.append((-total[0], -total[1]))
    r.append((-y[-1][0], -y[-1][1]))
    return [a[0] * (1.0 / SCALE) for a in y], [a[0] for a in r]


def finish(parts, basis, end_basis, fields, theta, closing, mismatch):
    total, rest = row_sum(parts)
    rest = rest + pltpu.roll(total, Z - 16, 1)
    gram = {}
    for n, (i, j) in enumerate(PAIRS):
        gram[i, j] = gram[j, i] = quick(
            *(jnp.broadcast_to(v[0:1, n : n + 1], (8, Z)) for v in (total, rest))
        )
    y, r = coefficients(gram, [theta[k] for k in range(ITERS)])

    def combine(v):
        x, m = y[0] * v[0], r[ITERS] * v[ITERS]
        for k in range(1, ITERS):
            x = x + y[k] * v[k]
        for k in range(ITERS):
            m = m + r[k] * v[k]
        return x, m

    lane = lax.broadcasted_iota(jnp.int32, (8, Z), 1)
    for half in (0, 8):
        rows = pl.ds(half, 8)
        ends = [
            combine([end_basis[k, q, rows] for k in range(ITERS + 1)]) for q in range(PER_GROUP)
        ]
        for p in range(X):
            g, q = divmod(p + HALO, PER_GROUP)
            inner = combine([basis[k, p, rows] for k in range(ITERS + 1)])
            both = []
            for value, end in zip(inner, ends[q]):
                low = pltpu.roll(end, (Z - GROUP * g - LOW_AT) % Z, 1)
                high = pltpu.roll(end, (Z - GROUP * g - HIGH_AT) % Z, 1)
                value = jnp.where(lane < HALO, low, value)
                both.append(jnp.where(lane >= Z - HALO, high, value))
            closing[p, rows] = fields[1, p, rows] + both[0]
            mismatch[p, rows] = both[1]


def trade(near, far, axes):
    ends = lax.axis_size(axes) - 1
    others = [p for i in range(1, ends, 2) for p in ((i, i + 1), (i + 1, i))]
    return lax.ppermute(far, axes, others), lax.all_gather(near, axes[1], axis=0)


def exchange(copies, axes):
    return lax.all_to_all(copies, axes, split_axis=0, concat_axis=0, tiled=True)


def body(opening, source, category, table, flags):
    brick = (X, Y, Z)
    place_x, place_y, place_z = (lax.axis_index(axes[1]).reshape(1) for axes in (GX, GY, GZ))
    whole = pltpu.VMEM(brick, jnp.int32)
    fields, near, far, theta = call(
        prepare,
        [SMEM] + [HBM] * 5,
        [(4, *brick), (SLAB_X, Y, Z), (SLAB_X, Y, Z), (ITERS, 8, Z)],
        [brick, brick, whole, whole, pltpu.SMEM(table.shape, F32), pltpu.SemaphoreType.DMA((5,))],
    )(
        place_x,
        *(
            pltpu.with_memory_space_constraint(a, pltpu.HBM)
            for a in (opening, source, category, flags, table)
        ),
    )
    by_x = trade(near, far, GX)
    near, far = call(slabs_y, [SMEM] * 2 + [VMEM] * 3, [(SLAB_Y, Z)] * 2)(
        place_x, place_y, fields, *by_x
    )
    by_y = trade(near, far, GY)
    packed = (PER_GROUP, ROWS, Z)
    wide, near, far = call(assemble, [SMEM] * 3 + [VMEM] * 5, [(4, PLANES, ROWS, Z), packed, packed])(
        place_x, place_y, place_z, fields, *by_x, *by_y
    )
    far, chip = trade(near, far, GZ)
    sided = (PLANES, ROWS, Z)
    middle = (3, PLANES, ROWS + 16, Z)
    basis, sums, ends = call(
        interior,
        [VMEM] * 2,
        [(ITERS + 1, *brick), (len(PAIRS), 8, Z), (4, *packed)],
        [sided, middle] + [sided] * 7,
        flops=20000000,
        vmem=12,
    )(wide, theta)
    first, second = (*GY, "gz_1"), (*GX, "gz_0")
    end_basis, dots = call(
        edges,
        [SMEM] + [VMEM] * 5,
        [(ITERS + 1, PER_GROUP, Y, Z), (lax.axis_size(first), 1, Z)],
        [(4, *packed), packed, (3, PER_GROUP, ROWS + 16, Z)] + [packed] * 7 + [(Z, Z)],
        flops=5000000,
    )(place_z, ends, far, chip, theta, sums)
    parts = exchange(dots, first)
    (copies,) = call(relay, [VMEM], [(lax.axis_size(second), 1, Z)])(parts)
    parts = exchange(copies, second)
    closing, mismatch = call(finish, [VMEM] * 5, [brick, brick])(
        parts, basis, end_basis, fields, theta
    )
    return closing, mismatch


def solution(mesh):
    pairs = [n for size in mesh.devices.shape for n in (size // 2, 2)]
    split = Mesh(mesh.devices.reshape(pairs), (*GX, *GY, *GZ))
    spec = P(GX, GY, GZ)
    return jax.shard_map(
        body, mesh=split, in_specs=(spec, spec, spec, P(), spec), out_specs=(spec, spec), check_vma=False
    )
```

```python
import jax
import jax.numpy as jnp
from jax import lax
from jax.experimental import pallas as pl
from jax.experimental.pallas import tpu as pltpu
from jax.sharding import Mesh
from jax.sharding import PartitionSpec as P

ITERS = 4
GX, GY, GZ = (("gx_0", "gx_1"), ("gy_0", "gy_1"), ("gz_0", "gz_1"))
F32 = jnp.float32
X, Y, Z = 8, 16, 128
HALO = ITERS + 1
WIDTHS = (5, 5, 4, 3)
PLANES = X + 2 * HALO
ROWS = 32
TOP = 8
SLAB_X = sum(WIDTHS)
AT_X = (0, 5, 10, 14)
AT_Y = (0, 90, 180, 244)
SLAB_Y = 288
GROUPS, PER_GROUP, GROUP = 4, 5, 32
LOW_AT, HIGH_AT = 5, 26
SCALE = 64.0
CHUNK = 4
PAIRS = [(i, j) for i in range(ITERS) for j in range(i, ITERS + 1)]
VMEM = pl.BlockSpec(memory_space=pltpu.VMEM)
HBM = pl.BlockSpec(memory_space=pltpu.HBM)
SMEM = pl.BlockSpec(memory_space=pltpu.SMEM)


def planes_of(k):
    return range(HALO - WIDTHS[k], PLANES - HALO + WIDTHS[k])


def call(kernel, ins, outs, scratch=(), flops=100000, vmem=8):
    return pl.pallas_call(
        kernel,
        in_specs=ins,
        out_specs=[VMEM] * len(outs),
        out_shape=[jax.ShapeDtypeStruct(s, F32) for s in outs],
        scratch_shapes=[pltpu.VMEM(s, F32) if isinstance(s, tuple) else s for s in scratch],
        compiler_params=pltpu.CompilerParams(vmem_limit_bytes=vmem * 2**20),
        cost_estimate=pl.CostEstimate(flops=flops, bytes_accessed=1000000, transcendentals=0),
    )


def prepare(
    place_x, opening_at, source_at, category_at, flags_at, table_at, fields, near, far, theta,
    opening, source, category, flags, table, arrived,
):
    copies = [
        pltpu.make_async_copy(a, b, arrived.at[n])
        for n, (a, b) in enumerate(
            (
                (table_at, table),
                (category_at, category),
                (flags_at, flags),
                (opening_at, opening),
                (source_at, source),
            )
        )
    ]
    for copy in copies:
        copy.start()
    for copy in copies:
        copy.wait()
    for k, shift in enumerate(shifts_of(table)):
        theta[k] = shift
    for p in range(X):
        kind = category[p]
        cond = jnp.full((Y, Z), table[0], F32)
        for n in range(1, table.shape[0]):
            cond = jnp.where(kind == n, table[n], cond)
        flag = flags[p].astype(F32)
        start = opening[p]
        values = (cond, start, 2.0 * source[p] - 6.0 * flag * start, flag)
        for k, v in enumerate(values):
            fields[k, p] = v
    first = place_x[0] == 0
    for k, w in enumerate(WIDTHS):
        for n in range(w):
            low, high = fields[k, n], fields[k, X - w + n]
            near[AT_X[k] + n] = jnp.where(first, high, low)
            far[AT_X[k] + n] = jnp.where(first, low, high)


def halo(place, far, pair, at, lower):
    far_side = (place == 0) if lower else (place == 1)
    return jnp.where(far_side, far[at], pair[(1 - place, *at)])


def plane(place, fields, far, pair, k, p, rows=slice(None)):
    if p < HALO:
        return halo(place, far, pair, (AT_X[k] + p - (HALO - WIDTHS[k]), rows), True)
    if p < HALO + X:
        return fields[k, p - HALO, rows]
    return halo(place, far, pair, (AT_X[k] + p - HALO - X, rows), False)


def slabs_y(place_x, place_y, fields, far_x, pair_x, near, far):
    first = place_y[0] == 0
    for k, w in enumerate(WIDTHS):
        for n, p in enumerate(planes_of(k)):
            to = pl.ds(AT_Y[k] + w * n, w)
            low, high = (
                plane(place_x[0], fields, far_x, pair_x, k, p, pl.ds(at, w)) for at in (0, Y - w)
            )
            near[to] = jnp.where(first, high, low)
            far[to] = jnp.where(first, low, high)


def assemble(place_x, place_y, place_z, fields, far_x, pair_x, far_y, pair_y, wide, near, far):
    lane = lax.broadcasted_iota(jnp.int32, (ROWS, Z), 1)
    first_core = place_z[0] == 0
    nothing = jnp.zeros((8, Z), F32)
    for k, w in enumerate(WIDTHS):
        for n, p in enumerate(planes_of(k)):
            at = (pl.ds(AT_Y[k] + w * n, w),)
            wide[k, p, 0:TOP] = nothing
            wide[k, p, TOP + Y : ROWS] = nothing
            wide[k, p, TOP : TOP + Y] = plane(place_x[0], fields, far_x, pair_x, k, p)
            wide[k, p, TOP - w : TOP] = halo(place_y[0], far_y, pair_y, at, True)
            wide[k, p, TOP + Y : TOP + Y + w] = halo(place_y[0], far_y, pair_y, at, False)
    for q in range(PER_GROUP):
        low = jnp.zeros((ROWS, Z), F32)
        high = low
        for g in range(GROUPS):
            p = PER_GROUP * g + q
            for k, w in enumerate(WIDTHS):
                if p in planes_of(k):
                    base = GROUP * g + AT_X[k]
                    turned = pltpu.roll(wide[k, p], base, 1)
                    place = lane if base else jnp.where(lane < Z // 2, lane, lane - Z)
                    low = jnp.where((place >= base) & (place < base + w), turned, low)
                    high = jnp.where((place >= base - w) & (place < base), turned, high)
        far[q] = jnp.where(first_core, low, high)
        near[q] = jnp.where(first_core, high, low)


def shifts_of(table):
    values = [jnp.full((8, Z), table[n], F32) for n in range(table.shape[0])]
    least, most, mean = values[0], values[0], values[0]
    for v in values[1:]:
        least, most, mean = jnp.minimum(least, v), jnp.maximum(most, v), mean + v
    mean = mean * (1.0 / len(values))
    top = 4.0 + 16.0 * most + 16.0 * mean
    low = 2.0 + 8.0 * least + 8.0 * mean
    middle, half = 0.5 * (top + low), 0.5 * (top - low)
    return [
        (middle + half * c) * (1.0 / SCALE) for c in (0.9238795, -0.9238795, 0.3826834, -0.3826834)
    ]


def smooth_xy(mid, planes, first, count):
    n = planes.shape[0] - 2
    here = planes[1:-1]
    mid[0:n, 8 : 8 + ROWS] = (planes[:-2] + here) + (here + planes[2:])
    sides = mid[0:n, pl.ds(7 + first, count)] + mid[0:n, pl.ds(9 + first, count)]
    return mid[0:n, pl.ds(8 + first, count)] + 0.5 * sides


def smooth_z(here, low, high):
    return here + 0.5 * (low + high)


def turned(values):
    return pltpu.roll(values, 1, 2), pltpu.roll(values, Z - 1, 2)


def newton_step(slope, diag, inside, shift, v, tv, tu):
    return ((diag - shift) * v - (slope * tv + tu)) * inside


def chunks(low, high, most):
    count = -(-(high - low) // most)
    size = -(-(high - low) // count)
    return [(p, min(p + size, high)) for p in range(low, high, size)]


def interior(wide, theta, basis, sums, ends, mid, tops, slopes, diag, inside, va, vb, za, zb, zc):
    lane = lax.broadcasted_iota(jnp.int32, (ROWS, Z), 1)
    slots = mid.shape[0]
    slot = [0]

    def smoothed(ref, p, q, first=0, count=ROWS):
        slot[0] += 1
        return smooth_xy(mid.at[slot[0] % slots], ref[p - 1 : q + 1], first, count)

    cond, start, rest, flag = (wide.at[k] for k in range(4))
    for p, q in chunks(0, PLANES, CHUNK):
        c, x = cond[p:q], start[p:q]
        (c_low, c_high), (x_low, x_high) = turned(c), turned(x)
        za[p:q] = smooth_z(c, c_low, c_high)
        zb[p:q] = smooth_z(x, x_low, x_high)
        zc[p:q] = smooth_z(c * x, c_low * x_low, c_high * x_high)
        for n, values in enumerate((c, c_low, c_high)):
            slopes[n, p:q] = values * (1.0 / SCALE)
    for p, q in chunks(1, PLANES - 1, CHUNK):
        tc, tx, tcx = (smoothed(ref, p, q) for ref in (za, zb, zc))
        c = cond[p:q]
        near = 16.0 * c + tc
        diag[p:q] = (1.0 + 6.0 * flag[p:q] + near) * (1.0 / SCALE)
        there = jnp.where(c > 0.0, 1.0, 0.0)
        inside[p:q] = there
        va[p:q] = (rest[p:q] - near * start[p:q] + (c * tx + tcx)) * there
    basis[0] = va[HALO : HALO + X, TOP : TOP + Y]
    for k in range(ITERS):
        v_old, v_new = (va, vb) if k % 2 == 0 else (vb, va)
        last = k + 1 == ITERS
        first, count = (TOP, Y) if last else (0, ROWS)
        rows = pl.ds(first, count)
        shift = jnp.tile(theta[k], (count // 8, 1))[None]
        for p, q in chunks(1 + k, PLANES - 1 - k, CHUNK):
            v = v_old[p:q]
            low, high = turned(v)
            za[p:q] = smooth_z(v, low, high)
            zb[p:q] = smooth_z(slopes[0, p:q] * v, slopes[1, p:q] * low, slopes[2, p:q] * high)
        for p, q in chunks(2 + k, PLANES - 2 - k, CHUNK):
            tv, tu = smoothed(za, p, q, first, count), smoothed(zb, p, q, first, count)
            v = newton_step(slopes[0, p:q, rows], diag[p:q, rows], inside[p:q, rows], shift, v_old[p:q, rows], tv, tu)
            if last:
                basis[k + 1, p - HALO : q - HALO] = v
            else:
                v_new[p:q] = v
        if not last:
            basis[k + 1] = v_new[HALO : HALO + X, TOP : TOP + Y]

    inner = (lane[:8] >= HALO) & (lane[:8] < Z - HALO)
    for n, (i, j) in enumerate(PAIRS):
        total = None
        for p in range(X):
            for half in (0, 8):
                rows = pl.ds(half, 8)
                term = basis[i, p, rows] * basis[j, p, rows]
                total = term if total is None else total + term
        sums[n] = jnp.where(inner, total, 0.0)

    place, from_high = lane % GROUP, (lane + HALO) % Z
    low_cells = (place >= LOW_AT) & (place < LOW_AT + 2 * HALO)
    high_cells = (place >= HIGH_AT - 2 * HALO) & (place < HIGH_AT)
    for k in range(4):
        for q in range(PER_GROUP):
            low = high = jnp.zeros((ROWS, Z), F32)
            for g in range(GROUPS):
                p = PER_GROUP * g + q
                if p in planes_of(k):
                    both = pltpu.roll(wide[k, p], GROUP * g + LOW_AT, 1)
                    low = jnp.where((lane // GROUP == g) & low_cells, both, low)
                    here = (from_high // GROUP == g) & (from_high % GROUP < 2 * HALO)
                    high = jnp.where(here, both, high)
            ends[k, q] = jnp.where(low_cells, low, 0.0)
            tops[k, q] = high
    for k in range(4):
        ends[k] = jnp.where(high_cells, pltpu.roll(tops[k], HIGH_AT - LOW_AT, 2), ends[k])


def edges(place_z, ends, far, chip, theta, inner_sums, basis, dots, cells, mid, slopes, stack):
    lane = lax.broadcasted_iota(jnp.int32, (ROWS, Z), 1)
    place = lane % GROUP
    slots = mid.shape[0]
    slot = [0]

    for q in range(PER_GROUP):
        below, above = (halo(place_z[0], far, chip, (q,), lower) for lower in (True, False))
        for k in range(4):
            low = pltpu.roll(below, (LOW_AT - AT_X[k]) % Z, 1)
            high = pltpu.roll(above, (HIGH_AT - AT_X[k]) % Z, 1)
            out = jnp.where(place < LOW_AT, low, ends[k, q])
            cells[k, q] = jnp.where((place >= HIGH_AT) & (place < HIGH_AT + HALO), high, out)

    def smoothed(planes, first=0, count=ROWS):
        slot[0] += 1
        return smooth_xy(mid.at[slot[0] % slots], planes, first, count)

    def spread(values):
        return [
            jnp.concatenate(
                [
                    pltpu.roll(values[PER_GROUP - 1], GROUP + by, 1)[None],
                    pltpu.roll(values, by % Z, 2) if by else values,
                    pltpu.roll(values[0], Z - GROUP + by, 1)[None],
                ]
            )
            for by in (0, 1, -1)
        ]

    cond, start, rest, flag = (cells[k] for k in range(4))
    cs, xs = spread(cond), spread(start)
    tc, tx, tcx = (
        smoothed(smooth_z(*values)) for values in (cs, xs, [c * x for c, x in zip(cs, xs)])
    )
    for n, values in enumerate(cs):
        slopes[n] = values * (1.0 / SCALE)
    near = 16.0 * cond + tc
    diag = (1.0 + 6.0 * flag + near) * (1.0 / SCALE)
    there = jnp.where(cond > 0.0, 1.0, 0.0)
    v = (rest - near * start + (cond * tx + tcx)) * there
    basis[0] = v[:, TOP : TOP + Y]
    for k in range(ITERS):
        last = k + 1 == ITERS
        first, count = (TOP, Y) if last else (0, ROWS)
        rows = slice(first, first + count)
        shift = jnp.tile(theta[k], (count // 8, 1))[None]
        vs = spread(v)
        tv = smoothed(smooth_z(*vs), first, count)
        tu = smoothed(smooth_z(*(slopes[n] * values for n, values in enumerate(vs))), first, count)
        v = newton_step(slopes[0, 1:-1][:, rows], diag[:, rows], there[:, rows], shift, v[:, rows], tv, tu)
        basis[k + 1] = v if last else v[:, TOP : TOP + Y]

    end_cells = ((place >= LOW_AT) & (place < LOW_AT + HALO)) | ((place >= HIGH_AT - HALO) & (place < HIGH_AT))
    mine = []
    for q in range(PER_GROUP):
        own = [g for g in range(GROUPS) if HALO <= PER_GROUP * g + q < HALO + X]
        at = (lane >= GROUP * own[0]) & (lane < GROUP * (own[-1] + 1))
        mine.append(jnp.where(at & end_cells, 1.0, 0.0)[:8])
    for n in range(16):
        total = None
        if n < len(PAIRS):
            i, j = PAIRS[n]
            total = inner_sums[n]
            for q in range(PER_GROUP):
                for half in (0, 8):
                    rows = pl.ds(half, 8)
                    total = total + (basis[i, q, rows] * mine[q]) * basis[j, q, rows]
        else:
            total = jnp.zeros((8, Z), F32)
        stack[pl.ds(8 * n, 8)] = total
    by_sum = stack[pl.ds(0, 16, stride=8)]
    for n in range(1, 8):
        by_sum = by_sum + stack[pl.ds(n, 16, stride=8)]
    total = lax.dot_general(
        jnp.ones((8, Z), F32), jnp.tile(by_sum, (8, 1)), (((1,), (1,)), ((), ())),
        precision=lax.Precision.HIGHEST, preferred_element_type=F32,
    )
    for n in range(dots.shape[0]):
        dots[n] = total[0:1]


def two_sum(a, b):
    s = a + b
    t = s - a
    return s, (a - (s - t)) + (b - t)


def row_sum(parts):
    rows = [(parts[n], None) for n in range(parts.shape[0])]
    while len(rows) > 1:
        pairs, rows = zip(rows[::2], rows[1::2]), []
        for (a, ea), (b, eb) in pairs:
            s, e = two_sum(a, b)
            rows.append((s, e if ea is None else e + (ea + eb)))
    return rows[0]


def relay(parts, copies):
    total, rest = row_sum(parts)
    lane = lax.broadcasted_iota(jnp.int32, total.shape, 1)
    total = jnp.where(lane < 16, total, rest)
    for n in range(copies.shape[0]):
        copies[n] = total


def quick(a, b):
    s = a + b
    return s, b - (s - a)


def halves(a):
    t = 4097.0 * a
    high = t - (t - a)
    return high, a - high


def plus(a, b):
    s, e = two_sum(a[0], b[0])
    return quick(s, e + (a[1] + b[1]))


def minus(a, b):
    return plus(a, (-b[0], -b[1]))


def times(a, b):
    p = a[0] * b[0]
    ah, al = halves(a[0])
    bh, bl = halves(b[0])
    e = ((ah * bh - p) + ah * bl + al * bh) + al * bl
    return quick(p, e + (a[0] * b[1] + a[1] * b[0]))


def reciprocal(a):
    q = 1.0 / a[0]
    qh, ql = halves(q)
    ah, al = halves(a[0])
    p = q * a[0]
    rest = ((1.0 - p) - (((qh * ah - p) + qh * al + ql * ah) + ql * al)) - q * a[1]
    return quick(q, q * rest)


def coefficients(gram, theta):
    none = jnp.zeros_like(theta[0])
    shift = [(t, none) for t in theta]
    system = [
        [plus(gram[i, j + 1], times(shift[j], gram[i, j])) for j in range(i + 1)]
        for i in range(ITERS)
    ]
    right = [gram[i, 0] for i in range(ITERS)]
    lower, inverse = {}, []
    for j in range(ITERS):
        inverse.append(reciprocal(system[j][j]))
        for i in range(j + 1, ITERS):
            lower[i, j] = times(system[i][j], inverse[j])
        for i in range(j + 1, ITERS):
            for k in range(j + 1, i + 1):
                system[i][k] = minus(system[i][k], times(lower[i, j], system[k][j]))
            right[i] = minus(right[i], times(lower[i, j], right[j]))
    y = [None] * ITERS
    for i in reversed(range(ITERS)):
        y[i] = times(right[i], inverse[i])
        for k in reversed(range(i + 1, ITERS)):
            y[i] = minus(y[i], times(lower[k, i], y[k]))
    r = [minus((none + 1.0, none), times(shift[0], y[0]))]
    for k in range(1, ITERS):
        total = plus(y[k - 1], times(shift[k], y[k]))
        r.append((-total[0], -total[1]))
    r.append((-y[-1][0], -y[-1][1]))
    return [a[0] * (1.0 / SCALE) for a in y], [a[0] for a in r]


def finish(parts, basis, end_basis, fields, theta, closing, mismatch):
    total, rest = row_sum(parts)
    rest = rest + pltpu.roll(total, Z - 16, 1)
    gram = {}
    for n, (i, j) in enumerate(PAIRS):
        gram[i, j] = gram[j, i] = quick(
            *(jnp.broadcast_to(v[0:1, n : n + 1], (8, Z)) for v in (total, rest))
        )
    y, r = coefficients(gram, [theta[k] for k in range(ITERS)])

    def combine(v):
        x, m = y[0] * v[0], r[ITERS] * v[ITERS]
        for k in range(1, ITERS):
            x = x + y[k] * v[k]
        for k in range(ITERS):
            m = m + r[k] * v[k]
        return x, m

    lane = lax.broadcasted_iota(jnp.int32, (8, Z), 1)
    for half in (0, 8):
        rows = pl.ds(half, 8)
        ends = [
            combine([end_basis[k, q, rows] for k in range(ITERS + 1)]) for q in range(PER_GROUP)
        ]
        for p in range(X):
            g, q = divmod(p + HALO, PER_GROUP)
            inner = combine([basis[k, p, rows] for k in range(ITERS + 1)])
            both = []
            for value, end in zip(inner, ends[q]):
                low = pltpu.roll(end, (Z - GROUP * g - LOW_AT) % Z, 1)
                high = pltpu.roll(end, (Z - GROUP * g - HIGH_AT) % Z, 1)
                value = jnp.where(lane < HALO, low, value)
                both.append(jnp.where(lane >= Z - HALO, high, value))
            closing[p, rows] = fields[1, p, rows] + both[0]
            mismatch[p, rows] = both[1]


def trade(near, far, axes):
    ends = lax.axis_size(axes) - 1
    others = [p for i in range(1, ends, 2) for p in ((i, i + 1), (i + 1, i))]
    return lax.ppermute(far, axes, others), lax.all_gather(near, axes[1], axis=0)


def exchange(copies, axes):
    return lax.all_to_all(copies, axes, split_axis=0, concat_axis=0, tiled=True)


def body(opening, source, category, table, flags):
    brick = (X, Y, Z)
    place_x, place_y, place_z = (lax.axis_index(axes[1]).reshape(1) for axes in (GX, GY, GZ))
    whole = pltpu.VMEM(brick, jnp.int32)
    fields, near, far, theta = call(
        prepare,
        [SMEM] + [HBM] * 5,
        [(4, *brick), (SLAB_X, Y, Z), (SLAB_X, Y, Z), (ITERS, 8, Z)],
        [brick, brick, whole, whole, pltpu.SMEM(table.shape, F32), pltpu.SemaphoreType.DMA((5,))],
    )(
        place_x,
        *(
            pltpu.with_memory_space_constraint(a, pltpu.HBM)
            for a in (opening, source, category, flags, table)
        ),
    )
    by_x = trade(near, far, GX)
    near, far = call(slabs_y, [SMEM] * 2 + [VMEM] * 3, [(SLAB_Y, Z)] * 2)(
        place_x, place_y, fields, *by_x
    )
    by_y = trade(near, far, GY)
    packed = (PER_GROUP, ROWS, Z)
    wide, near, far = call(assemble, [SMEM] * 3 + [VMEM] * 5, [(4, PLANES, ROWS, Z), packed, packed])(
        place_x, place_y, place_z, fields, *by_x, *by_y
    )
    far, chip = trade(near, far, GZ)
    sided = (PLANES, ROWS, Z)
    middle = (3, PLANES, ROWS + 16, Z)
    basis, sums, ends = call(
        interior,
        [VMEM] * 2,
        [(ITERS + 1, *brick), (len(PAIRS), 8, Z), (4, *packed)],
        [middle, (4, *packed), (3, *sided)] + [sided] * 7,
        flops=20000000,
        vmem=12,
    )(wide, theta)
    first, second = (*GY, "gz_1"), (*GX, "gz_0")
    end_basis, dots = call(
        edges,
        [SMEM] + [VMEM] * 5,
        [(ITERS + 1, PER_GROUP, Y, Z), (lax.axis_size(first), 1, Z)],
        [(4, *packed), (3, PER_GROUP, ROWS + 16, Z), (3, PER_GROUP + 2, ROWS, Z), (Z, Z)],
        flops=5000000,
    )(place_z, ends, far, chip, theta, sums)
    parts = exchange(dots, first)
    (copies,) = call(relay, [VMEM], [(lax.axis_size(second), 1, Z)])(parts)
    parts = exchange(copies, second)
    closing, mismatch = call(finish, [VMEM] * 5, [brick, brick])(
        parts, basis, end_basis, fields, theta
    )
    return closing, mismatch


def solution(mesh):
    pairs = [n for size in mesh.devices.shape for n in (size // 2, 2)]
    split = Mesh(mesh.devices.reshape(pairs), (*GX, *GY, *GZ))
    spec = P(GX, GY, GZ)
    return jax.shard_map(
        body, mesh=split, in_specs=(spec, spec, spec, P(), spec), out_specs=(spec, spec), check_vma=False
    )
```

```python
import jax
import jax.numpy as jnp
from jax import lax
from jax.experimental import pallas as pl
from jax.experimental.pallas import tpu as pltpu
from jax.sharding import Mesh
from jax.sharding import PartitionSpec as P

ITERS = 4
GX, GY, GZ = (("gx_0", "gx_1"), ("gy_0", "gy_1"), ("gz_0", "gz_1"))
F32 = jnp.float32
X, Y, Z = 8, 16, 128
HALO = ITERS + 1
WIDTHS = (5, 5, 4, 3)
PLANES = X + 2 * HALO
ROWS = 32
TOP = 8
SLAB_X = sum(WIDTHS)
AT_X = (0, 5, 10, 14)
AT_Y = (0, 90, 180, 244)
SLAB_Y = 288
GROUPS, PER_GROUP, GROUP = 4, 5, 32
LOW_AT, HIGH_AT = 5, 26
SCALE = 64.0
CHUNK = 3
PAIRS = [(i, j) for i in range(ITERS) for j in range(i, ITERS + 1)]
VMEM = pl.BlockSpec(memory_space=pltpu.VMEM)
HBM = pl.BlockSpec(memory_space=pltpu.HBM)
SMEM = pl.BlockSpec(memory_space=pltpu.SMEM)


def planes_of(k):
    return range(HALO - WIDTHS[k], PLANES - HALO + WIDTHS[k])


def call(kernel, ins, outs, scratch=(), flops=100000, vmem=8):
    return pl.pallas_call(
        kernel,
        in_specs=ins,
        out_specs=[VMEM] * len(outs),
        out_shape=[jax.ShapeDtypeStruct(s, F32) for s in outs],
        scratch_shapes=[pltpu.VMEM(s, F32) if isinstance(s, tuple) else s for s in scratch],
        compiler_params=pltpu.CompilerParams(vmem_limit_bytes=vmem * 2**20),
        cost_estimate=pl.CostEstimate(flops=flops, bytes_accessed=1000000, transcendentals=0),
    )


def prepare(
    place_x, opening_at, source_at, category_at, flags_at, table_at, fields, near, far, theta,
    opening, source, category, flags, table, arrived,
):
    copies = [
        pltpu.make_async_copy(a, b, arrived.at[n])
        for n, (a, b) in enumerate(
            (
                (table_at, table),
                (category_at, category),
                (flags_at, flags),
                (opening_at, opening),
                (source_at, source),
            )
        )
    ]
    for copy in copies:
        copy.start()
    for copy in copies:
        copy.wait()
    for k, shift in enumerate(shifts_of(table)):
        theta[k] = shift
    for p in range(X):
        kind = category[p]
        cond = jnp.full((Y, Z), table[0], F32)
        for n in range(1, table.shape[0]):
            cond = jnp.where(kind == n, table[n], cond)
        flag = flags[p].astype(F32)
        start = opening[p]
        values = (cond, start, 2.0 * source[p] - 6.0 * flag * start, flag)
        for k, v in enumerate(values):
            fields[k, p] = v
    first = place_x[0] == 0
    for k, w in enumerate(WIDTHS):
        for n in range(w):
            low, high = fields[k, n], fields[k, X - w + n]
            near[AT_X[k] + n] = jnp.where(first, high, low)
            far[AT_X[k] + n] = jnp.where(first, low, high)


def halo(place, far, pair, at, lower):
    far_side = (place == 0) if lower else (place == 1)
    return jnp.where(far_side, far[at], pair[(1 - place, *at)])


def plane(place, fields, far, pair, k, p, rows=slice(None)):
    if p < HALO:
        return halo(place, far, pair, (AT_X[k] + p - (HALO - WIDTHS[k]), rows), True)
    if p < HALO + X:
        return fields[k, p - HALO, rows]
    return halo(place, far, pair, (AT_X[k] + p - HALO - X, rows), False)


def slabs_y(place_x, place_y, fields, far_x, pair_x, near, far):
    first = place_y[0] == 0
    for k, w in enumerate(WIDTHS):
        for n, p in enumerate(planes_of(k)):
            to = pl.ds(AT_Y[k] + w * n, w)
            low, high = (
                plane(place_x[0], fields, far_x, pair_x, k, p, pl.ds(at, w)) for at in (0, Y - w)
            )
            near[to] = jnp.where(first, high, low)
            far[to] = jnp.where(first, low, high)


def assemble(place_x, place_y, place_z, fields, far_x, pair_x, far_y, pair_y, wide, near, far):
    lane = lax.broadcasted_iota(jnp.int32, (ROWS, Z), 1)
    first_core = place_z[0] == 0
    nothing = jnp.zeros((8, Z), F32)
    for k, w in enumerate(WIDTHS):
        for n, p in enumerate(planes_of(k)):
            at = (pl.ds(AT_Y[k] + w * n, w),)
            wide[k, p, 0:TOP] = nothing
            wide[k, p, TOP + Y : ROWS] = nothing
            wide[k, p, TOP : TOP + Y] = plane(place_x[0], fields, far_x, pair_x, k, p)
            wide[k, p, TOP - w : TOP] = halo(place_y[0], far_y, pair_y, at, True)
            wide[k, p, TOP + Y : TOP + Y + w] = halo(place_y[0], far_y, pair_y, at, False)
    for q in range(PER_GROUP):
        low = jnp.zeros((ROWS, Z), F32)
        high = low
        for g in range(GROUPS):
            p = PER_GROUP * g + q
            for k, w in enumerate(WIDTHS):
                if p in planes_of(k):
                    base = GROUP * g + AT_X[k]
                    turned = pltpu.roll(wide[k, p], base, 1)
                    place = lane if base else jnp.where(lane < Z // 2, lane, lane - Z)
                    low = jnp.where((place >= base) & (place < base + w), turned, low)
                    high = jnp.where((place >= base - w) & (place < base), turned, high)
        far[q] = jnp.where(first_core, low, high)
        near[q] = jnp.where(first_core, high, low)


def shifts_of(table):
    values = [jnp.full((8, Z), table[n], F32) for n in range(table.shape[0])]
    least, most, mean = values[0], values[0], values[0]
    for v in values[1:]:
        least, most, mean = jnp.minimum(least, v), jnp.maximum(most, v), mean + v
    mean = mean * (1.0 / len(values))
    top = 4.0 + 16.0 * most + 16.0 * mean
    low = 2.0 + 8.0 * least + 8.0 * mean
    middle, half = 0.5 * (top + low), 0.5 * (top - low)
    return [
        (middle + half * c) * (1.0 / SCALE) for c in (0.9238795, -0.9238795, 0.3826834, -0.3826834)
    ]


def smooth_xy(mid, planes, first, count):
    n = planes.shape[0] - 2
    pairs = planes[:-1] + planes[1:]
    mid[0:n, 8 : 8 + ROWS] = pairs[:-1] + pairs[1:]
    sides = mid[0:n, pl.ds(7 + first, count)] + mid[0:n, pl.ds(9 + first, count)]
    return mid[0:n, pl.ds(8 + first, count)] + 0.5 * sides


def smooth_z(here, low, high):
    return here + 0.5 * (low + high)


def turned(values):
    return pltpu.roll(values, 1, 2), pltpu.roll(values, Z - 1, 2)


def newton_step(slope, diag, inside, shift, v, tv, tu):
    return ((diag - shift) * v - (slope * tv + tu)) * inside


def chunks(low, high, most):
    count = -(-(high - low) // most)
    size = -(-(high - low) // count)
    return [(p, min(p + size, high)) for p in range(low, high, size)]


def interior(wide, theta, basis, sums, ends, mid, tops, slopes, diag, inside, va, vb, za, zb, zc):
    lane = lax.broadcasted_iota(jnp.int32, (ROWS, Z), 1)
    slots = mid.shape[0]
    slot = [0]

    def smoothed(ref, p, q, first=0, count=ROWS):
        slot[0] += 1
        return smooth_xy(mid.at[slot[0] % slots], ref[p - 1 : q + 1], first, count)

    place, from_high = lane % GROUP, (lane + HALO) % Z
    low_cells = (place >= LOW_AT) & (place < LOW_AT + 2 * HALO)
    high_cells = (place >= HIGH_AT - 2 * HALO) & (place < HIGH_AT)

    def pack(k, q):
        low = high = jnp.zeros((ROWS, Z), F32)
        for g in range(GROUPS):
            p = PER_GROUP * g + q
            if p in planes_of(k):
                both = pltpu.roll(wide[k, p], GROUP * g + LOW_AT, 1)
                low = jnp.where((lane // GROUP == g) & low_cells, both, low)
                here = (from_high // GROUP == g) & (from_high % GROUP < 2 * HALO)
                high = jnp.where(here, both, high)
        ends[k, q] = jnp.where(low_cells, low, 0.0)
        tops[k, q] = high

    to_pack = [(k, q) for k in range(4) for q in range(PER_GROUP)]

    def in_turn(low, high, turn, then):
        waiting, done = [], low + 1
        for p, q in chunks(low, high, CHUNK):
            turn(p, q)
            if to_pack:
                pack(*to_pack.pop(0))
            waiting.append((done, q - 1))
            done = q - 1
            if len(waiting) > 1:
                then(*waiting.pop(0))
        then(*waiting.pop(0))

    cond, start, rest, flag = (wide.at[k] for k in range(4))

    def turn_first(p, q):
        c, x = cond[p:q], start[p:q]
        (c_low, c_high), (x_low, x_high) = turned(c), turned(x)
        za[p:q] = smooth_z(c, c_low, c_high)
        zb[p:q] = smooth_z(x, x_low, x_high)
        zc[p:q] = smooth_z(c * x, c_low * x_low, c_high * x_high)
        for n, values in enumerate((c, c_low, c_high)):
            slopes[n, p:q] = values * (1.0 / SCALE)

    def first_vector(p, q):
        tc, tx, tcx = (smoothed(ref, p, q) for ref in (za, zb, zc))
        c = cond[p:q]
        near = 16.0 * c + tc
        diag[p:q] = (1.0 + 6.0 * flag[p:q] + near) * (1.0 / SCALE)
        there = jnp.where(c > 0.0, 1.0, 0.0)
        inside[p:q] = there
        va[p:q] = (rest[p:q] - near * start[p:q] + (c * tx + tcx)) * there

    in_turn(0, PLANES, turn_first, first_vector)
    basis[0] = va[HALO : HALO + X, TOP : TOP + Y]
    for k in range(ITERS):
        v_old, v_new = (va, vb) if k % 2 == 0 else (vb, va)
        last = k + 1 == ITERS
        first, count = (TOP, Y) if last else (0, ROWS)
        rows = pl.ds(first, count)
        shift = jnp.tile(theta[k], (count // 8, 1))[None]

        def turn(p, q):
            v = v_old[p:q]
            low, high = turned(v)
            za[p:q] = smooth_z(v, low, high)
            zb[p:q] = smooth_z(slopes[0, p:q] * v, slopes[1, p:q] * low, slopes[2, p:q] * high)

        def next_vector(p, q):
            tv, tu = smoothed(za, p, q, first, count), smoothed(zb, p, q, first, count)
            v = newton_step(slopes[0, p:q, rows], diag[p:q, rows], inside[p:q, rows], shift, v_old[p:q, rows], tv, tu)
            if last:
                basis[k + 1, p - HALO : q - HALO] = v
            else:
                v_new[p:q] = v

        in_turn(1 + k, PLANES - 1 - k, turn, next_vector)
        if not last:
            basis[k + 1] = v_new[HALO : HALO + X, TOP : TOP + Y]
    while to_pack:
        pack(*to_pack.pop(0))

    inner = (lane[:8] >= HALO) & (lane[:8] < Z - HALO)
    for n, (i, j) in enumerate(PAIRS):
        total = None
        for p in range(X):
            for half in (0, 8):
                rows = pl.ds(half, 8)
                term = basis[i, p, rows] * basis[j, p, rows]
                total = term if total is None else total + term
        sums[n] = jnp.where(inner, total, 0.0)

    for k in range(4):
        ends[k] = jnp.where(high_cells, pltpu.roll(tops[k], HIGH_AT - LOW_AT, 2), ends[k])


def edges(place_z, ends, far, chip, theta, inner_sums, basis, dots, mid, slopes, stack):
    lane = lax.broadcasted_iota(jnp.int32, (ROWS, Z), 1)
    place = lane % GROUP
    slots = mid.shape[0]
    slot = [0]

    below, above = (halo(place_z[0], far, chip, (slice(None),), lower) for lower in (True, False))

    def cells(k):
        low = pltpu.roll(below, (LOW_AT - AT_X[k]) % Z, 2)
        high = pltpu.roll(above, (HIGH_AT - AT_X[k]) % Z, 2)
        out = jnp.where(place < LOW_AT, low, ends[k])
        return jnp.where((place >= HIGH_AT) & (place < HIGH_AT + HALO), high, out)

    def smoothed(planes, first=0, count=ROWS):
        slot[0] += 1
        return smooth_xy(mid.at[slot[0] % slots], planes, first, count)

    def spread(values):
        return [
            jnp.concatenate(
                [
                    pltpu.roll(values[PER_GROUP - 1], GROUP + by, 1)[None],
                    pltpu.roll(values, by % Z, 2) if by else values,
                    pltpu.roll(values[0], Z - GROUP + by, 1)[None],
                ]
            )
            for by in (0, 1, -1)
        ]

    cond, start = cells(0), cells(1)
    cs, xs = spread(cond), spread(start)
    tc, tx, tcx = (
        smoothed(smooth_z(*values)) for values in (cs, xs, [c * x for c, x in zip(cs, xs)])
    )
    for n, values in enumerate(cs):
        slopes[n] = values * (1.0 / SCALE)
    rest, flag = cells(2), cells(3)
    near = 16.0 * cond + tc
    diag = (1.0 + 6.0 * flag + near) * (1.0 / SCALE)
    there = jnp.where(cond > 0.0, 1.0, 0.0)
    v = (rest - near * start + (cond * tx + tcx)) * there
    basis[0] = v[:, TOP : TOP + Y]
    for k in range(ITERS):
        last = k + 1 == ITERS
        first, count = (TOP, Y) if last else (0, ROWS)
        rows = slice(first, first + count)
        shift = jnp.tile(theta[k], (count // 8, 1))[None]
        vs = spread(v)
        tv = smoothed(smooth_z(*vs), first, count)
        tu = smoothed(smooth_z(*(slopes[n] * values for n, values in enumerate(vs))), first, count)
        v = newton_step(slopes[0, 1:-1][:, rows], diag[:, rows], there[:, rows], shift, v[:, rows], tv, tu)
        basis[k + 1] = v if last else v[:, TOP : TOP + Y]

    end_cells = ((place >= LOW_AT) & (place < LOW_AT + HALO)) | ((place >= HIGH_AT - HALO) & (place < HIGH_AT))
    mine = []
    for q in range(PER_GROUP):
        own = [g for g in range(GROUPS) if HALO <= PER_GROUP * g + q < HALO + X]
        at = (lane >= GROUP * own[0]) & (lane < GROUP * (own[-1] + 1))
        mine.append(jnp.where(at & end_cells, 1.0, 0.0)[:8])
    for n in range(16):
        total = None
        if n < len(PAIRS):
            i, j = PAIRS[n]
            total = inner_sums[n]
            for q in range(PER_GROUP):
                for half in (0, 8):
                    rows = pl.ds(half, 8)
                    total = total + (basis[i, q, rows] * mine[q]) * basis[j, q, rows]
        else:
            total = jnp.zeros((8, Z), F32)
        stack[pl.ds(8 * n, 8)] = total
    by_sum = stack[pl.ds(0, 16, stride=8)]
    for n in range(1, 8):
        by_sum = by_sum + stack[pl.ds(n, 16, stride=8)]
    total = lax.dot_general(
        jnp.ones((8, Z), F32), jnp.tile(by_sum, (8, 1)), (((1,), (1,)), ((), ())),
        precision=lax.Precision.HIGHEST, preferred_element_type=F32,
    )
    for n in range(dots.shape[0]):
        dots[n] = total[0:1]


def two_sum(a, b):
    s = a + b
    t = s - a
    return s, (a - (s - t)) + (b - t)


def row_sum(parts):
    rows = [(parts[n], None) for n in range(parts.shape[0])]
    while len(rows) > 1:
        pairs, rows = zip(rows[::2], rows[1::2]), []
        for (a, ea), (b, eb) in pairs:
            s, e = two_sum(a, b)
            rows.append((s, e if ea is None else e + (ea + eb)))
    return rows[0]


def relay(parts, copies):
    total, rest = row_sum(parts)
    lane = lax.broadcasted_iota(jnp.int32, total.shape, 1)
    total = jnp.where(lane < 16, total, rest)
    for n in range(copies.shape[0]):
        copies[n] = total


def quick(a, b):
    s = a + b
    return s, b - (s - a)


def halves(a):
    t = 4097.0 * a
    high = t - (t - a)
    return high, a - high


def plus(a, b):
    s, e = two_sum(a[0], b[0])
    return quick(s, e + (a[1] + b[1]))


def minus(a, b):
    return plus(a, (-b[0], -b[1]))


def times(a, b):
    p = a[0] * b[0]
    ah, al = halves(a[0])
    bh, bl = halves(b[0])
    e = ((ah * bh - p) + ah * bl + al * bh) + al * bl
    return quick(p, e + (a[0] * b[1] + a[1] * b[0]))


def reciprocal(a):
    q = 1.0 / a[0]
    qh, ql = halves(q)
    ah, al = halves(a[0])
    p = q * a[0]
    rest = ((1.0 - p) - (((qh * ah - p) + qh * al + ql * ah) + ql * al)) - q * a[1]
    return quick(q, q * rest)


def coefficients(gram, theta):
    none = jnp.zeros_like(theta[0])
    shift = [(t, none) for t in theta]
    system = [
        [plus(gram[i, j + 1], times(shift[j], gram[i, j])) for j in range(i + 1)]
        for i in range(ITERS)
    ]
    right = [gram[i, 0] for i in range(ITERS)]
    lower, inverse = {}, []
    for j in range(ITERS):
        inverse.append(reciprocal(system[j][j]))
        for i in range(j + 1, ITERS):
            lower[i, j] = times(system[i][j], inverse[j])
        for i in range(j + 1, ITERS):
            for k in range(j + 1, i + 1):
                system[i][k] = minus(system[i][k], times(lower[i, j], system[k][j]))
            right[i] = minus(right[i], times(lower[i, j], right[j]))
    y = [None] * ITERS
    for i in reversed(range(ITERS)):
        y[i] = times(right[i], inverse[i])
        for k in reversed(range(i + 1, ITERS)):
            y[i] = minus(y[i], times(lower[k, i], y[k]))
    r = [minus((none + 1.0, none), times(shift[0], y[0]))]
    for k in range(1, ITERS):
        total = plus(y[k - 1], times(shift[k], y[k]))
        r.append((-total[0], -total[1]))
    r.append((-y[-1][0], -y[-1][1]))
    return [a[0] * (1.0 / SCALE) for a in y], [a[0] for a in r]


def finish(parts, basis, end_basis, fields, theta, closing, mismatch):
    total, rest = row_sum(parts)
    rest = rest + pltpu.roll(total, Z - 16, 1)
    gram = {}
    for n, (i, j) in enumerate(PAIRS):
        gram[i, j] = gram[j, i] = quick(
            *(jnp.broadcast_to(v[0:1, n : n + 1], (8, Z)) for v in (total, rest))
        )
    y, r = coefficients(gram, [theta[k] for k in range(ITERS)])

    def combine(v):
        x, m = y[0] * v[0], r[ITERS] * v[ITERS]
        for k in range(1, ITERS):
            x = x + y[k] * v[k]
        for k in range(ITERS):
            m = m + r[k] * v[k]
        return x, m

    lane = lax.broadcasted_iota(jnp.int32, (8, Z), 1)
    for half in (0, 8):
        rows = pl.ds(half, 8)
        ends = [
            combine([end_basis[k, q, rows] for k in range(ITERS + 1)]) for q in range(PER_GROUP)
        ]
        for p in range(X):
            g, q = divmod(p + HALO, PER_GROUP)
            inner = combine([basis[k, p, rows] for k in range(ITERS + 1)])
            both = []
            for value, end in zip(inner, ends[q]):
                low = pltpu.roll(end, (Z - GROUP * g - LOW_AT) % Z, 1)
                high = pltpu.roll(end, (Z - GROUP * g - HIGH_AT) % Z, 1)
                value = jnp.where(lane < HALO, low, value)
                both.append(jnp.where(lane >= Z - HALO, high, value))
            closing[p, rows] = fields[1, p, rows] + both[0]
            mismatch[p, rows] = both[1]


def trade(near, far, axes):
    ends = lax.axis_size(axes) - 1
    others = [p for i in range(1, ends, 2) for p in ((i, i + 1), (i + 1, i))]
    return lax.ppermute(far, axes, others), lax.all_gather(near, axes[1], axis=0)


def exchange(copies, axes):
    return lax.all_to_all(copies, axes, split_axis=0, concat_axis=0, tiled=True)


def body(opening, source, category, table, flags):
    brick = (X, Y, Z)
    place_x, place_y, place_z = (lax.axis_index(axes[1]).reshape(1) for axes in (GX, GY, GZ))
    whole = pltpu.VMEM(brick, jnp.int32)
    fields, near, far, theta = call(
        prepare,
        [SMEM] + [HBM] * 5,
        [(4, *brick), (SLAB_X, Y, Z), (SLAB_X, Y, Z), (ITERS, 8, Z)],
        [brick, brick, whole, whole, pltpu.SMEM(table.shape, F32), pltpu.SemaphoreType.DMA((5,))],
    )(
        place_x,
        *(
            pltpu.with_memory_space_constraint(a, pltpu.HBM)
            for a in (opening, source, category, flags, table)
        ),
    )
    by_x = trade(near, far, GX)
    near, far = call(slabs_y, [SMEM] * 2 + [VMEM] * 3, [(SLAB_Y, Z)] * 2)(
        place_x, place_y, fields, *by_x
    )
    by_y = trade(near, far, GY)
    packed = (PER_GROUP, ROWS, Z)
    wide, near, far = call(assemble, [SMEM] * 3 + [VMEM] * 5, [(4, PLANES, ROWS, Z), packed, packed])(
        place_x, place_y, place_z, fields, *by_x, *by_y
    )
    far, chip = trade(near, far, GZ)
    sided = (PLANES, ROWS, Z)
    middle = (3, PLANES, ROWS + 16, Z)
    basis, sums, ends = call(
        interior,
        [VMEM] * 2,
        [(ITERS + 1, *brick), (len(PAIRS), 8, Z), (4, *packed)],
        [middle, (4, *packed), (3, *sided)] + [sided] * 7,
        flops=20000000,
        vmem=12,
    )(wide, theta)
    first, second = (*GY, "gz_1"), (*GX, "gz_0")
    end_basis, dots = call(
        edges,
        [SMEM] + [VMEM] * 5,
        [(ITERS + 1, PER_GROUP, Y, Z), (lax.axis_size(first), 1, Z)],
        [(3, PER_GROUP, ROWS + 16, Z), (3, PER_GROUP + 2, ROWS, Z), (Z, Z)],
        flops=5000000,
    )(place_z, ends, far, chip, theta, sums)
    parts = exchange(dots, first)
    (copies,) = call(relay, [VMEM], [(lax.axis_size(second), 1, Z)])(parts)
    parts = exchange(copies, second)
    closing, mismatch = call(finish, [VMEM] * 5, [brick, brick])(
        parts, basis, end_basis, fields, theta
    )
    return closing, mismatch


def solution(mesh):
    pairs = [n for size in mesh.devices.shape for n in (size // 2, 2)]
    split = Mesh(mesh.devices.reshape(pairs), (*GX, *GY, *GZ))
    spec = P(GX, GY, GZ)
    return jax.shard_map(
        body, mesh=split, in_specs=(spec, spec, spec, P(), spec), out_specs=(spec, spec), check_vma=False
    )
```

```python
import jax
import jax.numpy as jnp
from jax import lax
from jax.experimental import pallas as pl
from jax.experimental.pallas import tpu as pltpu
from jax.sharding import Mesh
from jax.sharding import PartitionSpec as P

ITERS = 4
GX, GY, GZ = (("gx_0", "gx_1"), ("gy_0", "gy_1"), ("gz_0", "gz_1"))
F32 = jnp.float32
X, Y, Z = 8, 16, 128
HALO = ITERS + 1
WIDTHS = (5, 5, 4, 3)
PLANES = X + 2 * HALO
ROWS = 32
TOP = 8
SLAB_X = sum(WIDTHS)
AT_X = (0, 5, 10, 14)
AT_Y = (0, 90, 180, 244)
SLAB_Y = 288
GROUPS, PER_GROUP, GROUP = 4, 5, 32
LOW_AT, HIGH_AT = 5, 26
SCALE = 64.0
CHUNK = 3
PAIRS = [(i, j) for i in range(ITERS) for j in range(i, ITERS + 1)]
VMEM = pl.BlockSpec(memory_space=pltpu.VMEM)
HBM = pl.BlockSpec(memory_space=pltpu.HBM)
SMEM = pl.BlockSpec(memory_space=pltpu.SMEM)


def planes_of(k):
    return range(HALO - WIDTHS[k], PLANES - HALO + WIDTHS[k])


def call(kernel, ins, outs, scratch=(), flops=100000, vmem=8):
    return pl.pallas_call(
        kernel,
        in_specs=ins,
        out_specs=[VMEM] * len(outs),
        out_shape=[jax.ShapeDtypeStruct(s, F32) for s in outs],
        scratch_shapes=[pltpu.VMEM(s, F32) if isinstance(s, tuple) else s for s in scratch],
        compiler_params=pltpu.CompilerParams(vmem_limit_bytes=vmem * 2**20),
        cost_estimate=pl.CostEstimate(flops=flops, bytes_accessed=1000000, transcendentals=0),
    )


def prepare(
    place_x, opening_at, source_at, category_at, flags_at, table_at, fields, near, far, theta,
    opening, source, category, flags, table, arrived,
):
    copies = [
        pltpu.make_async_copy(a, b, arrived.at[n])
        for n, (a, b) in enumerate(
            (
                (table_at, table),
                (category_at, category),
                (flags_at, flags),
                (opening_at, opening),
                (source_at, source),
            )
        )
    ]
    for copy in copies:
        copy.start()
    for copy in copies:
        copy.wait()
    for k, shift in enumerate(shifts_of(table)):
        theta[k] = shift
    for p in range(X):
        kind = category[p]
        cond = jnp.full((Y, Z), table[0], F32)
        for n in range(1, table.shape[0]):
            cond = jnp.where(kind == n, table[n], cond)
        flag = flags[p].astype(F32)
        start = opening[p]
        values = (cond, start, 2.0 * source[p] - 6.0 * flag * start, flag)
        for k, v in enumerate(values):
            fields[k, p] = v
    first = place_x[0] == 0
    for k, w in enumerate(WIDTHS):
        for n in range(w):
            low, high = fields[k, n], fields[k, X - w + n]
            near[AT_X[k] + n] = jnp.where(first, high, low)
            far[AT_X[k] + n] = jnp.where(first, low, high)


def halo(place, far, pair, at, lower):
    far_side = (place == 0) if lower else (place == 1)
    return jnp.where(far_side, far[at], pair[(1 - place, *at)])


def plane(place, fields, far, pair, k, p, rows=slice(None)):
    if p < HALO:
        return halo(place, far, pair, (AT_X[k] + p - (HALO - WIDTHS[k]), rows), True)
    if p < HALO + X:
        return fields[k, p - HALO, rows]
    return halo(place, far, pair, (AT_X[k] + p - HALO - X, rows), False)


def slabs_y(place_x, place_y, fields, far_x, pair_x, near, far):
    first = place_y[0] == 0
    for k, w in enumerate(WIDTHS):
        for n, p in enumerate(planes_of(k)):
            to = pl.ds(AT_Y[k] + w * n, w)
            low, high = (
                plane(place_x[0], fields, far_x, pair_x, k, p, pl.ds(at, w)) for at in (0, Y - w)
            )
            near[to] = jnp.where(first, high, low)
            far[to] = jnp.where(first, low, high)


def assemble(place_x, place_y, place_z, fields, far_x, pair_x, far_y, pair_y, wide, near, far):
    lane = lax.broadcasted_iota(jnp.int32, (ROWS, Z), 1)
    first_core = place_z[0] == 0
    nothing = jnp.zeros((8, Z), F32)
    for k, w in enumerate(WIDTHS):
        for n, p in enumerate(planes_of(k)):
            at = (pl.ds(AT_Y[k] + w * n, w),)
            wide[k, p, 0:TOP] = nothing
            wide[k, p, TOP + Y : ROWS] = nothing
            wide[k, p, TOP : TOP + Y] = plane(place_x[0], fields, far_x, pair_x, k, p)
            wide[k, p, TOP - w : TOP] = halo(place_y[0], far_y, pair_y, at, True)
            wide[k, p, TOP + Y : TOP + Y + w] = halo(place_y[0], far_y, pair_y, at, False)
    for q in range(PER_GROUP):
        low = jnp.zeros((ROWS, Z), F32)
        high = low
        for g in range(GROUPS):
            p = PER_GROUP * g + q
            for k, w in enumerate(WIDTHS):
                if p in planes_of(k):
                    base = GROUP * g + AT_X[k]
                    turned = pltpu.roll(wide[k, p], base, 1)
                    place = lane if base else jnp.where(lane < Z // 2, lane, lane - Z)
                    low = jnp.where((place >= base) & (place < base + w), turned, low)
                    high = jnp.where((place >= base - w) & (place < base), turned, high)
        far[q] = jnp.where(first_core, low, high)
        near[q] = jnp.where(first_core, high, low)


def shifts_of(table):
    values = [jnp.full((8, Z), table[n], F32) for n in range(table.shape[0])]
    least, most, mean = values[0], values[0], values[0]
    for v in values[1:]:
        least, most, mean = jnp.minimum(least, v), jnp.maximum(most, v), mean + v
    mean = mean * (1.0 / len(values))
    top = 4.0 + 16.0 * most + 16.0 * mean
    low = 2.0 + 8.0 * least + 8.0 * mean
    middle, half = 0.5 * (top + low), 0.5 * (top - low)
    return [
        (middle + half * c) * (1.0 / SCALE) for c in (-0.9238795, 0.9238795, -0.3826834, 0.3826834)
    ]


def smooth_xy(mid, planes, first, count):
    n = planes.shape[0] - 2
    pairs = planes[:-1] + planes[1:]
    mid[0:n, 8 : 8 + ROWS] = pairs[:-1] + pairs[1:]
    sides = mid[0:n, pl.ds(7 + first, count)] + mid[0:n, pl.ds(9 + first, count)]
    return mid[0:n, pl.ds(8 + first, count)] + 0.5 * sides


def smooth_z(here, low, high):
    return here + 0.5 * (low + high)


def turned(values):
    return pltpu.roll(values, 1, 2), pltpu.roll(values, Z - 1, 2)


def newton_step(slope, diag, inside, shift, v, tv, tu):
    return ((diag - shift) * v - (slope * tv + tu)) * inside


def chunks(low, high, most):
    count = -(-(high - low) // most)
    size = -(-(high - low) // count)
    return [(p, min(p + size, high)) for p in range(low, high, size)]


def interior(wide, theta, basis, sums, ends, mid, tops, slopes, diag, inside, va, vb, za, zb, zc):
    lane = lax.broadcasted_iota(jnp.int32, (ROWS, Z), 1)
    slots = mid.shape[0]
    slot = [0]

    def smoothed(ref, p, q, first=0, count=ROWS):
        slot[0] += 1
        return smooth_xy(mid.at[slot[0] % slots], ref[p - 1 : q + 1], first, count)

    place, from_high = lane % GROUP, (lane + HALO) % Z
    low_cells = (place >= LOW_AT) & (place < LOW_AT + 2 * HALO)
    high_cells = (place >= HIGH_AT - 2 * HALO) & (place < HIGH_AT)

    def pack(k, q):
        low = high = jnp.zeros((ROWS, Z), F32)
        for g in range(GROUPS):
            p = PER_GROUP * g + q
            if p in planes_of(k):
                both = pltpu.roll(wide[k, p], GROUP * g + LOW_AT, 1)
                low = jnp.where((lane // GROUP == g) & low_cells, both, low)
                here = (from_high // GROUP == g) & (from_high % GROUP < 2 * HALO)
                high = jnp.where(here, both, high)
        ends[k, q] = jnp.where(low_cells, low, 0.0)
        tops[k, q] = high

    to_pack = [(k, q) for k in range(4) for q in range(PER_GROUP)]

    def in_turn(low, high, turn, then):
        waiting, done = [], low + 1
        for p, q in chunks(low, high, CHUNK):
            turn(p, q)
            if to_pack:
                pack(*to_pack.pop(0))
            waiting.append((done, q - 1))
            done = q - 1
            if len(waiting) > 1:
                then(*waiting.pop(0))
        then(*waiting.pop(0))

    cond, start, rest, flag = (wide.at[k] for k in range(4))

    def turn_first(p, q):
        c, x = cond[p:q], start[p:q]
        (c_low, c_high), (x_low, x_high) = turned(c), turned(x)
        za[p:q] = smooth_z(c, c_low, c_high)
        zb[p:q] = smooth_z(x, x_low, x_high)
        zc[p:q] = smooth_z(c * x, c_low * x_low, c_high * x_high)
        for n, values in enumerate((c, c_low, c_high)):
            slopes[n, p:q] = values * (1.0 / SCALE)

    def first_vector(p, q):
        tc, tx, tcx = (smoothed(ref, p, q) for ref in (za, zb, zc))
        c = cond[p:q]
        near = 16.0 * c + tc
        diag[p:q] = (1.0 + 6.0 * flag[p:q] + near) * (1.0 / SCALE)
        there = jnp.where(c > 0.0, 1.0, 0.0)
        inside[p:q] = there
        va[p:q] = (rest[p:q] - near * start[p:q] + (c * tx + tcx)) * there

    in_turn(0, PLANES, turn_first, first_vector)
    basis[0] = va[HALO : HALO + X, TOP : TOP + Y]
    for k in range(ITERS):
        v_old, v_new = (va, vb) if k % 2 == 0 else (vb, va)
        last = k + 1 == ITERS
        first, count = (TOP, Y) if last else (0, ROWS)
        rows = pl.ds(first, count)
        shift = jnp.tile(theta[k], (count // 8, 1))[None]

        def turn(p, q):
            v = v_old[p:q]
            low, high = turned(v)
            za[p:q] = smooth_z(v, low, high)
            zb[p:q] = smooth_z(slopes[0, p:q] * v, slopes[1, p:q] * low, slopes[2, p:q] * high)

        def next_vector(p, q):
            tv, tu = smoothed(za, p, q, first, count), smoothed(zb, p, q, first, count)
            v = newton_step(slopes[0, p:q, rows], diag[p:q, rows], inside[p:q, rows], shift, v_old[p:q, rows], tv, tu)
            if last:
                basis[k + 1, p - HALO : q - HALO] = v
            else:
                v_new[p:q] = v

        in_turn(1 + k, PLANES - 1 - k, turn, next_vector)
        if not last:
            basis[k + 1] = v_new[HALO : HALO + X, TOP : TOP + Y]
    while to_pack:
        pack(*to_pack.pop(0))

    inner = (lane[:8] >= HALO) & (lane[:8] < Z - HALO)
    for n, (i, j) in enumerate(PAIRS):
        total = None
        for p in range(X):
            for half in (0, 8):
                rows = pl.ds(half, 8)
                term = basis[i, p, rows] * basis[j, p, rows]
                total = term if total is None else total + term
        sums[n] = jnp.where(inner, total, 0.0)

    for k in range(4):
        ends[k] = jnp.where(high_cells, pltpu.roll(tops[k], HIGH_AT - LOW_AT, 2), ends[k])


def edges(place_z, ends, far, chip, theta, inner_sums, basis, dots, mid, slopes, stack):
    lane = lax.broadcasted_iota(jnp.int32, (ROWS, Z), 1)
    place = lane % GROUP
    slots = mid.shape[0]
    slot = [0]

    below, above = (halo(place_z[0], far, chip, (slice(None),), lower) for lower in (True, False))

    def cells(k):
        low = pltpu.roll(below, (LOW_AT - AT_X[k]) % Z, 2)
        high = pltpu.roll(above, (HIGH_AT - AT_X[k]) % Z, 2)
        out = jnp.where(place < LOW_AT, low, ends[k])
        return jnp.where((place >= HIGH_AT) & (place < HIGH_AT + HALO), high, out)

    def smoothed(planes, first=0, count=ROWS):
        slot[0] += 1
        return smooth_xy(mid.at[slot[0] % slots], planes, first, count)

    def spread(values):
        return [
            jnp.concatenate(
                [
                    pltpu.roll(values[PER_GROUP - 1], GROUP + by, 1)[None],
                    pltpu.roll(values, by % Z, 2) if by else values,
                    pltpu.roll(values[0], Z - GROUP + by, 1)[None],
                ]
            )
            for by in (0, 1, -1)
        ]

    cond, start = cells(0), cells(1)
    cs, xs = spread(cond), spread(start)
    tc, tx, tcx = (
        smoothed(smooth_z(*values)) for values in (cs, xs, [c * x for c, x in zip(cs, xs)])
    )
    for n, values in enumerate(cs):
        slopes[n] = values * (1.0 / SCALE)
    rest, flag = cells(2), cells(3)
    near = 16.0 * cond + tc
    diag = (1.0 + 6.0 * flag + near) * (1.0 / SCALE)
    there = jnp.where(cond > 0.0, 1.0, 0.0)
    v = (rest - near * start + (cond * tx + tcx)) * there
    basis[0] = v[:, TOP : TOP + Y]
    for k in range(ITERS):
        last = k + 1 == ITERS
        first, count = (TOP, Y) if last else (0, ROWS)
        rows = slice(first, first + count)
        shift = jnp.tile(theta[k], (count // 8, 1))[None]
        vs = spread(v)
        tv = smoothed(smooth_z(*vs), first, count)
        tu = smoothed(smooth_z(*(slopes[n] * values for n, values in enumerate(vs))), first, count)
        v = newton_step(slopes[0, 1:-1][:, rows], diag[:, rows], there[:, rows], shift, v[:, rows], tv, tu)
        basis[k + 1] = v if last else v[:, TOP : TOP + Y]

    end_cells = ((place >= LOW_AT) & (place < LOW_AT + HALO)) | ((place >= HIGH_AT - HALO) & (place < HIGH_AT))
    mine = []
    for q in range(PER_GROUP):
        own = [g for g in range(GROUPS) if HALO <= PER_GROUP * g + q < HALO + X]
        at = (lane >= GROUP * own[0]) & (lane < GROUP * (own[-1] + 1))
        mine.append(jnp.where(at & end_cells, 1.0, 0.0)[:8])
    for n in range(16):
        total = None
        if n < len(PAIRS):
            i, j = PAIRS[n]
            total = inner_sums[n]
            for q in range(PER_GROUP):
                for half in (0, 8):
                    rows = pl.ds(half, 8)
                    total = total + (basis[i, q, rows] * mine[q]) * basis[j, q, rows]
        else:
            total = jnp.zeros((8, Z), F32)
        stack[pl.ds(8 * n, 8)] = total
    by_sum = stack[pl.ds(0, 16, stride=8)]
    for n in range(1, 8):
        by_sum = by_sum + stack[pl.ds(n, 16, stride=8)]
    total = lax.dot_general(
        jnp.ones((8, Z), F32), jnp.tile(by_sum, (8, 1)), (((1,), (1,)), ((), ())),
        precision=lax.Precision.HIGHEST, preferred_element_type=F32,
    )
    for n in range(dots.shape[0]):
        dots[n] = total[0:1]


def two_sum(a, b):
    s = a + b
    t = s - a
    return s, (a - (s - t)) + (b - t)


def row_sum(parts):
    rows = [(parts[n], None) for n in range(parts.shape[0])]
    while len(rows) > 1:
        pairs, rows = zip(rows[::2], rows[1::2]), []
        for (a, ea), (b, eb) in pairs:
            s, e = two_sum(a, b)
            rows.append((s, e if ea is None else e + (ea + eb)))
    return rows[0]


def relay(parts, copies):
    total, rest = row_sum(parts)
    lane = lax.broadcasted_iota(jnp.int32, total.shape, 1)
    total = jnp.where(lane < 16, total, rest)
    for n in range(copies.shape[0]):
        copies[n] = total


def quick(a, b):
    s = a + b
    return s, b - (s - a)


def halves(a):
    t = 4097.0 * a
    high = t - (t - a)
    return high, a - high


def plus(a, b):
    s, e = two_sum(a[0], b[0])
    return quick(s, e + (a[1] + b[1]))


def minus(a, b):
    return plus(a, (-b[0], -b[1]))


def times(a, b):
    p = a[0] * b[0]
    ah, al = halves(a[0])
    bh, bl = halves(b[0])
    e = ((ah * bh - p) + ah * bl + al * bh) + al * bl
    return quick(p, e + (a[0] * b[1] + a[1] * b[0]))


def reciprocal(a):
    q = 1.0 / a[0]
    qh, ql = halves(q)
    ah, al = halves(a[0])
    p = q * a[0]
    rest = ((1.0 - p) - (((qh * ah - p) + qh * al + ql * ah) + ql * al)) - q * a[1]
    return quick(q, q * rest)


def coefficients(gram, theta):
    none = jnp.zeros_like(theta[0])
    shift = [(t, none) for t in theta]
    system = [
        [plus(gram[i, j + 1], times(shift[j], gram[i, j])) for j in range(i + 1)]
        for i in range(ITERS)
    ]
    right = [gram[i, 0] for i in range(ITERS)]
    lower, inverse = {}, []
    for j in range(ITERS):
        inverse.append(reciprocal(system[j][j]))
        for i in range(j + 1, ITERS):
            lower[i, j] = times(system[i][j], inverse[j])
        for i in range(j + 1, ITERS):
            for k in range(j + 1, i + 1):
                system[i][k] = minus(system[i][k], times(lower[i, j], system[k][j]))
            right[i] = minus(right[i], times(lower[i, j], right[j]))
    y = [None] * ITERS
    for i in reversed(range(ITERS)):
        y[i] = times(right[i], inverse[i])
        for k in reversed(range(i + 1, ITERS)):
            y[i] = minus(y[i], times(lower[k, i], y[k]))
    r = [minus((none + 1.0, none), times(shift[0], y[0]))]
    for k in range(1, ITERS):
        total = plus(y[k - 1], times(shift[k], y[k]))
        r.append((-total[0], -total[1]))
    r.append((-y[-1][0], -y[-1][1]))
    return [a[0] * (1.0 / SCALE) for a in y], [a[0] for a in r]


def finish(parts, basis, end_basis, fields, theta, closing, mismatch):
    total, rest = row_sum(parts)
    rest = rest + pltpu.roll(total, Z - 16, 1)
    gram = {}
    for n, (i, j) in enumerate(PAIRS):
        gram[i, j] = gram[j, i] = quick(
            *(jnp.broadcast_to(v[0:1, n : n + 1], (8, Z)) for v in (total, rest))
        )
    y, r = coefficients(gram, [theta[k] for k in range(ITERS)])

    def combine(v):
        x, m = y[0] * v[0], r[ITERS] * v[ITERS]
        for k in range(1, ITERS):
            x = x + y[k] * v[k]
        for k in range(ITERS):
            m = m + r[k] * v[k]
        return x, m

    lane = lax.broadcasted_iota(jnp.int32, (8, Z), 1)
    for half in (0, 8):
        rows = pl.ds(half, 8)
        ends = [
            combine([end_basis[k, q, rows] for k in range(ITERS + 1)]) for q in range(PER_GROUP)
        ]
        for p in range(X):
            g, q = divmod(p + HALO, PER_GROUP)
            inner = combine([basis[k, p, rows] for k in range(ITERS + 1)])
            both = []
            for value, end in zip(inner, ends[q]):
                low = pltpu.roll(end, (Z - GROUP * g - LOW_AT) % Z, 1)
                high = pltpu.roll(end, (Z - GROUP * g - HIGH_AT) % Z, 1)
                value = jnp.where(lane < HALO, low, value)
                both.append(jnp.where(lane >= Z - HALO, high, value))
            closing[p, rows] = fields[1, p, rows] + both[0]
            mismatch[p, rows] = both[1]


def trade(near, far, axes):
    ends = lax.axis_size(axes) - 1
    others = [p for i in range(1, ends, 2) for p in ((i, i + 1), (i + 1, i))]
    return lax.ppermute(far, axes, others), lax.all_gather(near, axes[1], axis=0)


def exchange(copies, axes):
    return lax.all_to_all(copies, axes, split_axis=0, concat_axis=0, tiled=True)


def body(opening, source, category, table, flags):
    brick = (X, Y, Z)
    place_x, place_y, place_z = (lax.axis_index(axes[1]).reshape(1) for axes in (GX, GY, GZ))
    whole = pltpu.VMEM(brick, jnp.int32)
    fields, near, far, theta = call(
        prepare,
        [SMEM] + [HBM] * 5,
        [(4, *brick), (SLAB_X, Y, Z), (SLAB_X, Y, Z), (ITERS, 8, Z)],
        [brick, brick, whole, whole, pltpu.SMEM(table.shape, F32), pltpu.SemaphoreType.DMA((5,))],
    )(
        place_x,
        *(
            pltpu.with_memory_space_constraint(a, pltpu.HBM)
            for a in (opening, source, category, flags, table)
        ),
    )
    by_x = trade(near, far, GX)
    near, far = call(slabs_y, [SMEM] * 2 + [VMEM] * 3, [(SLAB_Y, Z)] * 2)(
        place_x, place_y, fields, *by_x
    )
    by_y = trade(near, far, GY)
    packed = (PER_GROUP, ROWS, Z)
    wide, near, far = call(assemble, [SMEM] * 3 + [VMEM] * 5, [(4, PLANES, ROWS, Z), packed, packed])(
        place_x, place_y, place_z, fields, *by_x, *by_y
    )
    far, chip = trade(near, far, GZ)
    sided = (PLANES, ROWS, Z)
    middle = (3, PLANES, ROWS + 16, Z)
    basis, sums, ends = call(
        interior,
        [VMEM] * 2,
        [(ITERS + 1, *brick), (len(PAIRS), 8, Z), (4, *packed)],
        [middle, (4, *packed), (3, *sided)] + [sided] * 7,
        flops=20000000,
        vmem=12,
    )(wide, theta)
    first, second = (*GY, "gz_1"), (*GX, "gz_0")
    end_basis, dots = call(
        edges,
        [SMEM] + [VMEM] * 5,
        [(ITERS + 1, PER_GROUP, Y, Z), (lax.axis_size(first), 1, Z)],
        [(3, PER_GROUP, ROWS + 16, Z), (3, PER_GROUP + 2, ROWS, Z), (Z, Z)],
        flops=5000000,
    )(place_z, ends, far, chip, theta, sums)
    parts = exchange(dots, first)
    (copies,) = call(relay, [VMEM], [(lax.axis_size(second), 1, Z)])(parts)
    parts = exchange(copies, second)
    closing, mismatch = call(finish, [VMEM] * 5, [brick, brick])(
        parts, basis, end_basis, fields, theta
    )
    return closing, mismatch


def solution(mesh):
    pairs = [n for size in mesh.devices.shape for n in (size // 2, 2)]
    split = Mesh(mesh.devices.reshape(pairs), (*GX, *GY, *GZ))
    spec = P(GX, GY, GZ)
    return jax.shard_map(
        body, mesh=split, in_specs=(spec, spec, spec, P(), spec), out_specs=(spec, spec), check_vma=False
    )
```

```python
import jax
import jax.numpy as jnp
from jax import lax
from jax.experimental import pallas as pl
from jax.experimental.pallas import tpu as pltpu
from jax.sharding import Mesh
from jax.sharding import PartitionSpec as P

ITERS = 4
GX, GY, GZ = (("gx_0", "gx_1"), ("gy_0", "gy_1"), ("gz_0", "gz_1"))
F32 = jnp.float32
X, Y, Z = 8, 16, 128
HALO = ITERS + 1
WIDTHS = (5, 5, 4, 3)
PLANES = X + 2 * HALO
ROWS = 32
TOP = 8
SLAB_X = sum(WIDTHS)
AT_X = (0, 5, 10, 14)
AT_Y = (0, 90, 180, 244)
SLAB_Y = 288
GROUPS, PER_GROUP, GROUP = 4, 5, 32
LOW_AT, HIGH_AT = 5, 26
SCALE = 64.0
CHUNK = 3
PAIRS = [(i, j) for i in range(ITERS) for j in range(i, ITERS + 1)]
VMEM = pl.BlockSpec(memory_space=pltpu.VMEM)
HBM = pl.BlockSpec(memory_space=pltpu.HBM)
SMEM = pl.BlockSpec(memory_space=pltpu.SMEM)


def planes_of(k):
    return range(HALO - WIDTHS[k], PLANES - HALO + WIDTHS[k])


def call(kernel, ins, outs, scratch=(), flops=100000, vmem=8):
    return pl.pallas_call(
        kernel,
        in_specs=ins,
        out_specs=[VMEM] * len(outs),
        out_shape=[jax.ShapeDtypeStruct(s, F32) for s in outs],
        scratch_shapes=[pltpu.VMEM(s, F32) if isinstance(s, tuple) else s for s in scratch],
        compiler_params=pltpu.CompilerParams(vmem_limit_bytes=vmem * 2**20),
        cost_estimate=pl.CostEstimate(flops=flops, bytes_accessed=1000000, transcendentals=0),
    )


def prepare(
    place_x, opening_at, source_at, category_at, flags_at, table_at, fields, near, far, theta,
    opening, source, category, flags, table, arrived,
):
    copies = [
        pltpu.make_async_copy(a, b, arrived.at[n])
        for n, (a, b) in enumerate(
            (
                (table_at, table),
                (category_at, category),
                (flags_at, flags),
                (opening_at, opening),
                (source_at, source),
            )
        )
    ]
    for copy in copies:
        copy.start()
    for copy in copies:
        copy.wait()
    for k, shift in enumerate(shifts_of(table)):
        theta[k] = shift
    for p in range(X):
        kind = category[p]
        cond = jnp.full((Y, Z), table[0], F32)
        for n in range(1, table.shape[0]):
            cond = jnp.where(kind == n, table[n], cond)
        flag = flags[p].astype(F32)
        start = opening[p]
        values = (cond, start, 2.0 * source[p] - 6.0 * flag * start, flag)
        for k, v in enumerate(values):
            fields[k, p] = v
    first = place_x[0] == 0
    for k, w in enumerate(WIDTHS):
        for n in range(w):
            low, high = fields[k, n], fields[k, X - w + n]
            near[AT_X[k] + n] = jnp.where(first, high, low)
            far[AT_X[k] + n] = jnp.where(first, low, high)


def halo(place, far, pair, at, lower):
    far_side = (place == 0) if lower else (place == 1)
    return jnp.where(far_side, far[at], pair[(1 - place, *at)])


def plane(place, fields, far, pair, k, p, rows=slice(None)):
    if p < HALO:
        return halo(place, far, pair, (AT_X[k] + p - (HALO - WIDTHS[k]), rows), True)
    if p < HALO + X:
        return fields[k, p - HALO, rows]
    return halo(place, far, pair, (AT_X[k] + p - HALO - X, rows), False)


def slabs_y(place_x, place_y, fields, far_x, pair_x, near, far):
    first = place_y[0] == 0
    for k, w in enumerate(WIDTHS):
        for n, p in enumerate(planes_of(k)):
            to = pl.ds(AT_Y[k] + w * n, w)
            low, high = (
                plane(place_x[0], fields, far_x, pair_x, k, p, pl.ds(at, w)) for at in (0, Y - w)
            )
            near[to] = jnp.where(first, high, low)
            far[to] = jnp.where(first, low, high)


def assemble(place_x, place_y, place_z, fields, far_x, pair_x, far_y, pair_y, wide, near, far):
    lane = lax.broadcasted_iota(jnp.int32, (ROWS, Z), 1)
    first_core = place_z[0] == 0
    nothing = jnp.zeros((8, Z), F32)
    for k, w in enumerate(WIDTHS):
        for n, p in enumerate(planes_of(k)):
            at = (pl.ds(AT_Y[k] + w * n, w),)
            wide[k, p, 0:TOP] = nothing
            wide[k, p, TOP + Y : ROWS] = nothing
            wide[k, p, TOP : TOP + Y] = plane(place_x[0], fields, far_x, pair_x, k, p)
            wide[k, p, TOP - w : TOP] = halo(place_y[0], far_y, pair_y, at, True)
            wide[k, p, TOP + Y : TOP + Y + w] = halo(place_y[0], far_y, pair_y, at, False)
    for q in range(PER_GROUP):
        low = jnp.zeros((ROWS, Z), F32)
        high = low
        for g in range(GROUPS):
            p = PER_GROUP * g + q
            for k, w in enumerate(WIDTHS):
                if p in planes_of(k):
                    base = GROUP * g + AT_X[k]
                    turned = pltpu.roll(wide[k, p], base, 1)
                    place = lane if base else jnp.where(lane < Z // 2, lane, lane - Z)
                    low = jnp.where((place >= base) & (place < base + w), turned, low)
                    high = jnp.where((place >= base - w) & (place < base), turned, high)
        far[q] = jnp.where(first_core, low, high)
        near[q] = jnp.where(first_core, high, low)


def shifts_of(table):
    values = [jnp.full((8, Z), table[n], F32) for n in range(table.shape[0])]
    least, most, mean = values[0], values[0], values[0]
    for v in values[1:]:
        least, most, mean = jnp.minimum(least, v), jnp.maximum(most, v), mean + v
    mean = mean * (1.0 / len(values))
    top = 4.0 + 16.0 * most + 16.0 * mean
    low = 2.0 + 8.0 * least + 8.0 * mean
    middle, half = 0.5 * (top + low), 0.5 * (top - low)
    return [
        (middle + half * c) * (1.0 / SCALE) for c in (-0.9238795, 0.9238795, -0.3826834, 0.3826834)
    ]


def smooth_xy(mid, planes, first, count):
    n = planes.shape[0] - 2
    pairs = planes[:-1] + planes[1:]
    mid[0:n, 8 : 8 + ROWS] = pairs[:-1] + pairs[1:]
    sides = mid[0:n, pl.ds(7 + first, count)] + mid[0:n, pl.ds(9 + first, count)]
    return mid[0:n, pl.ds(8 + first, count)] + 0.5 * sides


def smooth_z(here, low, high):
    return here + 0.5 * (low + high)


def turned(values):
    return pltpu.roll(values, 1, 2), pltpu.roll(values, Z - 1, 2)


def newton_step(slope, diag, inside, shift, v, tv, tu):
    return ((diag - shift) * v - (slope * tv + tu)) * inside


def chunks(low, high, most):
    count = -(-(high - low) // most)
    size = -(-(high - low) // count)
    return [(p, min(p + size, high)) for p in range(low, high, size)]


def interior(wide, theta, basis, sums, ends, mid, tops, slopes, diag, inside, va, vb, za, zb, zc):
    lane = lax.broadcasted_iota(jnp.int32, (ROWS, Z), 1)
    slots = mid.shape[0]
    slot = [0]

    def smoothed(ref, p, q, first=0, count=ROWS):
        slot[0] += 1
        return smooth_xy(mid.at[slot[0] % slots], ref[p - 1 : q + 1], first, count)

    place, from_high = lane % GROUP, (lane + HALO) % Z
    low_cells = (place >= LOW_AT) & (place < LOW_AT + 2 * HALO)
    high_cells = (place >= HIGH_AT - 2 * HALO) & (place < HIGH_AT)

    def pack(k, q):
        low = high = jnp.zeros((ROWS, Z), F32)
        for g in range(GROUPS):
            p = PER_GROUP * g + q
            if p in planes_of(k):
                both = pltpu.roll(wide[k, p], GROUP * g + LOW_AT, 1)
                low = jnp.where((lane // GROUP == g) & low_cells, both, low)
                here = (from_high // GROUP == g) & (from_high % GROUP < 2 * HALO)
                high = jnp.where(here, both, high)
        ends[k, q] = jnp.where(low_cells, low, 0.0)
        tops[k, q] = high

    to_pack = [(k, q) for k in range(4) for q in range(PER_GROUP)]

    def in_turn(low, high, turn, then):
        waiting, done = [], low + 1
        for p, q in chunks(low, high, CHUNK):
            turn(p, q)
            if to_pack:
                pack(*to_pack.pop(0))
            waiting.append((done, q - 1))
            done = q - 1
            if len(waiting) > 1:
                then(*waiting.pop(0))
        then(*waiting.pop(0))

    cond, start, rest, flag = (wide.at[k] for k in range(4))

    def turn_first(p, q):
        c, x = cond[p:q], start[p:q]
        (c_low, c_high), (x_low, x_high) = turned(c), turned(x)
        za[p:q] = smooth_z(c, c_low, c_high)
        zb[p:q] = smooth_z(x, x_low, x_high)
        zc[p:q] = smooth_z(c * x, c_low * x_low, c_high * x_high)
        for n, values in enumerate((c, c_low, c_high)):
            slopes[n, p:q] = values * (1.0 / SCALE)

    def first_vector(p, q):
        tc, tx, tcx = (smoothed(ref, p, q) for ref in (za, zb, zc))
        c = cond[p:q]
        near = 16.0 * c + tc
        diag[p:q] = (1.0 + 6.0 * flag[p:q] + near) * (1.0 / SCALE)
        there = jnp.where(c > 0.0, 1.0, 0.0)
        inside[p:q] = there
        va[p:q] = (rest[p:q] - near * start[p:q] + (c * tx + tcx)) * there

    in_turn(0, PLANES, turn_first, first_vector)
    basis[0] = va[HALO : HALO + X, TOP : TOP + Y]
    for k in range(ITERS):
        v_old, v_new = (va, vb) if k % 2 == 0 else (vb, va)
        last = k + 1 == ITERS
        first, count = (TOP, Y) if last else (0, ROWS)
        rows = pl.ds(first, count)
        shift = jnp.tile(theta[k], (count // 8, 1))[None]

        def turn(p, q):
            v = v_old[p:q]
            low, high = turned(v)
            za[p:q] = smooth_z(v, low, high)
            zb[p:q] = smooth_z(slopes[0, p:q] * v, slopes[1, p:q] * low, slopes[2, p:q] * high)

        def next_vector(p, q):
            tv, tu = smoothed(za, p, q, first, count), smoothed(zb, p, q, first, count)
            v = newton_step(slopes[0, p:q, rows], diag[p:q, rows], inside[p:q, rows], shift, v_old[p:q, rows], tv, tu)
            if last:
                basis[k + 1, p - HALO : q - HALO] = v
            else:
                v_new[p:q] = v

        in_turn(1 + k, PLANES - 1 - k, turn, next_vector)
        if not last:
            basis[k + 1] = v_new[HALO : HALO + X, TOP : TOP + Y]
    while to_pack:
        pack(*to_pack.pop(0))

    inner = (lane[:8] >= HALO) & (lane[:8] < Z - HALO)
    for n, (i, j) in enumerate(PAIRS):
        total = None
        for p in range(X):
            for half in (0, 8):
                rows = pl.ds(half, 8)
                term = basis[i, p, rows] * basis[j, p, rows]
                total = term if total is None else total + term
        sums[n] = jnp.where(inner, total, 0.0)

    for k in range(4):
        ends[k] = jnp.where(high_cells, pltpu.roll(tops[k], HIGH_AT - LOW_AT, 2), ends[k])


def edges(place_z, ends, far, chip, theta, inner_sums, basis, dots, mid, slopes, stack):
    lane = lax.broadcasted_iota(jnp.int32, (ROWS, Z), 1)
    place = lane % GROUP
    slots = mid.shape[0]
    slot = [0]

    below, above = (halo(place_z[0], far, chip, (slice(None),), lower) for lower in (True, False))

    def cells(k):
        low = pltpu.roll(below, (LOW_AT - AT_X[k]) % Z, 2)
        high = pltpu.roll(above, (HIGH_AT - AT_X[k]) % Z, 2)
        out = jnp.where(place < LOW_AT, low, ends[k])
        return jnp.where((place >= HIGH_AT) & (place < HIGH_AT + HALO), high, out)

    def smoothed(planes, first=0, count=ROWS):
        slot[0] += 1
        return smooth_xy(mid.at[slot[0] % slots], planes, first, count)

    def spread(values):
        return [
            jnp.concatenate(
                [
                    pltpu.roll(values[PER_GROUP - 1], GROUP + by, 1)[None],
                    pltpu.roll(values, by % Z, 2) if by else values,
                    pltpu.roll(values[0], Z - GROUP + by, 1)[None],
                ]
            )
            for by in (0, 1, -1)
        ]

    cond, start = cells(0), cells(1)
    cs, xs = spread(cond), spread(start)
    tc, tx, tcx = (
        smoothed(smooth_z(*values)) for values in (cs, xs, [c * x for c, x in zip(cs, xs)])
    )
    for n, values in enumerate(cs):
        slopes[n] = values * (1.0 / SCALE)
    rest, flag = cells(2), cells(3)
    near = 16.0 * cond + tc
    diag = (1.0 + 6.0 * flag + near) * (1.0 / SCALE)
    there = jnp.where(cond > 0.0, 1.0, 0.0)
    v = (rest - near * start + (cond * tx + tcx)) * there
    basis[0] = v[:, TOP : TOP + Y]
    for k in range(ITERS):
        last = k + 1 == ITERS
        first, count = (TOP, Y) if last else (0, ROWS)
        rows = slice(first, first + count)
        shift = jnp.tile(theta[k], (count // 8, 1))[None]
        vs = spread(v)
        tv = smoothed(smooth_z(*vs), first, count)
        tu = smoothed(smooth_z(*(slopes[n] * values for n, values in enumerate(vs))), first, count)
        v = newton_step(slopes[0, 1:-1][:, rows], diag[:, rows], there[:, rows], shift, v[:, rows], tv, tu)
        basis[k + 1] = v if last else v[:, TOP : TOP + Y]

    end_cells = ((place >= LOW_AT) & (place < LOW_AT + HALO)) | ((place >= HIGH_AT - HALO) & (place < HIGH_AT))
    mine = []
    for q in range(PER_GROUP):
        own = [g for g in range(GROUPS) if HALO <= PER_GROUP * g + q < HALO + X]
        at = (lane >= GROUP * own[0]) & (lane < GROUP * (own[-1] + 1))
        mine.append(jnp.where(at & end_cells, 1.0, 0.0)[:8])
    for n in range(16):
        total = None
        if n < len(PAIRS):
            i, j = PAIRS[n]
            total = inner_sums[n]
            for q in range(PER_GROUP):
                for half in (0, 8):
                    rows = pl.ds(half, 8)
                    total = total + (basis[i, q, rows] * mine[q]) * basis[j, q, rows]
        else:
            total = jnp.zeros((8, Z), F32)
        stack[pl.ds(8 * n, 8)] = total
    by_sum = stack[pl.ds(0, 16, stride=8)]
    for n in range(1, 8):
        by_sum = by_sum + stack[pl.ds(n, 16, stride=8)]
    total = lax.dot_general(
        jnp.ones((8, Z), F32), jnp.tile(by_sum, (8, 1)), (((1,), (1,)), ((), ())),
        precision=lax.Precision.HIGHEST, preferred_element_type=F32,
    )
    for n in range(dots.shape[0]):
        dots[n] = total[0:1]


def two_sum(a, b):
    s = a + b
    t = s - a
    return s, (a - (s - t)) + (b - t)


def row_sum(parts):
    rows = [(parts[n, 0:1], None) for n in range(parts.shape[0])]
    while len(rows) > 1:
        pairs, rows = zip(rows[::2], rows[1::2]), []
        for (a, ea), (b, eb) in pairs:
            s, e = two_sum(a, b)
            rows.append((s, e if ea is None else e + (ea + eb)))
    return rows[0]


def relay(parts, copies):
    total, rest = row_sum(parts)
    for n in range(copies.shape[0]):
        copies[n, 0:1] = total
        copies[n, 1:2] = rest


def quick(a, b):
    s = a + b
    return s, b - (s - a)


def halves(a):
    t = 4097.0 * a
    high = t - (t - a)
    return high, a - high


def plus(a, b):
    s, e = two_sum(a[0], b[0])
    return quick(s, e + (a[1] + b[1]))


def minus(a, b):
    return plus(a, (-b[0], -b[1]))


def times(a, b):
    p = a[0] * b[0]
    ah, al = halves(a[0])
    bh, bl = halves(b[0])
    e = ((ah * bh - p) + ah * bl + al * bh) + al * bl
    return quick(p, e + (a[0] * b[1] + a[1] * b[0]))


def reciprocal(a):
    q = 1.0 / a[0]
    qh, ql = halves(q)
    ah, al = halves(a[0])
    p = q * a[0]
    rest = ((1.0 - p) - (((qh * ah - p) + qh * al + ql * ah) + ql * al)) - q * a[1]
    return quick(q, q * rest)


def coefficients(gram, theta):
    none = jnp.zeros_like(theta[0])
    shift = [(t, none) for t in theta]
    system = [
        [plus(gram[i, j + 1], times(shift[j], gram[i, j])) for j in range(i + 1)]
        for i in range(ITERS)
    ]
    right = [gram[i, 0] for i in range(ITERS)]
    lower, inverse = {}, []
    for j in range(ITERS):
        inverse.append(reciprocal(system[j][j]))
        for i in range(j + 1, ITERS):
            lower[i, j] = times(system[i][j], inverse[j])
        for i in range(j + 1, ITERS):
            for k in range(j + 1, i + 1):
                system[i][k] = minus(system[i][k], times(lower[i, j], system[k][j]))
            right[i] = minus(right[i], times(lower[i, j], right[j]))
    y = [None] * ITERS
    for i in reversed(range(ITERS)):
        y[i] = times(right[i], inverse[i])
        for k in reversed(range(i + 1, ITERS)):
            y[i] = minus(y[i], times(lower[k, i], y[k]))
    r = [minus((none + 1.0, none), times(shift[0], y[0]))]
    for k in range(1, ITERS):
        total = plus(y[k - 1], times(shift[k], y[k]))
        r.append((-total[0], -total[1]))
    r.append((-y[-1][0], -y[-1][1]))
    return [a[0] * (1.0 / SCALE) for a in y], [a[0] for a in r]


def finish(parts, basis, end_basis, fields, theta, closing, mismatch):
    total, rest = row_sum(parts)
    for n in range(parts.shape[0]):
        rest = rest + parts[n, 1:2]
    gram = {}
    for n, (i, j) in enumerate(PAIRS):
        gram[i, j] = gram[j, i] = quick(
            *(jnp.broadcast_to(v[0:1, n : n + 1], (8, Z)) for v in (total, rest))
        )
    y, r = coefficients(gram, [theta[k] for k in range(ITERS)])

    def combine(v):
        x, m = y[0] * v[0], r[ITERS] * v[ITERS]
        for k in range(1, ITERS):
            x = x + y[k] * v[k]
        for k in range(ITERS):
            m = m + r[k] * v[k]
        return x, m

    lane = lax.broadcasted_iota(jnp.int32, (8, Z), 1)
    for half in (0, 8):
        rows = pl.ds(half, 8)
        ends = [
            combine([end_basis[k, q, rows] for k in range(ITERS + 1)]) for q in range(PER_GROUP)
        ]
        for p in range(X):
            g, q = divmod(p + HALO, PER_GROUP)
            inner = combine([basis[k, p, rows] for k in range(ITERS + 1)])
            both = []
            for value, end in zip(inner, ends[q]):
                low = pltpu.roll(end, (Z - GROUP * g - LOW_AT) % Z, 1)
                high = pltpu.roll(end, (Z - GROUP * g - HIGH_AT) % Z, 1)
                value = jnp.where(lane < HALO, low, value)
                both.append(jnp.where(lane >= Z - HALO, high, value))
            closing[p, rows] = fields[1, p, rows] + both[0]
            mismatch[p, rows] = both[1]


def trade(near, far, axes):
    ends = lax.axis_size(axes) - 1
    others = [p for i in range(1, ends, 2) for p in ((i, i + 1), (i + 1, i))]
    return lax.ppermute(far, axes, others), lax.all_gather(near, axes[1], axis=0)


def exchange(copies, axes):
    return lax.all_to_all(copies, axes, split_axis=0, concat_axis=0, tiled=True)


def body(opening, source, category, table, flags):
    brick = (X, Y, Z)
    place_x, place_y, place_z = (lax.axis_index(axes[1]).reshape(1) for axes in (GX, GY, GZ))
    whole = pltpu.VMEM(brick, jnp.int32)
    fields, near, far, theta = call(
        prepare,
        [SMEM] + [HBM] * 5,
        [(4, *brick), (SLAB_X, Y, Z), (SLAB_X, Y, Z), (ITERS, 8, Z)],
        [brick, brick, whole, whole, pltpu.SMEM(table.shape, F32), pltpu.SemaphoreType.DMA((5,))],
    )(
        place_x,
        *(
            pltpu.with_memory_space_constraint(a, pltpu.HBM)
            for a in (opening, source, category, flags, table)
        ),
    )
    by_x = trade(near, far, GX)
    near, far = call(slabs_y, [SMEM] * 2 + [VMEM] * 3, [(SLAB_Y, Z)] * 2)(
        place_x, place_y, fields, *by_x
    )
    by_y = trade(near, far, GY)
    packed = (PER_GROUP, ROWS, Z)
    wide, near, far = call(assemble, [SMEM] * 3 + [VMEM] * 5, [(4, PLANES, ROWS, Z), packed, packed])(
        place_x, place_y, place_z, fields, *by_x, *by_y
    )
    far, chip = trade(near, far, GZ)
    sided = (PLANES, ROWS, Z)
    middle = (3, PLANES, ROWS + 16, Z)
    basis, sums, ends = call(
        interior,
        [VMEM] * 2,
        [(ITERS + 1, *brick), (len(PAIRS), 8, Z), (4, *packed)],
        [middle, (4, *packed), (3, *sided)] + [sided] * 7,
        flops=20000000,
        vmem=12,
    )(wide, theta)
    first, second = (*GY, "gz_1"), (*GX, "gz_0")
    end_basis, dots = call(
        edges,
        [SMEM] + [VMEM] * 5,
        [(ITERS + 1, PER_GROUP, Y, Z), (lax.axis_size(first), 1, Z)],
        [(3, PER_GROUP, ROWS + 16, Z), (3, PER_GROUP + 2, ROWS, Z), (Z, Z)],
        flops=5000000,
    )(place_z, ends, far, chip, theta, sums)
    parts = exchange(dots, first)
    (copies,) = call(relay, [VMEM], [(lax.axis_size(second), 2, Z)])(parts)
    parts = exchange(copies, second)
    closing, mismatch = call(finish, [VMEM] * 5, [brick, brick])(
        parts, basis, end_basis, fields, theta
    )
    return closing, mismatch


def solution(mesh):
    pairs = [n for size in mesh.devices.shape for n in (size // 2, 2)]
    split = Mesh(mesh.devices.reshape(pairs), (*GX, *GY, *GZ))
    spec = P(GX, GY, GZ)
    return jax.shard_map(
        body, mesh=split, in_specs=(spec, spec, spec, P(), spec), out_specs=(spec, spec), check_vma=False
    )
```
